32 devices in a mesh: dp: 2 (over x), sp2: 4 (over z), sp: 4 (over y, core).
Axes of the slice: x: 2, y: 2, z: 4, core: 2. Of those that a mesh axis runs over, the one named last changes fastest.
Arguments:
- x: bfloat16 [32, 64, 512, 64], P('dp', 'sp', 'sp2'), parts along dimension 0
- w_a: bfloat16 [4, 3, 3, 64, 64], replicated
- bn_a: float32 [4, 2, 64], replicated
- w_down: bfloat16 [3, 3, 64, 128], replicated
- bn_down: float32 [2, 128], replicated
- w_b: bfloat16 [1, 3, 3, 128, 128], replicated
- bn_b: float32 [1, 2, 128], replicated
Outputs:
- output: bfloat16 [32, 32, 256, 128], P('dp', 'sp', 'sp2'), parts along dimension 0
There are 2 independent parts. The reference program is written for one: setup_inputs(seed, part) draws one part's arguments, and reference() takes and returns one part's arrays. A program takes and returns all parts, laid end to end along the dimension named above; an argument that names none is the same for every part.
All inputs are finite; a program needn't handle non-finite values.
Results may differ from the reference program's by a relative error of at most 0.00533103.
Values are sent between devices in bfloat16 or wider.
A program may use at most 1 GiB of HBM per device.

```python
import jax
import jax.numpy as jnp
from jax import lax

IMAGES = 16
IMG_HEIGHT = 64
IMG_WIDTH = 512
CHAN_A = 64
CHAN_B = 128
LAYERS_A = 4
LAYERS_B = 1

CONV_DIMS = ("NHWC", "HWIO", "NHWC")
SAME_PADS = ((1, 1), (1, 1))
DOWN_PADS = ((0, 1), (0, 1))


def norm_pairs(pair_key, lead_shape, num_chan):
    gain_key, shift_key = jax.random.split(pair_key)
    gains = 1.0 + 0.3 * jax.random.normal(gain_key, lead_shape + (1, num_chan), jnp.float32)
    shifts = 0.5 * jax.random.normal(shift_key, lead_shape + (1, num_chan), jnp.float32)
    return jnp.concatenate([gains, shifts], axis=-2)


def conv_weights(w_key, lead_shape, chan_in, chan_out):
    raw_w = jax.random.normal(w_key, lead_shape + (3, 3, chan_in, chan_out), jnp.float32)
    return (raw_w * (9 * chan_in) ** -0.5).astype(jnp.bfloat16)


def setup_inputs(seed: int = 0, part: int = 0) -> dict:
    sub_keys = jax.random.split(jax.random.key(seed), 7)
    img_keys = jax.random.split(jax.random.fold_in(sub_keys[0], part), 3)
    noise = jax.random.normal(img_keys[0], (IMAGES, IMG_HEIGHT, IMG_WIDTH, CHAN_A), jnp.float32)
    row_amp = jax.random.normal(img_keys[1], (IMAGES, 1, 1, CHAN_A), jnp.float32)
    col_amp = jax.random.normal(img_keys[2], (IMAGES, 1, 1, CHAN_A), jnp.float32)
    row_pos = (2.0 * (jnp.arange(IMG_HEIGHT, dtype=jnp.float32) + 0.5) / IMG_HEIGHT - 1.0).reshape(1, IMG_HEIGHT, 1, 1)
    col_pos = (2.0 * (jnp.arange(IMG_WIDTH, dtype=jnp.float32) + 0.5) / IMG_WIDTH - 1.0).reshape(1, 1, IMG_WIDTH, 1)
    images = (noise + 1.5 * row_amp * row_pos + col_amp * col_pos).astype(jnp.bfloat16)
    return {
        "x": images,
        "w_a": conv_weights(sub_keys[1], (LAYERS_A,), CHAN_A, CHAN_A),
        "bn_a": norm_pairs(sub_keys[2], (LAYERS_A,), CHAN_A),
        "w_down": conv_weights(sub_keys[3], (), CHAN_A, CHAN_B),
        "bn_down": norm_pairs(sub_keys[4], (), CHAN_B),
        "w_b": conv_weights(sub_keys[5], (LAYERS_B,), CHAN_B, CHAN_B),
        "bn_b": norm_pairs(sub_keys[6], (LAYERS_B,), CHAN_B),
    }


def conv_bn(act_in, weight, norm_pair, stride, pad_pairs):
    pre_norm = lax.conv_general_dilated(act_in.astype(jnp.float32), weight.astype(jnp.float32), (stride, stride), pad_pairs, dimension_numbers=CONV_DIMS)
    num_pos = pre_norm.shape[0] * pre_norm.shape[1] * pre_norm.shape[2]
    mean_val = jnp.sum(pre_norm, axis=(0, 1, 2)) / num_pos
    var_val = jnp.sum(pre_norm * pre_norm, axis=(0, 1, 2)) / num_pos - mean_val * mean_val
    normed = norm_pair[0] * (pre_norm - mean_val) * lax.rsqrt(var_val + 1e-5) + norm_pair[1]
    return jnp.maximum(normed, 0.0).astype(jnp.bfloat16)


def reference(x, w_a, bn_a, w_down, bn_down, w_b, bn_b):
    def stage_step(carry_act, layer_in):
        return conv_bn(carry_act, layer_in[0], layer_in[1], 1, SAME_PADS), None

    act_out, scan_rest = lax.scan(stage_step, x, (w_a, bn_a))
    act_out = conv_bn(act_out, w_down, bn_down, 2, DOWN_PADS)
    act_out, scan_rest = lax.scan(stage_step, act_out, (w_b, bn_b))
    return act_out
```

```python
import functools

import jax
import jax.numpy as jnp
from jax import lax
from jax.experimental import pallas as pl
from jax.experimental.pallas import tpu as pltpu
from jax.sharding import PartitionSpec as P

MESH = pl.DeviceIdType.MESH
F32 = jnp.float32
BF16 = jnp.bfloat16
BIG = 3.0e38
EPS = 1e-5
PAD = 8


def kernel(dims, x_ref, w_a, bn_a, w_down, bn_down, w_b, bn_b, out_ref,
           xv, z, as0, as1, bb0, bb1, wmat, edge_l, edge_r, halo_u, halo_d, halo_l, halo_r, corner_s, corner_r,
           stats, acc, cst, caps, x_sem, row_send, row_recv, col_send, col_recv, cor_send, cor_recv, st_send, st_recv):
    n_img, rows, pairs, ch, n_sp2, n_sp = dims
    half = rows // 2
    last = PAD + pairs
    n_dev = n_sp2 * n_sp
    sp = lax.axis_index("sp")
    sp2 = lax.axis_index("sp2")
    me = sp2 * n_sp + sp
    has_u, has_d = sp > 0, sp < n_sp - 1
    has_l, has_r = sp2 > 0, sp2 < n_sp2 - 1

    def x_copy(img):
        return pltpu.make_async_copy(x_ref.at[img], xv.at[img], x_sem.at[img])

    for img in range(n_img):
        x_copy(img).start()

    def clear(img, carry):
        for par in range(2):
            halo_u[par, img] = jnp.zeros((pairs + 2 * PAD, 128), F32)
            halo_d[par, img] = jnp.zeros((pairs + 2 * PAD, 128), F32)
            halo_l[par, img] = jnp.zeros((rows, 128), F32)
            halo_r[par, img] = jnp.zeros((rows, 128), F32)
        return carry

    lax.fori_loop(0, n_img, clear, 0)
    for par in range(2):
        for c in range(4):
            corner_r[par, c] = jnp.zeros((n_img, 128), F32)

    sub = lax.broadcasted_iota(jnp.int32, (8, 128), 0)
    lane8 = lax.broadcasted_iota(jnp.int32, (8, 128), 1)
    caps[0] = jnp.where((sub == 0) & (lane8 >= ch), jnp.where(has_l, BIG, 0.0), BIG)
    caps[1] = jnp.where((sub == 7) & (lane8 < ch), jnp.where(has_r, BIG, 0.0), BIG)
    caps[2] = jnp.full((8, 128), jnp.where(has_u, BIG, 0.0), F32)
    caps[3] = jnp.full((8, 128), jnp.where(has_d, BIG, 0.0), F32)
    caps[4] = jnp.where(sub == 0, jnp.where(has_l, BIG, 0.0), BIG)
    caps[5] = jnp.where(sub == 7, jnp.where(has_r, BIG, 0.0), BIG)

    barrier = pltpu.get_barrier_semaphore()
    for d in range(1, n_dev):
        peer = lax.rem(me + d, n_dev)
        pl.semaphore_signal(barrier, inc=1, device_id={"sp2": peer // n_sp, "sp": lax.rem(peer, n_sp)}, device_id_type=MESH)
    pl.semaphore_wait(barrier, n_dev - 1)

    def rcopy(src, dst, ssem, rsem, to_sp2, to_sp):
        return pltpu.make_async_remote_copy(src_ref=src, dst_ref=dst, send_sem=ssem, recv_sem=rsem,
                                            device_id={"sp2": to_sp2, "sp": to_sp}, device_id_type=MESH)

    row_data = pl.ds(PAD, pairs)

    def start_edges(img, par, n_rows):
        @pl.when(has_u)
        def _():
            rcopy(z.at[img, 0, row_data], halo_d.at[par, img, row_data], row_send.at[0], row_recv.at[par, 1], sp2, sp - 1).start()

        @pl.when(has_d)
        def _():
            rcopy(z.at[img, n_rows - 1, row_data], halo_u.at[par, img, row_data], row_send.at[1], row_recv.at[par, 0], sp2, sp + 1).start()

        r_all = pl.ds(0, n_rows)

        @pl.when(has_l)
        def _():
            rcopy(edge_l.at[img, r_all], halo_r.at[par, img, r_all], col_send.at[0], col_recv.at[par, 1], sp2 - 1, sp).start()

        @pl.when(has_r)
        def _():
            rcopy(edge_r.at[img, r_all], halo_l.at[par, img, r_all], col_send.at[1], col_recv.at[par, 0], sp2 + 1, sp).start()

    corner_to = ((has_u & has_l, -1, -1, 3), (has_u & has_r, 1, -1, 2), (has_d & has_l, -1, 1, 1), (has_d & has_r, 1, 1, 0))

    def start_corners(par):
        for c, (there, d_sp2, d_sp, slot) in enumerate(corner_to):
            @pl.when(there)
            def _():
                rcopy(corner_s.at[c], corner_r.at[par, slot], cor_send.at[c], cor_recv.at[par, slot], sp2 + d_sp2, sp + d_sp).start()

    def wait_edges(par, n_rows):
        r_all = pl.ds(0, n_rows)
        every = pl.ds(0, n_img)

        @pl.when(has_u)
        def _():
            rcopy(z.at[every, 0, row_data], halo_u.at[par, every, row_data], row_send.at[0], row_recv.at[par, 0], sp2, sp).wait()

        @pl.when(has_d)
        def _():
            rcopy(z.at[every, n_rows - 1, row_data], halo_d.at[par, every, row_data], row_send.at[1], row_recv.at[par, 1], sp2, sp).wait()

        @pl.when(has_l)
        def _():
            rcopy(edge_l.at[every, r_all], halo_l.at[par, every, r_all], col_send.at[0], col_recv.at[par, 0], sp2, sp).wait()

        @pl.when(has_r)
        def _():
            rcopy(edge_r.at[every, r_all], halo_r.at[par, every, r_all], col_send.at[1], col_recv.at[par, 1], sp2, sp).wait()

        for c, (there, d_sp2, d_sp, slot) in enumerate(corner_to):
            @pl.when(there)
            def _():
                rcopy(corner_s.at[c], corner_r.at[par, c], cor_send.at[c], cor_recv.at[par, c], sp2, sp).wait()

    def stat_copy(d, par):
        peer = lax.rem(me + d, n_dev)
        return rcopy(stats.at[par, me], stats.at[par, me], st_send.at[d - 1], st_recv.at[par, me], peer // n_sp, lax.rem(peer, n_sp))

    def start_stats(par):
        total = acc[0] + acc[1]
        both = jnp.concatenate([jnp.sum(total[:, :128], axis=0, keepdims=True), jnp.sum(total[:, 128:], axis=0, keepdims=True)], axis=0)
        stats[par, me] = both
        for d in range(1, n_dev):
            stat_copy(d, par).start()

    def wait_stats(par):
        for d in range(1, n_dev):
            stat_copy(d, par).wait_send()
            src = lax.rem(me + d, n_dev)
            rcopy(stats.at[par, src], stats.at[par, src], st_send.at[d - 1], st_recv.at[par, src], sp2, sp).wait_recv()

    def set_constants(par, gain, shift, count, paired):
        total = stats[par, 0]
        for src in range(1, n_dev):
            total = total + stats[par, src]
        if paired:
            total = total + pltpu.roll(total, ch, 1)
        mean = total[0:1] * (1.0 / count)
        var = total[1:2] * (1.0 / count) - mean * mean
        cst[0:1, :] = mean
        cst[1:2, :] = gain * lax.rsqrt(var + EPS)
        cst[2:3, :] = shift

    lane = lax.broadcasted_iota(jnp.int32, (pairs, 128), 1)

    def save_edges(img, n_rows):
        for r in range(n_rows):
            edge_l[img, r:r + 1, :] = z[img, r, PAD:PAD + 1, :]
            edge_r[img, r:r + 1, :] = z[img, r, last - 1:last, :]
        here = pl.ds(img, 1)
        corner_s[0, here, :] = z[img, 0, PAD:PAD + 1, :]
        corner_s[1, here, :] = z[img, 0, last - 1:last, :]
        corner_s[2, here, :] = z[img, n_rows - 1, PAD:PAD + 1, :]
        corner_s[3, here, :] = z[img, n_rows - 1, last - 1:last, :]

    def place_halos(img, par, n_rows):
        for r in range(n_rows):
            z[img, r, PAD - 1:PAD, :] = halo_l[par, img, r:r + 1, :]
            z[img, r, last:last + 1, :] = halo_r[par, img, r:r + 1, :]
        here = pl.ds(img, 1)
        halo_u[par, img, PAD - 1:PAD, :] = corner_r[par, 0, here, :]
        halo_u[par, img, last:last + 1, :] = corner_r[par, 1, here, :]
        halo_d[par, img, PAD - 1:PAD, :] = corner_r[par, 2, here, :]
        halo_d[par, img, last:last + 1, :] = corner_r[par, 3, here, :]

    def line_views(img, par, n_rows):
        def view(p):
            if p == 0:
                return lambda off: halo_u[par, img, off:off + pairs, :]
            if p == n_rows + 1:
                return lambda off: halo_d[par, img, off:off + pairs, :]
            return lambda off: z[img, p - 1, off:off + pairs, :]
        return view

    def normalise(v, lower):
        return jnp.maximum((v - cst[0:1, :]) * cst[1:2, :] + cst[2:3, :], lower)

    def cap_cols(v, first, final):
        return jnp.concatenate([jnp.minimum(v[0:8], caps[first]), v[8:pairs - 8], jnp.minimum(v[pairs - 8:], caps[final])], axis=0)

    def build_pairs(img, par, dst, lower, skip_top=False):
        place_halos(img, par, rows)
        view = line_views(img, par, rows)
        for p in range(1 if skip_top else 0, rows + 2):
            load = view(p)
            own = load(PAD)
            if lower is None:
                side = jnp.where(lane < ch, load(PAD + 1), load(PAD - 1))
            else:
                own = normalise(own, lower)
                side = normalise(jnp.where(lane < ch, load(PAD + 1), load(PAD - 1)), lower)
            side = cap_cols(side, 0, 1) if lower is not None else mask_cols(side)
            if p in (0, rows + 1):
                edge = 2 if p == 0 else 3
                if lower is not None:
                    own = jnp.minimum(own, caps[edge, 0:1, :])
                    side = jnp.minimum(side, caps[edge, 0:1, :])
            base = (p % 2) * 256
            dst[p // 2, :, base:base + 128] = own.astype(BF16)
            dst[p // 2, :, base + 128:base + 256] = side.astype(BF16)

    def mask_cols(v):
        return v

    def build_wide(img, par, dst):
        place_halos(img, par, half)
        view = line_views(img, par, half)
        for p in range(half + 2):
            load = view(p)
            base = (p % 2) * 384
            for k in range(3):
                v = normalise(load(PAD - 1 + k), 0.0)
                if k == 0:
                    v = jnp.concatenate([jnp.minimum(v[0:8], caps[4]), v[8:]], axis=0)
                if k == 2:
                    v = jnp.concatenate([v[:pairs - 8], jnp.minimum(v[pairs - 8:], caps[5])], axis=0)
                if p in (0, half + 1):
                    v = jnp.minimum(v, caps[2 if p == 0 else 3, 0:1, :])
                dst[p // 2, :, base + 128 * k:base + 128 * (k + 1)] = v.astype(BF16)

    def add_stats(o):
        folded = o.reshape(o.shape[0] // 8, 8, o.shape[1])
        s = jnp.sum(folded, axis=0)
        q = jnp.sum(folded * folded, axis=0)
        acc[0] += jnp.concatenate([s[:, :128], q[:, :128]], axis=1)
        acc[1] += jnp.concatenate([s[:, 128:], q[:, 128:]], axis=1)

    def put_rows(img, o):
        for i in range(o.shape[0] // pairs):
            part = o[i * pairs:(i + 1) * pairs]
            z[img, 2 * i, row_data, :] = part[:, :128]
            z[img, 2 * i + 1, row_data, :] = part[:, 128:]

    def dot(a, b):
        return jnp.dot(a, b, preferred_element_type=F32)

    def conv_pairs(img, src):
        o = dot(src[0:half].reshape(half * pairs, 512), wmat[0:512]) + dot(src[1:half + 1].reshape(half * pairs, 512), wmat[512:1024])
        put_rows(img, o)
        add_stats(o)
        save_edges(img, rows)

    def conv_down(img, src):
        quarter = half // 2

        def pick(offset, lo):
            return jnp.concatenate([src[2 * i + offset, :, lo:512] for i in range(quarter)], axis=0)

        o = dot(pick(0, 256), wmat[0:256]) + dot(pick(1, 0), wmat[256:768]) + dot(pick(2, 0), wmat[768:1280])
        put_rows(img, o)
        add_stats(o)
        save_edges(img, half)

    def conv_wide(img, src):
        quarter = half // 2
        o = dot(src[0:quarter].reshape(quarter * pairs, 768), wmat[0:768]) + dot(src[1:quarter + 1].reshape(quarter * pairs, 768), wmat[768:1536])
        put_rows(img, o)
        add_stats(o)

    def run_layer(build, conv, buf0, buf1, par_out, rows_out, send):
        acc[...] = jnp.zeros_like(acc)
        build(0, buf0)

        def body(t, carry):
            i0 = 2 * t
            build(i0 + 1, buf1)
            conv(i0, buf0)
            if send:
                start_edges(i0, par_out, rows_out)
            build(jnp.minimum(i0 + 2, n_img - 1), buf0)
            conv(i0 + 1, buf1)
            if send:
                start_edges(i0 + 1, par_out, rows_out)
            return carry

        lax.fori_loop(0, n_img // 2, body, 0)

    def put_block(k, n_rows_k, n_taps, blocks):
        for o, blk in enumerate(blocks):
            val = jnp.zeros((n_rows_k, 128), BF16) if blk is None else blk
            wmat[k * n_rows_k:(k + 1) * n_rows_k, o * 128:(o + 1) * 128] = val

    def weights_pairs(layer):
        zero = jnp.zeros((ch, ch), BF16)
        q = []
        for kh in range(3):
            w0, w1, w2 = w_a[layer, kh, 0], w_a[layer, kh, 1], w_a[layer, kh, 2]
            q.append(jnp.concatenate([
                jnp.concatenate([w1, w0], axis=1),
                jnp.concatenate([w2, w1], axis=1),
                jnp.concatenate([zero, w2], axis=1),
                jnp.concatenate([w0, zero], axis=1)], axis=0))
        for k in range(4):
            put_block(k, 256, 4, [q[k] if k < 3 else None, q[k - 1] if k > 0 else None])

    def weights_down():
        d = [jnp.concatenate([w_down[kh, 0], w_down[kh, 1], w_down[kh, 2], jnp.zeros((ch, 128), BF16)], axis=0) for kh in range(3)]
        for k in range(5):
            put_block(k, 256, 4, [d[k] if k < 3 else None, d[k - 2] if k >= 2 else None])

    def weights_wide():
        e = [jnp.concatenate([w_b[0, kh, 0], w_b[0, kh, 1], w_b[0, kh, 2]], axis=0) for kh in range(3)]
        for k in range(4):
            put_block(k, 384, 3, [e[k] if k < 3 else None, e[k - 1] if k > 0 else None])

    wrow = lax.broadcasted_iota(jnp.int32, (128, 128), 0)
    wcol = lax.broadcasted_iota(jnp.int32, (128, 128), 1)
    source = jnp.where(wrow < pairs, 2 * wrow, 2 * (wrow - pairs) + 1)
    wmat[0:128, 0:128] = jnp.where(source == wcol, 1.0, 0.0).astype(BF16)

    def load_image(img, carry):
        x_copy(img).wait()
        for g in range(rows // 4):
            block = xv[img, 4 * g:4 * g + 4].reshape(4 * ch, 128)
            t = lax.dot_general(wmat[0:128, 0:128], block, (((1,), (1,)), ((), ())), preferred_element_type=F32)
            for b in range(2):
                even = t[0:pairs, 128 * b:128 * b + 128]
                odd = t[pairs:2 * pairs, 128 * b:128 * b + 128]
                r = 4 * g + 2 * b
                z[img, r, row_data, :] = jnp.where(lane < ch, even, pltpu.roll(odd, ch, 1))
                z[img, r + 1, row_data, :] = jnp.where(lane < ch, pltpu.roll(even, ch, 1), odd)
        save_edges(img, rows)
        start_edges(img, 0, rows)
        return carry

    lax.fori_loop(0, n_img, load_image, 0)
    start_corners(0)

    count_a = float(n_dev * n_img * rows * pairs * 2)
    count_b = float(n_dev * n_img * half * pairs)

    weights_pairs(0)
    wait_edges(0, rows)
    run_layer(lambda i, buf: build_pairs(i, 0, buf, None), conv_pairs, as0, as1, 1, rows, True)
    start_corners(1)
    start_stats(1)

    def gains(layer):
        g, s = bn_a[layer, 0:1, :], bn_a[layer, 1:2, :]
        return jnp.concatenate([g, g], axis=1), jnp.concatenate([s, s], axis=1)

    n_layers = w_a.shape[0]

    def a_layer(layer, carry):
        par = lax.rem(layer, 2)
        weights_pairs(layer)
        wait_edges(par, rows)
        wait_stats(par)
        g, s = gains(layer - 1)
        set_constants(par, g, s, count_a, True)
        run_layer(lambda i, buf: build_pairs(i, par, buf, 0.0), conv_pairs, as0, as1, 1 - par, rows, True)
        start_corners(1 - par)
        start_stats(1 - par)
        return carry

    lax.fori_loop(1, n_layers, a_layer, 0)

    par = n_layers % 2
    weights_down()
    wait_edges(par, rows)
    wait_stats(par)
    g, s = gains(n_layers - 1)
    set_constants(par, g, s, count_a, True)
    run_layer(lambda i, buf: build_pairs(i, par, buf, 0.0, True), conv_down, as0, as1, 1 - par, half, True)
    start_corners(1 - par)
    start_stats(1 - par)

    weights_wide()
    wait_edges(1 - par, half)
    wait_stats(1 - par)
    set_constants(1 - par, bn_down[0:1, :], bn_down[1:2, :], count_b, False)
    run_layer(lambda i, buf: build_wide(i, 1 - par, buf), conv_wide, bb0, bb1, par, half, False)
    start_stats(par)
    wait_stats(par)
    set_constants(par, bn_b[0, 0:1, :], bn_b[0, 1:2, :], count_b, False)

    def finish(img, carry):
        for r in range(half):
            out_ref[img, r] = normalise(z[img, r, row_data, :], 0.0).astype(BF16)
        return carry

    lax.fori_loop(0, n_img, finish, 0)


def solution(mesh):
    n_sp, n_sp2 = mesh.shape["sp"], mesh.shape["sp2"]

    def per_device(x, w_a, bn_a, w_down, bn_down, w_b, bn_b):
        n_img, rows, cols, ch = x.shape
        pairs, half = cols // 2, rows // 2
        n_dev = n_sp * n_sp2
        dims = (n_img, rows, pairs, ch, n_sp2, n_sp)
        wide = pairs + 2 * PAD
        vmem = pltpu.VMEM
        dma = pltpu.SemaphoreType.DMA
        scratch = [
            vmem((n_img, rows, ch, cols), BF16),
            vmem((n_img, rows, wide, 128), F32),
            vmem((half + 1, pairs, 512), BF16),
            vmem((half + 1, pairs, 512), BF16),
            vmem((half // 2 + 1, pairs, 768), BF16),
            vmem((half // 2 + 1, pairs, 768), BF16),
            vmem((1536, 256), BF16),
            vmem((n_img, rows, 128), F32),
            vmem((n_img, rows, 128), F32),
            vmem((2, n_img, wide, 128), F32),
            vmem((2, n_img, wide, 128), F32),
            vmem((2, n_img, rows, 128), F32),
            vmem((2, n_img, rows, 128), F32),
            vmem((4, n_img, 128), F32),
            vmem((2, 4, n_img, 128), F32),
            vmem((2, n_dev, 2, 128), F32),
            vmem((2, 8, 256), F32),
            vmem((8, 128), F32),
            vmem((6, 8, 128), F32),
            dma((n_img,)),
            dma((2,)), dma((2, 2)),
            dma((2,)), dma((2, 2)),
            dma((4,)), dma((2, 4)),
            dma((n_dev - 1,)), dma((2, n_dev)),
        ]
        in_vmem = pl.BlockSpec(memory_space=pltpu.VMEM)
        return pl.pallas_call(
            functools.partial(kernel, dims),
            out_shape=jax.ShapeDtypeStruct((n_img, half, pairs, 128), BF16),
            in_specs=[pl.BlockSpec(memory_space=pl.ANY)] + [in_vmem] * 6,
            out_specs=in_vmem,
            scratch_shapes=scratch,
            compiler_params=pltpu.CompilerParams(collective_id=0, has_side_effects=True, vmem_limit_bytes=56 * 1024 * 1024),
        )(jnp.transpose(x, (0, 1, 3, 2)), w_a, bn_a, w_down, bn_down, w_b, bn_b)

    tile_spec = P("dp", "sp", "sp2", None)
    return jax.shard_map(per_device, mesh=mesh, in_specs=(tile_spec, P(), P(), P(), P(), P(), P()), out_specs=tile_spec, check_vma=False)
```

```python
import functools

import jax
import jax.numpy as jnp
from jax import lax
from jax.experimental import pallas as pl
from jax.experimental.pallas import tpu as pltpu
from jax.sharding import PartitionSpec as P

MESH = pl.DeviceIdType.MESH
F32 = jnp.float32
BF16 = jnp.bfloat16
EPS = 1e-5
GROUP = 2
EDGE = 8


def normalise(v, cst):
    return jnp.maximum((v - cst[0:1, :]) * cst[1:2, :] + cst[2:3, :], 0.0)


def stack_kernel(dims, x_ref, w_a, bn_a, w_down, bn_down, w_b, bn_b, z_out, cst_out,
                 xv, z, as0, as1, bb0, bb1, lines, wmat, perm, edge_l, edge_r, halo_u, halo_d, halo_l, halo_r,
                 corner_s, corner_r, corner_n, stats, acc, cst,
                 x_sem, z_sem, row_send, row_recv, col_send, col_recv, cor_send, cor_recv, st_send, st_recv):
    n_img, rows, pairs, ch, n_sp2, n_sp = dims
    half, quarter = rows // 2, rows // 4
    wide = pairs + 2 * EDGE
    n_dev = n_sp2 * n_sp
    sp = lax.axis_index("sp")
    sp2 = lax.axis_index("sp2")
    me = sp2 * n_sp + sp
    has_u, has_d = sp > 0, sp < n_sp - 1
    has_l, has_r = sp2 > 0, sp2 < n_sp2 - 1

    def x_copy(img):
        return pltpu.make_async_copy(x_ref.at[img], xv.at[img], x_sem.at[img])

    for img in range(n_img):
        x_copy(img).start()

    barrier = pltpu.get_barrier_semaphore()
    for d in range(1, n_dev):
        peer = lax.rem(me + d, n_dev)
        pl.semaphore_signal(barrier, inc=1, device_id={"sp2": peer // n_sp, "sp": lax.rem(peer, n_sp)}, device_id_type=MESH)

    def rcopy(src, dst, ssem, rsem, to_sp2, to_sp):
        return pltpu.make_async_remote_copy(src_ref=src, dst_ref=dst, send_sem=ssem, recv_sem=rsem,
                                            device_id={"sp2": to_sp2, "sp": to_sp}, device_id_type=MESH)

    def start_edges(img, par, n_rows):
        r_all = pl.ds(0, n_rows)

        @pl.when(has_u)
        def _():
            rcopy(z.at[img, 0], halo_d.at[par, img], row_send.at[0], row_recv.at[par, 1], sp2, sp - 1).start()

        @pl.when(has_d)
        def _():
            rcopy(z.at[img, n_rows - 1], halo_u.at[par, img], row_send.at[1], row_recv.at[par, 0], sp2, sp + 1).start()

        @pl.when(has_l)
        def _():
            rcopy(edge_l.at[img, r_all], halo_r.at[par, img, r_all], col_send.at[0], col_recv.at[par, 1], sp2 - 1, sp).start()

        @pl.when(has_r)
        def _():
            rcopy(edge_r.at[img, r_all], halo_l.at[par, img, r_all], col_send.at[1], col_recv.at[par, 0], sp2 + 1, sp).start()

    corner_to = ((has_u & has_l, -1, -1, 3), (has_u & has_r, 1, -1, 2), (has_d & has_l, -1, 1, 1), (has_d & has_r, 1, 1, 0))

    def start_corners(par):
        for c, (there, d_sp2, d_sp, slot) in enumerate(corner_to):
            @pl.when(there)
            def _():
                rcopy(corner_s.at[c], corner_r.at[par, slot], cor_send.at[c], cor_recv.at[par, slot], sp2 + d_sp2, sp + d_sp).start()

    def wait_edges(par, n_rows):
        r_all = pl.ds(0, n_rows)
        every = pl.ds(0, n_img)

        @pl.when(has_u)
        def _():
            rcopy(z.at[every, 0], halo_u.at[par], row_send.at[0], row_recv.at[par, 0], sp2, sp).wait()

        @pl.when(has_d)
        def _():
            rcopy(z.at[every, n_rows - 1], halo_d.at[par], row_send.at[1], row_recv.at[par, 1], sp2, sp).wait()

        @pl.when(has_l)
        def _():
            rcopy(edge_l.at[every, r_all], halo_l.at[par, every, r_all], col_send.at[0], col_recv.at[par, 0], sp2, sp).wait()

        @pl.when(has_r)
        def _():
            rcopy(edge_r.at[every, r_all], halo_r.at[par, every, r_all], col_send.at[1], col_recv.at[par, 1], sp2, sp).wait()

        for c, (there, d_sp2, d_sp, slot) in enumerate(corner_to):
            @pl.when(there)
            def _():
                rcopy(corner_s.at[c], corner_r.at[par, c], cor_send.at[c], cor_recv.at[par, c], sp2, sp).wait()

    def stat_copy(d, par):
        peer = lax.rem(me + d, n_dev)
        return rcopy(stats.at[par, me], stats.at[par, me], st_send.at[d - 1], st_recv.at[par, me], peer // n_sp, lax.rem(peer, n_sp))

    def start_stats(par):
        total = acc[0] + acc[1]
        stats[par, me] = jnp.concatenate([jnp.sum(total[:, :128], axis=0, keepdims=True), jnp.sum(total[:, 128:], axis=0, keepdims=True)], axis=0)
        for d in range(1, n_dev):
            stat_copy(d, par).start()

    def wait_stats(par):
        for d in range(1, n_dev):
            stat_copy(d, par).wait_send()
            src = lax.rem(me + d, n_dev)
            rcopy(stats.at[par, src], stats.at[par, src], st_send.at[d - 1], st_recv.at[par, src], sp2, sp).wait_recv()

    def set_constants(par, gain, shift, count, paired):
        total = stats[par, 0]
        for src in range(1, n_dev):
            total = total + stats[par, src]
        if paired:
            total = total + pltpu.roll(total, ch, 1)
        mean = total[0:1] * (1.0 / count)
        var = total[1:2] * (1.0 / count) - mean * mean
        cst[0:1, :] = mean
        cst[1:2, :] = gain * lax.rsqrt(var + EPS)
        cst[2:3, :] = shift

    lane = lax.broadcasted_iota(jnp.int32, (pairs, 128), 1)

    def save_edges(img, n_rows):
        flat = z.at[img].reshape(rows * pairs, 128)
        first = flat[pl.ds(0, n_rows, stride=pairs), :]
        final = flat[pl.ds(pairs - 1, n_rows, stride=pairs), :]
        edge_l[img, 0:n_rows, :] = first
        edge_r[img, 0:n_rows, :] = final
        here = pl.ds(img, 1)
        corner_s[0, here, :] = first[0:1]
        corner_s[1, here, :] = final[0:1]
        corner_s[2, here, :] = first[n_rows - 1:n_rows]
        corner_s[3, here, :] = final[n_rows - 1:n_rows]

    def act(v, raw):
        return v if raw else normalise(v, cst)

    def prepare_corners(par, raw):
        for c, (there, d_sp2, d_sp, slot) in enumerate(corner_to):
            corner_n[c] = jnp.where(there, act(corner_r[par, c], raw), 0.0)

    def fill_lines(img, par, a, n_rows, raw, first_p):
        left = jnp.where(has_l, act(halo_l[par, img, 0:n_rows, :], raw), 0.0)
        right = jnp.where(has_r, act(halo_r[par, img, 0:n_rows, :], raw), 0.0)
        lines[a, pl.ds(wide + EDGE - 1, n_rows, stride=wide), :] = left
        lines[a, pl.ds(wide + EDGE + pairs, n_rows, stride=wide), :] = right
        here = pl.ds(img, 1)
        bottom = (n_rows + 1) * wide
        lines[a, EDGE - 1:EDGE, :] = corner_n[0, here, :]
        lines[a, EDGE + pairs:EDGE + pairs + 1, :] = corner_n[1, here, :]
        lines[a, bottom + EDGE - 1:bottom + EDGE, :] = corner_n[2, here, :]
        lines[a, bottom + EDGE + pairs:bottom + EDGE + pairs + 1, :] = corner_n[3, here, :]
        out = []
        for p in range(first_p, n_rows + 2):
            if p == 0:
                v = jnp.where(has_u, act(halo_u[par, img], raw), 0.0)
            elif p == n_rows + 1:
                v = jnp.where(has_d, act(halo_d[par, img], raw), 0.0)
            else:
                v = act(z[img, p - 1], raw)
            base = p * wide + EDGE
            lines[a, base:base + pairs, :] = v
            out.append((p, base, v))
        return out

    def build_pairs(g, par, dst, raw, first_p=0):
        for a in range(GROUP):
            for p, base, own in fill_lines(g * GROUP + a, par, a, rows, raw, first_p):
                side = jnp.where(lane < ch, lines[a, base + 1:base + 1 + pairs, :], lines[a, base - 1:base - 1 + pairs, :])
                dst[2 * (p % 2), a, p // 2] = own.astype(BF16)
                dst[2 * (p % 2) + 1, a, p // 2] = side.astype(BF16)

    def build_wide(g, par, dst):
        for a in range(GROUP):
            for p, base, own in fill_lines(g * GROUP + a, par, a, half, False, 0):
                c = 3 * (p % 2)
                dst[c, a, p // 2] = lines[a, base - 1:base - 1 + pairs, :].astype(BF16)
                dst[c + 1, a, p // 2] = own.astype(BF16)
                dst[c + 2, a, p // 2] = lines[a, base + 1:base + 1 + pairs, :].astype(BF16)

    def finish_conv(g, o, n_pairs):
        folded = o.reshape(o.shape[0] // 8, 8, 256)
        s = jnp.sum(folded, axis=0)
        q = jnp.sum(folded * folded, axis=0)
        acc[0] += jnp.concatenate([s[:, :128], q[:, :128]], axis=1)
        acc[1] += jnp.concatenate([s[:, 128:], q[:, 128:]], axis=1)
        for a in range(GROUP):
            for i in range(n_pairs):
                at = (a * n_pairs + i) * pairs
                z[g * GROUP + a, 2 * i] = o[at:at + pairs, :128]
                z[g * GROUP + a, 2 * i + 1] = o[at:at + pairs, 128:]

    def dot(parts, lo):
        lhs = jnp.concatenate(parts, axis=1)
        hi = lo + lhs.shape[1]
        rhs = jnp.concatenate([wmat[0, lo:hi], wmat[1, lo:hi]], axis=1)
        return jnp.dot(lhs, rhs, preferred_element_type=F32)

    def conv_pairs(g, src):
        def part(c, lo):
            return src[c, :, lo:lo + half].reshape(GROUP * half * pairs, 128)

        o = dot([part(c, 0) for c in range(4)], 0) + dot([part(c, 1) for c in range(4)], 512)
        finish_conv(g, o, half)
        for a in range(GROUP):
            save_edges(g * GROUP + a, rows)

    def conv_down(g, src):
        def part(c, offset):
            return jnp.concatenate([src[c, a, 2 * i + offset] for a in range(GROUP) for i in range(quarter)], axis=0)

        o = (dot([part(c, 0) for c in (2, 3)], 0) + dot([part(c, 1) for c in range(4)], 256) + dot([part(c, 2) for c in range(4)], 768))
        finish_conv(g, o, quarter)
        for a in range(GROUP):
            save_edges(g * GROUP + a, half)

    def conv_wide(g, src):
        def part(c, lo):
            return src[c, :, lo:lo + quarter].reshape(GROUP * quarter * pairs, 128)

        o = dot([part(c, 0) for c in range(6)], 0) + dot([part(c, 1) for c in range(6)], 768)
        finish_conv(g, o, quarter)

    n_groups = n_img // GROUP

    def run_layer(build, conv, buf0, buf1, done):
        acc[...] = jnp.zeros_like(acc)
        build(0, buf0)

        def body(t, carry):
            g = 2 * t
            build(g + 1, buf1)
            conv(g, buf0)
            done(g)
            build(jnp.minimum(g + 2, n_groups - 1), buf0)
            conv(g + 1, buf1)
            done(g + 1)
            return carry

        lax.fori_loop(0, n_groups // 2, body, 0)

    def send_edges(par, n_rows):
        def done(g):
            for a in range(GROUP):
                start_edges(g * GROUP + a, par, n_rows)
        return done

    def z_copy(g):
        some = pl.ds(g * GROUP, GROUP)
        return pltpu.make_async_copy(z.at[some, pl.ds(0, half)], z_out.at[some], z_sem.at[g])

    def put_block(k, n_k, blocks):
        for o, blk in enumerate(blocks):
            wmat[o, k * n_k:(k + 1) * n_k, :] = jnp.zeros((n_k, 128), BF16) if blk is None else blk

    def weights_pairs(layer):
        zero = jnp.zeros((ch, ch), BF16)
        q = []
        for kh in range(3):
            w0, w1, w2 = w_a[layer, kh, 0], w_a[layer, kh, 1], w_a[layer, kh, 2]
            q.append(jnp.concatenate([
                jnp.concatenate([w1, w0], axis=1),
                jnp.concatenate([w2, w1], axis=1),
                jnp.concatenate([zero, w2], axis=1),
                jnp.concatenate([w0, zero], axis=1)], axis=0))
        for k in range(4):
            put_block(k, 256, [q[k] if k < 3 else None, q[k - 1] if k > 0 else None])

    def weights_down():
        d = [jnp.concatenate([w_down[kh, 0], w_down[kh, 1], w_down[kh, 2], jnp.zeros((ch, 128), BF16)], axis=0) for kh in range(3)]
        for k in range(5):
            put_block(k, 256, [d[k] if k < 3 else None, d[k - 2] if k >= 2 else None])

    def weights_wide():
        e = [jnp.concatenate([w_b[0, kh, 0], w_b[0, kh, 1], w_b[0, kh, 2]], axis=0) for kh in range(3)]
        for k in range(4):
            put_block(k, 384, [e[k] if k < 3 else None, e[k - 1] if k > 0 else None])

    wrow = lax.broadcasted_iota(jnp.int32, (128, 128), 0)
    wcol = lax.broadcasted_iota(jnp.int32, (128, 128), 1)
    source = jnp.where(wrow < pairs, 2 * wrow, 2 * (wrow - pairs) + 1)
    perm[...] = jnp.where(source == wcol, 1.0, 0.0).astype(BF16)
    pl.semaphore_wait(barrier, n_dev - 1)

    def load_image(img, carry):
        x_copy(img).wait()
        for g in range(rows // 4):
            block = xv[img, 4 * g:4 * g + 4].reshape(4 * ch, 128)
            t = lax.dot_general(perm[...], block, (((1,), (1,)), ((), ())), preferred_element_type=F32)
            for b in range(2):
                even = t[0:pairs, 128 * b:128 * b + 128]
                odd = t[pairs:2 * pairs, 128 * b:128 * b + 128]
                r = 4 * g + 2 * b
                z[img, r] = jnp.where(lane < ch, even, pltpu.roll(odd, ch, 1))
                z[img, r + 1] = jnp.where(lane < ch, pltpu.roll(even, ch, 1), odd)
        save_edges(img, rows)
        start_edges(img, 0, rows)
        return carry

    lax.fori_loop(0, n_img, load_image, 0)
    start_corners(0)

    count_a = float(n_dev * n_img * rows * pairs * 2)
    count_b = float(n_dev * n_img * half * pairs)

    weights_pairs(0)
    wait_edges(0, rows)
    prepare_corners(0, True)
    run_layer(lambda g, buf: build_pairs(g, 0, buf, True), conv_pairs, as0, as1, send_edges(1, rows))
    start_stats(1)
    start_corners(1)

    def gains(layer):
        g, s = bn_a[layer, 0:1, :], bn_a[layer, 1:2, :]
        return jnp.concatenate([g, g], axis=1), jnp.concatenate([s, s], axis=1)

    n_layers = w_a.shape[0]

    def a_layer(layer, carry):
        par = lax.rem(layer, 2)
        weights_pairs(layer)
        wait_edges(par, rows)
        wait_stats(par)
        g, s = gains(layer - 1)
        set_constants(par, g, s, count_a, True)
        prepare_corners(par, False)
        run_layer(lambda g, buf: build_pairs(g, par, buf, False), conv_pairs, as0, as1, send_edges(1 - par, rows))
        start_stats(1 - par)
        start_corners(1 - par)
        return carry

    lax.fori_loop(1, n_layers, a_layer, 0)

    par = n_layers % 2
    weights_down()
    wait_edges(par, rows)
    wait_stats(par)
    g, s = gains(n_layers - 1)
    set_constants(par, g, s, count_a, True)
    prepare_corners(par, False)
    run_layer(lambda g, buf: build_pairs(g, par, buf, False, 1), conv_down, as0, as1, send_edges(1 - par, half))
    start_stats(1 - par)
    start_corners(1 - par)

    weights_wide()
    wait_edges(1 - par, half)
    wait_stats(1 - par)
    set_constants(1 - par, bn_down[0:1, :], bn_down[1:2, :], count_b, False)
    prepare_corners(1 - par, False)
    run_layer(lambda g, buf: build_wide(g, 1 - par, buf), conv_wide, bb0, bb1, lambda g: z_copy(g).start())
    start_stats(par)
    wait_stats(par)
    set_constants(par, bn_b[0, 0:1, :], bn_b[0, 1:2, :], count_b, False)
    cst_out[...] = cst[...]
    for g in range(n_groups):
        z_copy(g).wait()


def finish_kernel(z_ref, cst_ref, out_ref):
    for img in range(z_ref.shape[0]):
        for r in range(z_ref.shape[1]):
            out_ref[img, r] = normalise(z_ref[img, r], cst_ref).astype(BF16)


def solution(mesh):
    n_sp, n_sp2 = mesh.shape["sp"], mesh.shape["sp2"]

    def per_device(x, w_a, bn_a, w_down, bn_down, w_b, bn_b):
        n_img, rows, cols, ch = x.shape
        pairs, half = cols // 2, rows // 2
        n_dev = n_sp * n_sp2
        dims = (n_img, rows, pairs, ch, n_sp2, n_sp)
        vmem = pltpu.VMEM
        dma = pltpu.SemaphoreType.DMA
        scratch = [
            vmem((n_img, rows, ch, cols), BF16),
            vmem((n_img, rows, pairs, 128), F32),
            vmem((4, GROUP, half + 1, pairs, 128), BF16),
            vmem((4, GROUP, half + 1, pairs, 128), BF16),
            vmem((6, GROUP, half // 2 + 1, pairs, 128), BF16),
            vmem((6, GROUP, half // 2 + 1, pairs, 128), BF16),
            vmem((GROUP, (rows + 2) * (pairs + 2 * EDGE), 128), F32),
            vmem((2, 1536, 128), BF16),
            vmem((128, 128), BF16),
            vmem((n_img, rows, 128), F32),
            vmem((n_img, rows, 128), F32),
            vmem((2, n_img, pairs, 128), F32),
            vmem((2, n_img, pairs, 128), F32),
            vmem((2, n_img, rows, 128), F32),
            vmem((2, n_img, rows, 128), F32),
            vmem((4, n_img, 128), F32),
            vmem((2, 4, n_img, 128), F32),
            vmem((4, n_img, 128), F32),
            vmem((2, n_dev, 2, 128), F32),
            vmem((2, 8, 256), F32),
            vmem((8, 128), F32),
            dma((n_img,)),
            dma((n_img // GROUP,)),
            dma((2,)), dma((2, 2)),
            dma((2,)), dma((2, 2)),
            dma((4,)), dma((2, 4)),
            dma((n_dev - 1,)), dma((2, n_dev)),
        ]
        in_vmem = pl.BlockSpec(memory_space=pltpu.VMEM)
        in_any = pl.BlockSpec(memory_space=pl.ANY)
        z, cst = pl.pallas_call(
            functools.partial(stack_kernel, dims),
            out_shape=(jax.ShapeDtypeStruct((n_img, half, pairs, 128), F32), jax.ShapeDtypeStruct((8, 128), F32)),
            in_specs=[in_any] + [in_vmem] * 6,
            out_specs=(in_any, in_vmem),
            scratch_shapes=scratch,
            compiler_params=pltpu.CompilerParams(collective_id=0, has_side_effects=True, vmem_limit_bytes=48 * 1024 * 1024),
        )(jnp.transpose(x, (0, 1, 3, 2)), w_a, bn_a, w_down, bn_down, w_b, bn_b)
        block = pl.BlockSpec((GROUP, half, pairs, 128), lambda i: (i, 0, 0, 0))
        return pl.pallas_call(
            finish_kernel,
            grid=(n_img // GROUP,),
            out_shape=jax.ShapeDtypeStruct((n_img, half, pairs, 128), BF16),
            in_specs=[block, pl.BlockSpec((8, 128), lambda i: (0, 0))],
            out_specs=block,
        )(z, cst)

    tile_spec = P("dp", "sp", "sp2", None)
    return jax.shard_map(per_device, mesh=mesh, in_specs=(tile_spec, P(), P(), P(), P(), P(), P()), out_specs=tile_spec, check_vma=False)
```

```python
import functools

import jax
import jax.numpy as jnp
from jax import lax
from jax.experimental import pallas as pl
from jax.experimental.pallas import tpu as pltpu
from jax.sharding import PartitionSpec as P

MESH = pl.DeviceIdType.MESH
F32 = jnp.float32
BF16 = jnp.bfloat16
EPS = 1e-5
UNROLL = 4
SPLIT = 1
VMEM_LIMIT = 56 * 1024 * 1024
EDGE = 8


def normalise(v, cst):
    return jnp.maximum((v - cst[0:1, :]) * cst[1:2, :] + cst[2:3, :], 0.0)


def stack_kernel(dims, x_ref, w_a_ref, bn_a, w_down_ref, bn_down, w_b_ref, bn_b, z_out, cst_out,
                 xv, w_a, w_down, w_b, z, bufs, lines, wmat, perm, edge_u, edge_d, first_u, first_d, edge_l, edge_r, halo_u, halo_d, halo_l, halo_r,
                 corner_s, corner_r, corner_n, stats, acc, cst,
                 x_sem, w_sem, z_sem, row_send, row_recv, col_send, col_recv, cor_send, cor_recv, st_send, st_recv):
    n_img, rows, pairs, ch, n_sp2, n_sp = dims
    half, quarter = rows // 2, rows // 4
    wide = pairs + 2 * EDGE
    n_dev = n_sp2 * n_sp
    sp = lax.axis_index("sp")
    sp2 = lax.axis_index("sp2")
    me = sp2 * n_sp + sp
    has_u, has_d = sp > 0, sp < n_sp - 1
    has_l, has_r = sp2 > 0, sp2 < n_sp2 - 1

    def x_copy(img):
        return pltpu.make_async_copy(x_ref.at[img], xv.at[img], x_sem.at[img])

    for img in range(n_img):
        x_copy(img).start()

    w_copies = [pltpu.make_async_copy(src, dst, w_sem.at[i]) for i, (src, dst) in enumerate(((w_a_ref, w_a), (w_down_ref, w_down), (w_b_ref, w_b)))]
    for copy in w_copies:
        copy.start()

    barrier = pltpu.get_barrier_semaphore()
    for d in range(1, n_dev):
        peer = lax.rem(me + d, n_dev)
        pl.semaphore_signal(barrier, inc=1, device_id={"sp2": peer // n_sp, "sp": lax.rem(peer, n_sp)}, device_id_type=MESH)

    def rcopy(src, dst, ssem, rsem, to_sp2, to_sp):
        return pltpu.make_async_remote_copy(src_ref=src, dst_ref=dst, send_sem=ssem, recv_sem=rsem,
                                            device_id={"sp2": to_sp2, "sp": to_sp}, device_id_type=MESH)

    def start_edges(img, par, n_rows, first=False):
        r_all = pl.ds(0, n_rows)

        @pl.when(has_u)
        def _():
            src, dst = (edge_u.at[img], first_d.at[img]) if first else (z.at[img, 0], halo_d.at[par, img])
            rcopy(src, dst, row_send.at[0], row_recv.at[par, 1], sp2, sp - 1).start()

        @pl.when(has_d)
        def _():
            src, dst = (edge_d.at[img], first_u.at[img]) if first else (z.at[img, n_rows - 1], halo_u.at[par, img])
            rcopy(src, dst, row_send.at[1], row_recv.at[par, 0], sp2, sp + 1).start()

        @pl.when(has_l)
        def _():
            rcopy(edge_l.at[img, r_all], halo_r.at[par, img, r_all], col_send.at[0], col_recv.at[par, 1], sp2 - 1, sp).start()

        @pl.when(has_r)
        def _():
            rcopy(edge_r.at[img, r_all], halo_l.at[par, img, r_all], col_send.at[1], col_recv.at[par, 0], sp2 + 1, sp).start()

    corner_to = ((has_u & has_l, -1, -1, 3), (has_u & has_r, 1, -1, 2), (has_d & has_l, -1, 1, 1), (has_d & has_r, 1, 1, 0))

    def start_corners(par):
        for c, (there, d_sp2, d_sp, slot) in enumerate(corner_to):
            @pl.when(there)
            def _():
                rcopy(corner_s.at[c], corner_r.at[par, slot], cor_send.at[c], cor_recv.at[par, slot], sp2 + d_sp2, sp + d_sp).start()

    def wait_edges(par, n_rows, first=False):
        r_all = pl.ds(0, n_rows)
        every = pl.ds(0, n_img)

        @pl.when(has_u)
        def _():
            src, dst = (edge_u, first_u) if first else (z.at[every, 0], halo_u.at[par])
            rcopy(src, dst, row_send.at[0], row_recv.at[par, 0], sp2, sp).wait()

        @pl.when(has_d)
        def _():
            src, dst = (edge_d, first_d) if first else (z.at[every, n_rows - 1], halo_d.at[par])
            rcopy(src, dst, row_send.at[1], row_recv.at[par, 1], sp2, sp).wait()

        @pl.when(has_l)
        def _():
            rcopy(edge_l.at[every, r_all], halo_l.at[par, every, r_all], col_send.at[0], col_recv.at[par, 0], sp2, sp).wait()

        @pl.when(has_r)
        def _():
            rcopy(edge_r.at[every, r_all], halo_r.at[par, every, r_all], col_send.at[1], col_recv.at[par, 1], sp2, sp).wait()

        for c, (there, d_sp2, d_sp, slot) in enumerate(corner_to):
            @pl.when(there)
            def _():
                rcopy(corner_s.at[c], corner_r.at[par, c], cor_send.at[c], cor_recv.at[par, c], sp2, sp).wait()

    def stat_copy(d, par):
        peer = lax.rem(me + d, n_dev)
        return rcopy(stats.at[par, me], stats.at[par, me], st_send.at[d - 1], st_recv.at[par, me], peer // n_sp, lax.rem(peer, n_sp))

    def start_stats(par):
        total = acc[0] + acc[1]
        stats[par, me] = jnp.concatenate([jnp.sum(total[:, :128], axis=0, keepdims=True), jnp.sum(total[:, 128:], axis=0, keepdims=True)], axis=0)
        for d in range(1, n_dev):
            stat_copy(d, par).start()

    def wait_stats(par):
        for d in range(1, n_dev):
            stat_copy(d, par).wait_send()
            src = lax.rem(me + d, n_dev)
            rcopy(stats.at[par, src], stats.at[par, src], st_send.at[d - 1], st_recv.at[par, src], sp2, sp).wait_recv()

    def set_constants(par, gain, shift, count, paired):
        total = stats[par, 0]
        for src in range(1, n_dev):
            total = total + stats[par, src]
        if paired:
            total = total + pltpu.roll(total, ch, 1)
        mean = total[0:1] * (1.0 / count)
        var = total[1:2] * (1.0 / count) - mean * mean
        cst[0:1, :] = mean
        cst[1:2, :] = gain * lax.rsqrt(var + EPS)
        cst[2:3, :] = shift

    lane = lax.broadcasted_iota(jnp.int32, (pairs, 128), 1)

    def save_edges(img, n_rows):
        flat = z.at[img].reshape(rows * pairs, 128)
        first = flat[pl.ds(0, n_rows, stride=pairs), :]
        final = flat[pl.ds(pairs - 1, n_rows, stride=pairs), :]
        edge_l[img, 0:n_rows, :] = first
        edge_r[img, 0:n_rows, :] = final
        here = pl.ds(img, 1)
        corner_s[0, here, :] = first[0:1]
        corner_s[1, here, :] = final[0:1]
        corner_s[2, here, :] = first[n_rows - 1:n_rows]
        corner_s[3, here, :] = final[n_rows - 1:n_rows]

    def act(v, raw):
        return v if raw else normalise(v, cst)

    def prepare_corners(par, raw):
        for c, (there, d_sp2, d_sp, slot) in enumerate(corner_to):
            corner_n[c] = jnp.where(there, act(corner_r[par, c], raw), 0.0)

    def fill_lines(img, par, u, n_rows, raw, first_p):
        buf = lines[u]
        left = jnp.where(has_l, act(halo_l[par, img, 0:n_rows, :], raw), 0.0)
        right = jnp.where(has_r, act(halo_r[par, img, 0:n_rows, :], raw), 0.0)
        buf[pl.ds(wide + EDGE - 1, n_rows, stride=wide), :] = left
        buf[pl.ds(wide + EDGE + pairs, n_rows, stride=wide), :] = right
        here = pl.ds(img, 1)
        bottom = (n_rows + 1) * wide
        buf[EDGE - 1:EDGE, :] = corner_n[0, here, :]
        buf[EDGE + pairs:EDGE + pairs + 1, :] = corner_n[1, here, :]
        buf[bottom + EDGE - 1:bottom + EDGE, :] = corner_n[2, here, :]
        buf[bottom + EDGE + pairs:bottom + EDGE + pairs + 1, :] = corner_n[3, here, :]
        out = []
        for p in range(first_p, n_rows + 2):
            if p == 0:
                v = jnp.where(has_u, first_u[img].astype(F32) if raw else act(halo_u[par, img], raw), 0.0)
            elif p == n_rows + 1:
                v = jnp.where(has_d, first_d[img].astype(F32) if raw else act(halo_d[par, img], raw), 0.0)
            else:
                v = act(z[img, p - 1], raw)
            base = p * wide + EDGE
            buf[base:base + pairs, :] = v
            out.append((p, base, v))
        return out

    def build_pairs(img, par, u, raw, first_p=0):
        n_q = half + 1
        for p, base, own in fill_lines(img, par, u, rows, raw, first_p):
            side = jnp.where(lane < ch, lines[u][base + 1:base + 1 + pairs, :], lines[u][base - 1:base - 1 + pairs, :])
            bufs[u][2 * (p % 2) * n_q + p // 2] = own.astype(BF16)
            bufs[u][(2 * (p % 2) + 1) * n_q + p // 2] = side.astype(BF16)

    def build_wide(img, par, u):
        n_q = quarter + 1
        for p, base, own in fill_lines(img, par, u, half, False, 0):
            at = 3 * (p % 2) * n_q + p // 2
            bufs[u][at] = lines[u][base - 1:base - 1 + pairs, :].astype(BF16)
            bufs[u][at + n_q] = own.astype(BF16)
            bufs[u][at + 2 * n_q] = lines[u][base + 1:base + 1 + pairs, :].astype(BF16)

    def finish_conv(img, i0, o):
        folded = o.reshape(o.shape[0] // 8, 8, 256)
        s = jnp.sum(folded, axis=0)
        q = jnp.sum(folded * folded, axis=0)
        acc[0] += jnp.concatenate([s[:, :128], q[:, :128]], axis=1)
        acc[1] += jnp.concatenate([s[:, 128:], q[:, 128:]], axis=1)
        for i in range(o.shape[0] // pairs):
            z[img, 2 * (i0 + i)] = o[i * pairs:(i + 1) * pairs, :128]
            z[img, 2 * (i0 + i) + 1] = o[i * pairs:(i + 1) * pairs, 128:]

    def dot(parts):
        lhs = jnp.concatenate(parts, axis=1)
        rhs = jnp.concatenate([wmat[0, 0:lhs.shape[1]], wmat[1, 0:lhs.shape[1]]], axis=1)
        return jnp.dot(lhs, rhs, preferred_element_type=F32)

    def conv_pairs(img, u):
        n_q, n_i = half + 1, half // SPLIT
        for i0 in range(0, half, n_i):
            at = [c * n_q + i0 + lo for lo in (0, 1) for c in range(4)]
            finish_conv(img, i0, dot([bufs[u][k:k + n_i].reshape(n_i * pairs, 128) for k in at]))
        save_edges(img, rows)

    def conv_down(img, u):
        n_q = half + 1
        at = [c * n_q + k for k, c in ((0, 2), (0, 3), (1, 0), (1, 1), (1, 2), (1, 3), (2, 0), (2, 1), (2, 2), (2, 3))]
        finish_conv(img, 0, dot([jnp.concatenate([bufs[u][k + 2 * i] for i in range(quarter)], axis=0) for k in at]))
        save_edges(img, half)

    def conv_wide(img, u):
        n_q = quarter + 1
        at = [c * n_q + lo for lo in (0, 1) for c in range(6)]
        finish_conv(img, 0, dot([bufs[u][k:k + quarter].reshape(quarter * pairs, 128) for k in at]))

    def run_layer(build, conv, done):
        acc[...] = jnp.zeros_like(acc)

        def body(t, carry):
            for u in range(UNROLL):
                build(t * UNROLL + u, u)
                conv(t * UNROLL + u, u)
            for u in range(UNROLL):
                done(t * UNROLL + u)
            return carry

        lax.fori_loop(0, n_img // UNROLL, body, 0)

    def z_copy(img):
        return pltpu.make_async_copy(z.at[img, pl.ds(0, half)], z_out.at[img], z_sem.at[img])

    def put_block(k, n_k, blocks):
        for o, blk in enumerate(blocks):
            wmat[o, k * n_k:(k + 1) * n_k, :] = jnp.zeros((n_k, 128), BF16) if blk is None else blk

    def weights_pairs(layer):
        zero = jnp.zeros((ch, ch), BF16)
        q = []
        for kh in range(3):
            w0, w1, w2 = w_a[layer, kh, 0], w_a[layer, kh, 1], w_a[layer, kh, 2]
            q.append(jnp.concatenate([
                jnp.concatenate([w1, w0], axis=1),
                jnp.concatenate([w2, w1], axis=1),
                jnp.concatenate([zero, w2], axis=1),
                jnp.concatenate([w0, zero], axis=1)], axis=0))
        for k in range(4):
            put_block(k, 256, [q[k] if k < 3 else None, q[k - 1] if k > 0 else None])

    def weights_down():
        d = [jnp.concatenate([w_down[kh, 0], w_down[kh, 1], w_down[kh, 2], jnp.zeros((ch, 128), BF16)], axis=0) for kh in range(3)]
        for k in range(5):
            put_block(k, 256, [d[k] if k < 3 else None, d[k - 2] if k >= 2 else None])

    def weights_wide():
        e = [jnp.concatenate([w_b[0, kh, 0], w_b[0, kh, 1], w_b[0, kh, 2]], axis=0) for kh in range(3)]
        for k in range(4):
            put_block(k, 384, [e[k] if k < 3 else None, e[k - 1] if k > 0 else None])

    wrow = lax.broadcasted_iota(jnp.int32, (128, 128), 0)
    wcol = lax.broadcasted_iota(jnp.int32, (128, 128), 1)
    source = jnp.where(wrow < pairs, 2 * wrow, 2 * (wrow - pairs) + 1)
    perm[...] = jnp.where(source == wcol, 1.0, 0.0).astype(BF16)
    pl.semaphore_wait(barrier, n_dev - 1)

    def load_images(t, carry):
        for img in [t * UNROLL + u for u in range(UNROLL)]:
            x_copy(img).wait()
        for img in [t * UNROLL + u for u in range(UNROLL)]:
            for g in range(rows // 4):
                block = xv[img, 4 * g:4 * g + 4].reshape(4 * ch, 128)
                m = lax.dot_general(perm[...], block, (((1,), (1,)), ((), ())), preferred_element_type=F32)
                for b in range(2):
                    even = m[0:pairs, 128 * b:128 * b + 128]
                    odd = m[pairs:2 * pairs, 128 * b:128 * b + 128]
                    r = 4 * g + 2 * b
                    upper = jnp.where(lane < ch, even, pltpu.roll(odd, ch, 1))
                    lower = jnp.where(lane < ch, pltpu.roll(even, ch, 1), odd)
                    z[img, r] = upper
                    z[img, r + 1] = lower
                    if r == 0:
                        edge_u[img] = upper.astype(BF16)
                    if r + 2 == rows:
                        edge_d[img] = lower.astype(BF16)
            save_edges(img, rows)
        for img in [t * UNROLL + u for u in range(UNROLL)]:
            start_edges(img, 0, rows, True)
        return carry

    lax.fori_loop(0, n_img // UNROLL, load_images, 0)
    start_corners(0)

    count_a = float(n_dev * n_img * rows * pairs * 2)
    count_b = float(n_dev * n_img * half * pairs)

    for copy in w_copies:
        copy.wait()
    weights_pairs(0)
    wait_edges(0, rows, True)
    prepare_corners(0, True)
    run_layer(lambda i, u: build_pairs(i, 0, u, True), conv_pairs, lambda i: start_edges(i, 1, rows))
    start_stats(1)
    start_corners(1)

    def gains(layer):
        g, s = bn_a[layer, 0:1, :], bn_a[layer, 1:2, :]
        return jnp.concatenate([g, g], axis=1), jnp.concatenate([s, s], axis=1)

    n_layers = w_a.shape[0]

    def a_layer(layer, carry):
        par = lax.rem(layer, 2)
        weights_pairs(layer)
        wait_edges(par, rows)
        wait_stats(par)
        g, s = gains(layer - 1)
        set_constants(par, g, s, count_a, True)
        prepare_corners(par, False)
        run_layer(lambda i, u: build_pairs(i, par, u, False), conv_pairs, lambda i: start_edges(i, 1 - par, rows))
        start_stats(1 - par)
        start_corners(1 - par)
        return carry

    lax.fori_loop(1, n_layers, a_layer, 0)

    par = n_layers % 2
    weights_down()
    wait_edges(par, rows)
    wait_stats(par)
    g, s = gains(n_layers - 1)
    set_constants(par, g, s, count_a, True)
    prepare_corners(par, False)
    run_layer(lambda i, u: build_pairs(i, par, u, False, 1), conv_down, lambda i: start_edges(i, 1 - par, half))
    start_stats(1 - par)
    start_corners(1 - par)

    weights_wide()
    wait_edges(1 - par, half)
    wait_stats(1 - par)
    set_constants(1 - par, bn_down[0:1, :], bn_down[1:2, :], count_b, False)
    prepare_corners(1 - par, False)
    run_layer(lambda i, u: build_wide(i, 1 - par, u), conv_wide, lambda i: z_copy(i).start())
    start_stats(par)
    wait_stats(par)
    set_constants(par, bn_b[0, 0:1, :], bn_b[0, 1:2, :], count_b, False)
    cst_out[...] = cst[...]
    for img in range(n_img):
        z_copy(img).wait()


def finish_kernel(z_ref, cst_ref, out_ref, z, y, in_sem, out_sem):
    n_img, n_rows = z.shape[:2]

    def fetch(img):
        return pltpu.make_async_copy(z_ref.at[img], z.at[img], in_sem.at[img])

    def copy(img):
        return pltpu.make_async_copy(y.at[img], out_ref.at[img], out_sem.at[img])

    for img in range(n_img):
        fetch(img).start()

    def step(img, carry):
        fetch(img).wait()
        for r in range(n_rows):
            y[img, r] = normalise(z[img, r], cst_ref).astype(BF16)
        copy(img).start()
        return carry

    lax.fori_loop(0, n_img, step, 0)
    for img in range(n_img):
        copy(img).wait()


def solution(mesh):
    n_sp, n_sp2 = mesh.shape["sp"], mesh.shape["sp2"]

    def per_device(x, w_a, bn_a, w_down, bn_down, w_b, bn_b):
        n_img, rows, cols, ch = x.shape
        pairs, half = cols // 2, rows // 2
        n_dev = n_sp * n_sp2
        dims = (n_img, rows, pairs, ch, n_sp2, n_sp)
        vmem = pltpu.VMEM
        dma = pltpu.SemaphoreType.DMA
        scratch = [
            vmem((n_img, rows, ch, cols), BF16),
            vmem(w_a.shape, BF16), vmem(w_down.shape, BF16), vmem(w_b.shape, BF16),
            vmem((n_img, rows, pairs, 128), F32),
            [vmem((4 * (half + 1), pairs, 128), BF16) for _ in range(UNROLL)],
            [vmem(((rows + 2) * (pairs + 2 * EDGE), 128), F32) for _ in range(UNROLL)],
            vmem((2, 1536, 128), BF16),
            vmem((128, 128), BF16),
            vmem((n_img, pairs, 128), BF16), vmem((n_img, pairs, 128), BF16),
            vmem((n_img, pairs, 128), BF16), vmem((n_img, pairs, 128), BF16),
            vmem((n_img, rows, 128), F32),
            vmem((n_img, rows, 128), F32),
            vmem((2, n_img, pairs, 128), F32),
            vmem((2, n_img, pairs, 128), F32),
            vmem((2, n_img, rows, 128), F32),
            vmem((2, n_img, rows, 128), F32),
            vmem((4, n_img, 128), F32),
            vmem((2, 4, n_img, 128), F32),
            vmem((4, n_img, 128), F32),
            vmem((2, n_dev, 2, 128), F32),
            vmem((2, 8, 256), F32),
            vmem((8, 128), F32),
            dma((n_img,)),
            dma((3,)),
            dma((n_img,)),
            dma((2,)), dma((2, 2)),
            dma((2,)), dma((2, 2)),
            dma((4,)), dma((2, 4)),
            dma((n_dev - 1,)), dma((2, n_dev)),
        ]
        in_vmem = pl.BlockSpec(memory_space=pltpu.VMEM)
        in_hbm = pl.BlockSpec(memory_space=pltpu.HBM)
        in_any = pl.BlockSpec(memory_space=pl.ANY)
        z, cst = pl.pallas_call(
            functools.partial(stack_kernel, dims),
            out_shape=(jax.ShapeDtypeStruct((n_img, half, pairs, 128), F32), jax.ShapeDtypeStruct((8, 128), F32)),
            in_specs=[in_hbm, in_hbm, in_vmem, in_hbm, in_vmem, in_hbm, in_vmem],
            out_specs=(in_any, in_vmem),
            scratch_shapes=scratch,
            compiler_params=pltpu.CompilerParams(collective_id=0, has_side_effects=True, vmem_limit_bytes=VMEM_LIMIT),
        )(jnp.transpose(x, (0, 1, 3, 2)), w_a, bn_a, w_down, bn_down, w_b, bn_b)
        return pl.pallas_call(
            finish_kernel,
            out_shape=jax.ShapeDtypeStruct((n_img, half, pairs, 128), BF16),
            in_specs=[in_any, in_vmem],
            out_specs=in_any,
            scratch_shapes=[vmem((n_img, half, pairs, 128), F32), vmem((n_img, half, pairs, 128), BF16), dma((n_img,)), dma((n_img,))],
            compiler_params=pltpu.CompilerParams(vmem_limit_bytes=VMEM_LIMIT),
        )(z, cst)

    tile_spec = P("dp", "sp", "sp2", None)
    return jax.shard_map(per_device, mesh=mesh, in_specs=(tile_spec, P(), P(), P(), P(), P(), P()), out_specs=tile_spec, check_vma=False)
```

```python
import functools

import jax
import jax.numpy as jnp
from jax import lax
from jax.experimental import pallas as pl
from jax.experimental.pallas import tpu as pltpu
from jax.sharding import PartitionSpec as P

MESH = pl.DeviceIdType.MESH
F32 = jnp.float32
BF16 = jnp.bfloat16
EPS = 1e-5
UNROLL = 4
VMEM_LIMIT = 56 * 1024 * 1024
EDGE = 8


def normalise(v, cst):
    return jnp.maximum((v - cst[0:1, :]) * cst[1:2, :] + cst[2:3, :], 0.0)


def stack_kernel(dims, x_ref, w_a_ref, bn_a, w_down_ref, bn_down, w_b_ref, bn_b, z_out, cst_out,
                 xv, w_a, w_down, w_b, z, bufs, lines, wmat, perm, edge_u, edge_d, halo_u, halo_d,
                 mid_s, mid_r, end_s, end_r, corner_s, corner_r, corner_n, stats, acc, cst,
                 x_sem, w_sem, z_sem, row_send, row_recv, mid_send, mid_recv, end_send, end_recv, cor_send, cor_recv, st_send, st_recv):
    n_img, rows, pairs, ch, n_sp2, n_sp = dims
    half, quarter = rows // 2, rows // 4
    wide = pairs + 2 * EDGE
    n_dev = n_sp2 * n_sp
    n_steps = n_img // UNROLL
    sp = lax.axis_index("sp")
    sp2 = lax.axis_index("sp2")
    me = sp2 * n_sp + sp
    has_u, has_d = sp > 0, sp < n_sp - 1
    has_l, has_r = sp2 > 0, sp2 < n_sp2 - 1

    def x_copy(img):
        return pltpu.make_async_copy(x_ref.at[img], xv.at[img], x_sem.at[img])

    for img in range(n_img):
        x_copy(img).start()
    w_copies = [pltpu.make_async_copy(src, dst, w_sem.at[i]) for i, (src, dst) in enumerate(((w_a_ref, w_a), (w_down_ref, w_down), (w_b_ref, w_b)))]
    for copy in w_copies:
        copy.start()

    barrier = pltpu.get_barrier_semaphore()
    for d in range(1, n_dev):
        peer = lax.rem(me + d, n_dev)
        pl.semaphore_signal(barrier, inc=1, device_id={"sp2": peer // n_sp, "sp": lax.rem(peer, n_sp)}, device_id_type=MESH)

    def rcopy(src, dst, ssem, rsem, to_sp2, to_sp):
        return pltpu.make_async_remote_copy(src_ref=src, dst_ref=dst, send_sem=ssem, recv_sem=rsem,
                                            device_id={"sp2": to_sp2, "sp": to_sp}, device_id_type=MESH)

    def batch(t):
        return pl.ds(t * UNROLL, UNROLL)

    def start_rows(t):
        some = batch(t)

        @pl.when(has_u)
        def _():
            rcopy(edge_u.at[some], halo_d.at[some], row_send.at[0], row_recv.at[1], sp2, sp - 1).start()

        @pl.when(has_d)
        def _():
            rcopy(edge_d.at[some], halo_u.at[some], row_send.at[1], row_recv.at[0], sp2, sp + 1).start()

    def wait_rows():
        @pl.when(has_u)
        def _():
            rcopy(edge_u, halo_u, row_send.at[0], row_recv.at[0], sp2, sp).wait()

        @pl.when(has_d)
        def _():
            rcopy(edge_d, halo_d, row_send.at[1], row_recv.at[1], sp2, sp).wait()

    def start_columns(src, dst, ssem, rsem, t, par):
        some = batch(t)

        @pl.when(has_l)
        def _():
            rcopy(src.at[par, 0, some], dst.at[par, 1, some], ssem.at[par, 0], rsem.at[par, 1, t], sp2 - 1, sp).start()

        @pl.when(has_r)
        def _():
            rcopy(src.at[par, 1, some], dst.at[par, 0, some], ssem.at[par, 1], rsem.at[par, 0, t], sp2 + 1, sp).start()

    def wait_columns(t, par):
        some = batch(t)
        for side, there in ((0, has_l), (1, has_r)):
            @pl.when(there)
            def _():
                rcopy(mid_s.at[par, side, some], mid_r.at[par, side, some], mid_send.at[par, side], mid_recv.at[par, side, t], sp2, sp).wait_recv()
                rcopy(end_s.at[par, side, some], end_r.at[par, side, some], end_send.at[par, side], end_recv.at[par, side, t], sp2, sp).wait_recv()

    def wait_columns_sent(par):
        for side, there in ((0, has_l), (1, has_r)):
            @pl.when(there)
            def _():
                rcopy(mid_s.at[par, side], mid_r.at[par, side], mid_send.at[par, side], mid_recv.at[par, side, 0], sp2, sp).wait_send()
                rcopy(end_s.at[par, side], end_r.at[par, side], end_send.at[par, side], end_recv.at[par, side, 0], sp2, sp).wait_send()

    corner_to = ((has_u & has_l, -1, -1, 3), (has_u & has_r, 1, -1, 2), (has_d & has_l, -1, 1, 1), (has_d & has_r, 1, 1, 0))

    def start_corners(par):
        for c, (there, d_sp2, d_sp, slot) in enumerate(corner_to):
            @pl.when(there)
            def _():
                rcopy(corner_s.at[c], corner_r.at[par, slot], cor_send.at[c], cor_recv.at[par, slot], sp2 + d_sp2, sp + d_sp).start()

    def wait_corners(par):
        for c, (there, d_sp2, d_sp, slot) in enumerate(corner_to):
            @pl.when(there)
            def _():
                rcopy(corner_s.at[c], corner_r.at[par, c], cor_send.at[c], cor_recv.at[par, c], sp2, sp).wait()

    def stat_copy(d, par):
        peer = lax.rem(me + d, n_dev)
        return rcopy(stats.at[par, me], stats.at[par, me], st_send.at[d - 1], st_recv.at[par, me], peer // n_sp, lax.rem(peer, n_sp))

    def start_stats(par):
        total = acc[0] + acc[1]
        stats[par, me] = jnp.concatenate([jnp.sum(total[:, :128], axis=0, keepdims=True), jnp.sum(total[:, 128:], axis=0, keepdims=True)], axis=0)
        for d in range(1, n_dev):
            stat_copy(d, par).start()

    def wait_stats(par):
        for d in range(1, n_dev):
            stat_copy(d, par).wait_send()
            src = lax.rem(me + d, n_dev)
            rcopy(stats.at[par, src], stats.at[par, src], st_send.at[d - 1], st_recv.at[par, src], sp2, sp).wait_recv()

    def set_constants(par, gain, shift, count, paired):
        total = stats[par, 0]
        for src in range(1, n_dev):
            total = total + stats[par, src]
        if paired:
            total = total + pltpu.roll(total, ch, 1)
        mean = total[0:1] * (1.0 / count)
        var = total[1:2] * (1.0 / count) - mean * mean
        cst[0:1, :] = mean
        cst[1:2, :] = gain * lax.rsqrt(var + EPS)
        cst[2:3, :] = shift

    lane = lax.broadcasted_iota(jnp.int32, (pairs, 128), 1)

    def act(v, raw):
        return v if raw else normalise(v, cst)

    def column(img, side, first, count):
        flat = z.at[img].reshape(rows * pairs, 128)
        return flat[pl.ds(first * pairs + side * (pairs - 1), count, stride=pairs), :]

    def save_mid(img, n_rows, par):
        for side in range(2):
            mid_s[par, side, img, 0:n_rows - 4, :] = column(img, side, 2, n_rows - 4)

    def save_end(img, n_rows, par):
        here = pl.ds(img, 1)
        for side in range(2):
            top, bottom = column(img, side, 0, 2), column(img, side, n_rows - 2, 2)
            end_s[par, side, img, 0:2, :] = top
            end_s[par, side, img, 2:4, :] = bottom
            corner_s[side, here, :] = top[0:1]
            corner_s[2 + side, here, :] = bottom[1:2]

    def prepare_corners(par, raw):
        for c, (there, d_sp2, d_sp, slot) in enumerate(corner_to):
            corner_n[c] = jnp.where(there, act(corner_r[par, c], raw), 0.0)

    def line_place(p):
        return p * wide + EDGE

    def inner_lines(img, par, u, n_rows, raw):
        buf = lines[u]
        for side, there, off in ((0, has_l, -1), (1, has_r, pairs)):
            for src, at, count, r in ((end_r, 0, 2, 0), (mid_r, 0, n_rows - 4, 2), (end_r, 2, 2, n_rows - 2)):
                v = jnp.where(there, act(src[par, side, img, at:at + count, :], raw), 0.0)
                buf[pl.ds(line_place(r + 1) + off, count, stride=wide), :] = v
        for p in range(1, n_rows + 1):
            v = act(z[img, p - 1], raw)
            buf[line_place(p):line_place(p) + pairs, :] = v
            yield p, v

    def outer_lines(img, u, n_rows, which):
        buf = lines[u]
        here = pl.ds(img, 1)
        for side in which:
            p = side * (n_rows + 1)
            v = jnp.where((has_u, has_d)[side], (halo_u, halo_d)[side][img].astype(F32), 0.0)
            at = line_place(p)
            buf[at - 1:at, :] = corner_n[2 * side, here, :]
            buf[at + pairs:at + pairs + 1, :] = corner_n[2 * side + 1, here, :]
            buf[at:at + pairs, :] = v
            yield p, v

    def put_pairs(t, u, p, own):
        n_q, at = half + 1, line_place(p)
        side = jnp.where(lane < ch, lines[u][at + 1:at + 1 + pairs, :], lines[u][at - 1:at - 1 + pairs, :])
        bufs[u][t, 2 * (p % 2) * n_q + p // 2] = own.astype(BF16)
        bufs[u][t, (2 * (p % 2) + 1) * n_q + p // 2] = side.astype(BF16)

    def put_wide(t, u, p, own):
        n_q, at = quarter + 1, line_place(p)
        slot = 3 * (p % 2) * n_q + p // 2
        bufs[u][t, slot] = lines[u][at - 1:at - 1 + pairs, :].astype(BF16)
        bufs[u][t, slot + n_q] = own.astype(BF16)
        bufs[u][t, slot + 2 * n_q] = lines[u][at + 1:at + 1 + pairs, :].astype(BF16)

    def slots_pairs(i):
        return [c * (half + 1) + i + lo for lo in (0, 1) for c in range(4)]

    def slots_down(i):
        return [c * (half + 1) + 2 * i + k for k, c in ((0, 2), (0, 3), (1, 0), (1, 1), (1, 2), (1, 3), (2, 0), (2, 1), (2, 2), (2, 3))]

    def slots_wide(i):
        return [c * (quarter + 1) + i + lo for lo in (0, 1) for c in range(6)]

    def conv(t, blocks, slots):
        lhs = jnp.concatenate([jnp.concatenate([bufs[u][t, slots(i)[k]] for u, i in blocks], axis=0) for k in range(len(slots(0)))], axis=1)
        rhs = jnp.concatenate([wmat[0, 0:lhs.shape[1]], wmat[1, 0:lhs.shape[1]]], axis=1)
        o = jnp.dot(lhs, rhs, preferred_element_type=F32)
        folded = o.reshape(o.shape[0] // 8, 8, 256)
        s = jnp.sum(folded, axis=0)
        q = jnp.sum(folded * folded, axis=0)
        acc[0] += jnp.concatenate([s[:, :128], q[:, :128]], axis=1)
        acc[1] += jnp.concatenate([s[:, 128:], q[:, 128:]], axis=1)
        for n, (u, i) in enumerate(blocks):
            z[t * UNROLL + u, 2 * i] = o[n * pairs:(n + 1) * pairs, :128]
            z[t * UNROLL + u, 2 * i + 1] = o[n * pairs:(n + 1) * pairs, 128:]

    def run_layer(par, raw, n_rows, put, slots, inner, outer, sides, join, n_out, par_out):
        acc[...] = jnp.zeros_like(acc)
        if not raw:
            def send_rows(t, carry):
                for u in range(UNROLL):
                    img = t * UNROLL + u
                    edge_u[img] = act(z[img, 0], raw).astype(BF16)
                    edge_d[img] = act(z[img, n_rows - 1], raw).astype(BF16)
                start_rows(t)
                return carry

            lax.fori_loop(0, n_steps, send_rows, 0)

        def groups(size):
            return [range(u, u + size) for u in range(0, UNROLL, size)]

        def first_pass(t, carry):
            wait_columns(t, par)
            for us in groups(join[0]):
                for u in us:
                    for p, own in inner_lines(t * UNROLL + u, par, u, n_rows, raw):
                        put(t, u, p, own)
                conv(t, [(u, i) for u in us for i in inner], slots)
            if n_out:
                for u in range(UNROLL):
                    save_mid(t * UNROLL + u, n_out, par_out)
                start_columns(mid_s, mid_r, mid_send, mid_recv, t, par_out)
            return carry

        lax.fori_loop(0, n_steps, first_pass, 0)
        wait_corners(par)
        prepare_corners(par, raw)
        wait_rows()

        def second_pass(t, carry):
            for us in groups(join[1]):
                for u in us:
                    for p, own in outer_lines(t * UNROLL + u, u, n_rows, sides):
                        put(t, u, p, own)
                conv(t, [(u, i) for u in us for i in outer], slots)
            if n_out:
                for u in range(UNROLL):
                    save_end(t * UNROLL + u, n_out, par_out)
                start_columns(end_s, end_r, end_send, end_recv, t, par_out)
            else:
                for u in range(UNROLL):
                    z_copy(t * UNROLL + u).start()
            return carry

        lax.fori_loop(0, n_steps, second_pass, 0)
        start_stats(par_out)
        if n_out:
            start_corners(par_out)

    def z_copy(img):
        return pltpu.make_async_copy(z.at[img, pl.ds(0, half)], z_out.at[img], z_sem.at[img])

    def put_block(k, n_k, blocks):
        for o, blk in enumerate(blocks):
            wmat[o, k * n_k:(k + 1) * n_k, :] = jnp.zeros((n_k, 128), BF16) if blk is None else blk

    def weights_pairs(layer):
        zero = jnp.zeros((ch, ch), BF16)
        q = []
        for kh in range(3):
            w0, w1, w2 = w_a[layer, kh, 0], w_a[layer, kh, 1], w_a[layer, kh, 2]
            q.append(jnp.concatenate([
                jnp.concatenate([w1, w0], axis=1),
                jnp.concatenate([w2, w1], axis=1),
                jnp.concatenate([zero, w2], axis=1),
                jnp.concatenate([w0, zero], axis=1)], axis=0))
        for k in range(4):
            put_block(k, 256, [q[k] if k < 3 else None, q[k - 1] if k > 0 else None])

    def weights_down():
        d = [jnp.concatenate([w_down[kh, 0], w_down[kh, 1], w_down[kh, 2], jnp.zeros((ch, 128), BF16)], axis=0) for kh in range(3)]
        for k in range(5):
            put_block(k, 256, [d[k] if k < 3 else None, d[k - 2] if k >= 2 else None])

    def weights_wide():
        e = [jnp.concatenate([w_b[0, kh, 0], w_b[0, kh, 1], w_b[0, kh, 2]], axis=0) for kh in range(3)]
        for k in range(4):
            put_block(k, 384, [e[k] if k < 3 else None, e[k - 1] if k > 0 else None])

    wrow = lax.broadcasted_iota(jnp.int32, (128, 128), 0)
    wcol = lax.broadcasted_iota(jnp.int32, (128, 128), 1)
    source = jnp.where(wrow < pairs, 2 * wrow, 2 * (wrow - pairs) + 1)
    perm[...] = jnp.where(source == wcol, 1.0, 0.0).astype(BF16)

    def load_images(t, carry):
        images = [t * UNROLL + u for u in range(UNROLL)]
        for img in images:
            x_copy(img).wait()
        for img in images:
            for g in range(rows // 4):
                block = xv[img, 4 * g:4 * g + 4].reshape(4 * ch, 128)
                m = lax.dot_general(perm[...], block, (((1,), (1,)), ((), ())), preferred_element_type=F32)
                for b in range(2):
                    even = m[0:pairs, 128 * b:128 * b + 128]
                    odd = m[pairs:2 * pairs, 128 * b:128 * b + 128]
                    r = 4 * g + 2 * b
                    upper = jnp.where(lane < ch, even, pltpu.roll(odd, ch, 1))
                    lower = jnp.where(lane < ch, pltpu.roll(even, ch, 1), odd)
                    z[img, r] = upper
                    z[img, r + 1] = lower
                    if r == 0:
                        edge_u[img] = upper.astype(BF16)
                    if r + 2 == rows:
                        edge_d[img] = lower.astype(BF16)
            save_mid(img, rows, 0)
            save_end(img, rows, 0)

        @pl.when(t == 0)
        def _():
            pl.semaphore_wait(barrier, n_dev - 1)

        start_columns(mid_s, mid_r, mid_send, mid_recv, t, 0)
        start_columns(end_s, end_r, end_send, end_recv, t, 0)
        start_rows(t)
        return carry

    lax.fori_loop(0, n_steps, load_images, 0)
    start_corners(0)

    count_a = float(n_dev * n_img * rows * pairs * 2)
    count_b = float(n_dev * n_img * half * pairs)
    a_inner, a_outer = range(1, half - 1), (0, half - 1)

    for copy in w_copies:
        copy.wait()
    weights_pairs(0)
    run_layer(0, True, rows, put_pairs, slots_pairs, a_inner, a_outer, (0, 1), (1, 2), rows, 1)

    def gains(layer):
        g, s = bn_a[layer, 0:1, :], bn_a[layer, 1:2, :]
        return jnp.concatenate([g, g], axis=1), jnp.concatenate([s, s], axis=1)

    n_layers = w_a.shape[0]

    def a_layer(layer, carry):
        par = lax.rem(layer, 2)
        weights_pairs(layer)
        wait_columns_sent(1 - par)
        wait_stats(par)
        g, s = gains(layer - 1)
        set_constants(par, g, s, count_a, True)
        run_layer(par, False, rows, put_pairs, slots_pairs, a_inner, a_outer, (0, 1), (1, 2), rows, 1 - par)
        return carry

    lax.fori_loop(1, n_layers, a_layer, 0)

    par = n_layers % 2
    weights_down()
    wait_columns_sent(1 - par)
    wait_stats(par)
    g, s = gains(n_layers - 1)
    set_constants(par, g, s, count_a, True)
    run_layer(par, False, rows, put_pairs, slots_down, range(quarter - 1), (quarter - 1,), (1,), (1, 2), half, 1 - par)

    weights_wide()
    wait_columns_sent(par)
    wait_columns_sent(1 - par)
    wait_stats(1 - par)
    set_constants(1 - par, bn_down[0:1, :], bn_down[1:2, :], count_b, False)
    run_layer(1 - par, False, half, put_wide, slots_wide, range(1, quarter - 1), (0, quarter - 1), (0, 1), (2, 2), 0, par)
    wait_stats(par)
    set_constants(par, bn_b[0, 0:1, :], bn_b[0, 1:2, :], count_b, False)
    cst_out[...] = cst[...]
    for img in range(n_img):
        z_copy(img).wait()


def finish_kernel(z_ref, cst_ref, out_ref, z, y, in_sem, out_sem):
    n_img, n_rows = z.shape[:2]

    def fetch(img):
        return pltpu.make_async_copy(z_ref.at[img], z.at[img], in_sem.at[img])

    def copy(img):
        return pltpu.make_async_copy(y.at[img], out_ref.at[img], out_sem.at[img])

    for img in range(n_img):
        fetch(img).start()

    def step(img, carry):
        fetch(img).wait()
        for r in range(n_rows):
            y[img, r] = normalise(z[img, r], cst_ref).astype(BF16)
        copy(img).start()
        return carry

    lax.fori_loop(0, n_img, step, 0)
    for img in range(n_img):
        copy(img).wait()


def solution(mesh):
    n_sp, n_sp2 = mesh.shape["sp"], mesh.shape["sp2"]

    def per_device(x, w_a, bn_a, w_down, bn_down, w_b, bn_b):
        n_img, rows, cols, ch = x.shape
        pairs, half = cols // 2, rows // 2
        n_dev = n_sp * n_sp2
        dims = (n_img, rows, pairs, ch, n_sp2, n_sp)
        vmem = pltpu.VMEM
        dma = pltpu.SemaphoreType.DMA
        scratch = [
            vmem((n_img, rows, ch, cols), BF16),
            vmem(w_a.shape, BF16), vmem(w_down.shape, BF16), vmem(w_b.shape, BF16),
            vmem((n_img, rows, pairs, 128), F32),
            [vmem((n_img // UNROLL, 4 * (half + 1), pairs, 128), BF16) for _ in range(UNROLL)],
            [vmem(((rows + 2) * (pairs + 2 * EDGE), 128), F32) for _ in range(UNROLL)],
            vmem((2, 1536, 128), BF16),
            vmem((128, 128), BF16),
            vmem((n_img, pairs, 128), BF16), vmem((n_img, pairs, 128), BF16),
            vmem((n_img, pairs, 128), BF16), vmem((n_img, pairs, 128), BF16),
            vmem((2, 2, n_img, rows - 4, 128), F32), vmem((2, 2, n_img, rows - 4, 128), F32),
            vmem((2, 2, n_img, 4, 128), F32), vmem((2, 2, n_img, 4, 128), F32),
            vmem((4, n_img, 128), F32),
            vmem((2, 4, n_img, 128), F32),
            vmem((4, n_img, 128), F32),
            vmem((2, n_dev, 2, 128), F32),
            vmem((2, 8, 256), F32),
            vmem((8, 128), F32),
            dma((n_img,)),
            dma((3,)),
            dma((n_img,)),
            dma((2,)), dma((2,)),
            dma((2, 2)), dma((2, 2, n_img // UNROLL)),
            dma((2, 2)), dma((2, 2, n_img // UNROLL)),
            dma((4,)), dma((2, 4)),
            dma((n_dev - 1,)), dma((2, n_dev)),
        ]
        in_vmem = pl.BlockSpec(memory_space=pltpu.VMEM)
        in_hbm = pl.BlockSpec(memory_space=pltpu.HBM)
        in_any = pl.BlockSpec(memory_space=pl.ANY)
        z, cst = pl.pallas_call(
            functools.partial(stack_kernel, dims),
            out_shape=(jax.ShapeDtypeStruct((n_img, half, pairs, 128), F32), jax.ShapeDtypeStruct((8, 128), F32)),
            in_specs=[in_hbm, in_hbm, in_vmem, in_hbm, in_vmem, in_hbm, in_vmem],
            out_specs=(in_any, in_vmem),
            scratch_shapes=scratch,
            compiler_params=pltpu.CompilerParams(collective_id=0, has_side_effects=True, vmem_limit_bytes=VMEM_LIMIT),
        )(jnp.transpose(x, (0, 1, 3, 2)), w_a, bn_a, w_down, bn_down, w_b, bn_b)
        return pl.pallas_call(
            finish_kernel,
            out_shape=jax.ShapeDtypeStruct((n_img, half, pairs, 128), BF16),
            in_specs=[in_any, in_vmem],
            out_specs=in_any,
            scratch_shapes=[vmem((n_img, half, pairs, 128), F32), vmem((n_img, half, pairs, 128), BF16), dma((n_img,)), dma((n_img,))],
            compiler_params=pltpu.CompilerParams(vmem_limit_bytes=VMEM_LIMIT),
        )(z, cst)

    tile_spec = P("dp", "sp", "sp2", None)
    return jax.shard_map(per_device, mesh=mesh, in_specs=(tile_spec, P(), P(), P(), P(), P(), P()), out_specs=tile_spec, check_vma=False)
```

```python
import functools

import jax
import jax.numpy as jnp
from jax import lax
from jax.experimental import pallas as pl
from jax.experimental.pallas import tpu as pltpu
from jax.sharding import PartitionSpec as P

MESH = pl.DeviceIdType.MESH
F32 = jnp.float32
BF16 = jnp.bfloat16
EPS = 1e-5
UNROLL = 4
SPLIT = 1
VMEM_LIMIT = 51 * 1024 * 1024
EDGE = 8


def normalise(v, cst):
    return jnp.maximum((v - cst[0:1, :]) * cst[1:2, :] + cst[2:3, :], 0.0)


def stack_kernel(dims, x_ref, w_a_ref, bn_a, w_down_ref, bn_down, w_b_ref, bn_b, z_out, cst_out,
                 xv, w_a, w_down, w_b, z, bufs, lines, wmat, perm, edge_u, edge_d, first_u, first_d, edge_l, edge_r, halo_u, halo_d, halo_l, halo_r,
                 corner_s, corner_r, corner_n, stats, acc, cst,
                 x_sem, w_sem, row_send, row_recv, col_send, col_recv, cor_send, cor_recv, st_send, st_recv):
    n_img, rows, pairs, ch, n_sp2, n_sp = dims
    half, quarter = rows // 2, rows // 4
    wide = pairs + 2 * EDGE
    n_dev = n_sp2 * n_sp
    sp = lax.axis_index("sp")
    sp2 = lax.axis_index("sp2")
    me = sp2 * n_sp + sp
    has_u, has_d = sp > 0, sp < n_sp - 1
    has_l, has_r = sp2 > 0, sp2 < n_sp2 - 1

    def x_copy(t):
        some = pl.ds(t * UNROLL, UNROLL)
        return pltpu.make_async_copy(x_ref.at[some], xv.at[some], x_sem.at[t])

    for t in range(n_img // UNROLL):
        x_copy(t).start()

    w_copies = [pltpu.make_async_copy(src, dst, w_sem.at[i]) for i, (src, dst) in enumerate(((w_a_ref, w_a), (w_down_ref, w_down), (w_b_ref, w_b)))]
    for copy in w_copies:
        copy.start()

    barrier = pltpu.get_barrier_semaphore()
    for d in range(1, n_dev):
        peer = lax.rem(me + d, n_dev)
        pl.semaphore_signal(barrier, inc=1, device_id={"sp2": peer // n_sp, "sp": lax.rem(peer, n_sp)}, device_id_type=MESH)

    def rcopy(src, dst, ssem, rsem, to_sp2, to_sp):
        return pltpu.make_async_remote_copy(src_ref=src, dst_ref=dst, send_sem=ssem, recv_sem=rsem,
                                            device_id={"sp2": to_sp2, "sp": to_sp}, device_id_type=MESH)

    def start_edges(t, par, n_rows, first=False):
        some, r_all = pl.ds(t * UNROLL, UNROLL), pl.ds(0, n_rows)

        @pl.when(has_u)
        def _():
            src, dst = (edge_u.at[some], first_d.at[some]) if first else (z.at[some, 0], halo_d.at[par, some])
            rcopy(src, dst, row_send.at[0], row_recv.at[par, 1], sp2, sp - 1).start()

        @pl.when(has_d)
        def _():
            src, dst = (edge_d.at[some], first_u.at[some]) if first else (z.at[some, n_rows - 1], halo_u.at[par, some])
            rcopy(src, dst, row_send.at[1], row_recv.at[par, 0], sp2, sp + 1).start()

        @pl.when(has_l)
        def _():
            rcopy(edge_l.at[some, r_all], halo_r.at[par, some, r_all], col_send.at[0], col_recv.at[par, 1], sp2 - 1, sp).start()

        @pl.when(has_r)
        def _():
            rcopy(edge_r.at[some, r_all], halo_l.at[par, some, r_all], col_send.at[1], col_recv.at[par, 0], sp2 + 1, sp).start()

    corner_to = ((has_u & has_l, -1, -1, 3), (has_u & has_r, 1, -1, 2), (has_d & has_l, -1, 1, 1), (has_d & has_r, 1, 1, 0))

    def start_corners(par):
        for c, (there, d_sp2, d_sp, slot) in enumerate(corner_to):
            @pl.when(there)
            def _():
                rcopy(corner_s.at[c], corner_r.at[par, slot], cor_send.at[c], cor_recv.at[par, slot], sp2 + d_sp2, sp + d_sp).start()

    def wait_edges(par, n_rows, first=False):
        r_all = pl.ds(0, n_rows)
        every = pl.ds(0, n_img)

        @pl.when(has_u)
        def _():
            src, dst = (edge_u, first_u) if first else (z.at[every, 0], halo_u.at[par])
            rcopy(src, dst, row_send.at[0], row_recv.at[par, 0], sp2, sp).wait()

        @pl.when(has_d)
        def _():
            src, dst = (edge_d, first_d) if first else (z.at[every, n_rows - 1], halo_d.at[par])
            rcopy(src, dst, row_send.at[1], row_recv.at[par, 1], sp2, sp).wait()

        @pl.when(has_l)
        def _():
            rcopy(edge_l.at[every, r_all], halo_l.at[par, every, r_all], col_send.at[0], col_recv.at[par, 0], sp2, sp).wait()

        @pl.when(has_r)
        def _():
            rcopy(edge_r.at[every, r_all], halo_r.at[par, every, r_all], col_send.at[1], col_recv.at[par, 1], sp2, sp).wait()

        for c, (there, d_sp2, d_sp, slot) in enumerate(corner_to):
            @pl.when(there)
            def _():
                rcopy(corner_s.at[c], corner_r.at[par, c], cor_send.at[c], cor_recv.at[par, c], sp2, sp).wait()

    def stat_copy(d, par):
        peer = lax.rem(me + d, n_dev)
        return rcopy(stats.at[par, me], stats.at[par, me], st_send.at[d - 1], st_recv.at[par, me], peer // n_sp, lax.rem(peer, n_sp))

    def start_stats(par):
        total = acc[0] + acc[1]
        stats[par, me] = jnp.concatenate([jnp.sum(total[:, :128], axis=0, keepdims=True), jnp.sum(total[:, 128:], axis=0, keepdims=True)], axis=0)
        for d in range(1, n_dev):
            stat_copy(d, par).start()

    def wait_stats(par):
        for d in range(1, n_dev):
            stat_copy(d, par).wait_send()
            src = lax.rem(me + d, n_dev)
            rcopy(stats.at[par, src], stats.at[par, src], st_send.at[d - 1], st_recv.at[par, src], sp2, sp).wait_recv()

    def set_constants(par, gain, shift, count, paired):
        total = stats[par, 0]
        for src in range(1, n_dev):
            total = total + stats[par, src]
        if paired:
            total = total + pltpu.roll(total, ch, 1)
        mean = total[0:1] * (1.0 / count)
        var = total[1:2] * (1.0 / count) - mean * mean
        cst[0:1, :] = mean
        cst[1:2, :] = gain * lax.rsqrt(var + EPS)
        cst[2:3, :] = shift

    lane = lax.broadcasted_iota(jnp.int32, (pairs, 128), 1)

    def save_edges(img, n_rows):
        flat = z.at[img].reshape(rows * pairs, 128)
        first = flat[pl.ds(0, n_rows, stride=pairs), :]
        final = flat[pl.ds(pairs - 1, n_rows, stride=pairs), :]
        edge_l[img, 0:n_rows, :] = first
        edge_r[img, 0:n_rows, :] = final
        here = pl.ds(img, 1)
        corner_s[0, here, :] = first[0:1]
        corner_s[1, here, :] = final[0:1]
        corner_s[2, here, :] = first[n_rows - 1:n_rows]
        corner_s[3, here, :] = final[n_rows - 1:n_rows]

    def act(v, raw):
        return v if raw else normalise(v, cst)

    def prepare_corners(par, raw):
        for c, (there, d_sp2, d_sp, slot) in enumerate(corner_to):
            corner_n[c] = jnp.where(there, act(corner_r[par, c], raw), 0.0)

    def fill_lines(img, par, u, n_rows, raw, first_p):
        buf = lines[u]
        left = jnp.where(has_l, act(halo_l[par, img, 0:n_rows, :], raw), 0.0)
        right = jnp.where(has_r, act(halo_r[par, img, 0:n_rows, :], raw), 0.0)
        buf[pl.ds(wide + EDGE - 1, n_rows, stride=wide), :] = left
        buf[pl.ds(wide + EDGE + pairs, n_rows, stride=wide), :] = right
        here = pl.ds(img, 1)
        bottom = (n_rows + 1) * wide
        buf[EDGE - 1:EDGE, :] = corner_n[0, here, :]
        buf[EDGE + pairs:EDGE + pairs + 1, :] = corner_n[1, here, :]
        buf[bottom + EDGE - 1:bottom + EDGE, :] = corner_n[2, here, :]
        buf[bottom + EDGE + pairs:bottom + EDGE + pairs + 1, :] = corner_n[3, here, :]
        out = []
        for p in range(first_p, n_rows + 2):
            if p == 0:
                v = jnp.where(has_u, first_u[img].astype(F32) if raw else act(halo_u[par, img], raw), 0.0)
            elif p == n_rows + 1:
                v = jnp.where(has_d, first_d[img].astype(F32) if raw else act(halo_d[par, img], raw), 0.0)
            else:
                v = act(z[img, p - 1], raw)
            base = p * wide + EDGE
            buf[base:base + pairs, :] = v
            out.append((p, base, v))
        return out

    def build_pairs(img, par, u, raw, first_p=0):
        n_q = half + 1
        for p, base, own in fill_lines(img, par, u, rows, raw, first_p):
            side = jnp.where(lane < ch, lines[u][base + 1:base + 1 + pairs, :], lines[u][base - 1:base - 1 + pairs, :])
            bufs[u][2 * (p % 2) * n_q + p // 2] = own.astype(BF16)
            bufs[u][(2 * (p % 2) + 1) * n_q + p // 2] = side.astype(BF16)

    def build_wide(img, par, u):
        n_q = quarter + 1
        for p, base, own in fill_lines(img, par, u, half, False, 0):
            at = 3 * (p % 2) * n_q + p // 2
            bufs[u][at] = lines[u][base - 1:base - 1 + pairs, :].astype(BF16)
            bufs[u][at + n_q] = own.astype(BF16)
            bufs[u][at + 2 * n_q] = lines[u][base + 1:base + 1 + pairs, :].astype(BF16)

    def finish_conv(img, i0, o, dst=z):
        folded = o.reshape(o.shape[0] // 8, 8, 256)
        s = jnp.sum(folded, axis=0)
        q = jnp.sum(folded * folded, axis=0)
        acc[0] += jnp.concatenate([s[:, :128], q[:, :128]], axis=1)
        acc[1] += jnp.concatenate([s[:, 128:], q[:, 128:]], axis=1)
        for i in range(o.shape[0] // pairs):
            dst[img, 2 * (i0 + i)] = o[i * pairs:(i + 1) * pairs, :128]
            dst[img, 2 * (i0 + i) + 1] = o[i * pairs:(i + 1) * pairs, 128:]

    def dot(parts):
        lhs = jnp.concatenate(parts, axis=1)
        rhs = jnp.concatenate([wmat[0, 0:lhs.shape[1]], wmat[1, 0:lhs.shape[1]]], axis=1)
        return jnp.dot(lhs, rhs, preferred_element_type=F32)

    def conv_pairs(img, u):
        n_q, n_i = half + 1, half // SPLIT
        for i0 in range(0, half, n_i):
            at = [c * n_q + i0 + lo for lo in (0, 1) for c in range(4)]
            finish_conv(img, i0, dot([bufs[u][k:k + n_i].reshape(n_i * pairs, 128) for k in at]))
        save_edges(img, rows)

    def conv_down(img, u):
        n_q = half + 1
        at = [c * n_q + k for k, c in ((0, 2), (0, 3), (1, 0), (1, 1), (1, 2), (1, 3), (2, 0), (2, 1), (2, 2), (2, 3))]
        finish_conv(img, 0, dot([jnp.concatenate([bufs[u][k + 2 * i] for i in range(quarter)], axis=0) for k in at]))
        save_edges(img, half)

    def conv_wide(img, u):
        n_q = quarter + 1
        at = [c * n_q + lo for lo in (0, 1) for c in range(6)]
        finish_conv(img, 0, dot([bufs[u][k:k + quarter].reshape(quarter * pairs, 128) for k in at]), z_out)

    def run_layer(build, conv, done):
        acc[...] = jnp.zeros_like(acc)

        def body(t, carry):
            for u in range(UNROLL):
                build(t * UNROLL + u, u)
                conv(t * UNROLL + u, u)
            done(t)
            return carry

        lax.fori_loop(0, n_img // UNROLL, body, 0)

    def put_block(k, n_k, blocks):
        for o, blk in enumerate(blocks):
            wmat[o, k * n_k:(k + 1) * n_k, :] = jnp.zeros((n_k, 128), BF16) if blk is None else blk

    def weights_pairs(layer):
        zero = jnp.zeros((ch, ch), BF16)
        q = []
        for kh in range(3):
            w0, w1, w2 = w_a[layer, kh, 0], w_a[layer, kh, 1], w_a[layer, kh, 2]
            q.append(jnp.concatenate([
                jnp.concatenate([w1, w0], axis=1),
                jnp.concatenate([w2, w1], axis=1),
                jnp.concatenate([zero, w2], axis=1),
                jnp.concatenate([w0, zero], axis=1)], axis=0))
        for k in range(4):
            put_block(k, 256, [q[k] if k < 3 else None, q[k - 1] if k > 0 else None])

    def weights_down():
        d = [jnp.concatenate([w_down[kh, 0], w_down[kh, 1], w_down[kh, 2], jnp.zeros((ch, 128), BF16)], axis=0) for kh in range(3)]
        for k in range(5):
            put_block(k, 256, [d[k] if k < 3 else None, d[k - 2] if k >= 2 else None])

    def weights_wide():
        e = [jnp.concatenate([w_b[0, kh, 0], w_b[0, kh, 1], w_b[0, kh, 2]], axis=0) for kh in range(3)]
        for k in range(4):
            put_block(k, 384, [e[k] if k < 3 else None, e[k - 1] if k > 0 else None])

    wrow = lax.broadcasted_iota(jnp.int32, (128, 128), 0)
    wcol = lax.broadcasted_iota(jnp.int32, (128, 128), 1)
    source = jnp.where(wrow < pairs, 2 * wrow, 2 * (wrow - pairs) + 1)
    perm[...] = jnp.where(source == wcol, 1.0, 0.0).astype(BF16)

    def load_images(t, carry):
        x_copy(t).wait()
        for img in [t * UNROLL + u for u in range(UNROLL)]:
            for g in range(rows // 4):
                block = xv[img, 4 * g:4 * g + 4].reshape(4 * ch, 128)
                m = lax.dot_general(perm[...], block, (((1,), (1,)), ((), ())), preferred_element_type=F32)
                for b in range(2):
                    even = m[0:pairs, 128 * b:128 * b + 128]
                    odd = m[pairs:2 * pairs, 128 * b:128 * b + 128]
                    r = 4 * g + 2 * b
                    upper = jnp.where(lane < ch, even, pltpu.roll(odd, ch, 1))
                    lower = jnp.where(lane < ch, pltpu.roll(even, ch, 1), odd)
                    z[img, r] = upper
                    z[img, r + 1] = lower
                    if r == 0:
                        edge_u[img] = upper.astype(BF16)
                    if r + 2 == rows:
                        edge_d[img] = lower.astype(BF16)
            save_edges(img, rows)

        @pl.when(t == 0)
        def _():
            pl.semaphore_wait(barrier, n_dev - 1)

        start_edges(t, 0, rows, True)
        return carry

    lax.fori_loop(0, n_img // UNROLL, load_images, 0)
    start_corners(0)

    count_a = float(n_dev * n_img * rows * pairs * 2)
    count_b = float(n_dev * n_img * half * pairs)

    for copy in w_copies:
        copy.wait()
    weights_pairs(0)
    wait_edges(0, rows, True)
    prepare_corners(0, True)
    run_layer(lambda i, u: build_pairs(i, 0, u, True), conv_pairs, lambda t: start_edges(t, 1, rows))
    start_stats(1)
    start_corners(1)

    def gains(layer):
        g, s = bn_a[layer, 0:1, :], bn_a[layer, 1:2, :]
        return jnp.concatenate([g, g], axis=1), jnp.concatenate([s, s], axis=1)

    n_layers = w_a.shape[0]

    def a_layer(layer, carry):
        par = lax.rem(layer, 2)
        weights_pairs(layer)
        wait_edges(par, rows)
        wait_stats(par)
        g, s = gains(layer - 1)
        set_constants(par, g, s, count_a, True)
        prepare_corners(par, False)
        run_layer(lambda i, u: build_pairs(i, par, u, False), conv_pairs, lambda t: start_edges(t, 1 - par, rows))
        start_stats(1 - par)
        start_corners(1 - par)
        return carry

    lax.fori_loop(1, n_layers, a_layer, 0)

    par = n_layers % 2
    weights_down()
    wait_edges(par, rows)
    wait_stats(par)
    g, s = gains(n_layers - 1)
    set_constants(par, g, s, count_a, True)
    prepare_corners(par, False)
    run_layer(lambda i, u: build_pairs(i, par, u, False, 1), conv_down, lambda t: start_edges(t, 1 - par, half))
    start_stats(1 - par)
    start_corners(1 - par)

    weights_wide()
    wait_edges(1 - par, half)
    wait_stats(1 - par)
    set_constants(1 - par, bn_down[0:1, :], bn_down[1:2, :], count_b, False)
    prepare_corners(1 - par, False)
    run_layer(lambda i, u: build_wide(i, 1 - par, u), conv_wide, lambda t: None)
    start_stats(par)
    wait_stats(par)
    set_constants(par, bn_b[0, 0:1, :], bn_b[0, 1:2, :], count_b, False)
    cst_out[...] = cst[...]


def finish_kernel(z, cst_ref, out_ref, y, out_sem):
    n_img, n_rows = z.shape[:2]

    def copy(img):
        return pltpu.make_async_copy(y.at[img], out_ref.at[img], out_sem.at[img])

    def step(img, carry):
        for r in range(n_rows):
            y[img, r] = normalise(z[img, r], cst_ref).astype(BF16)
        copy(img).start()
        return carry

    lax.fori_loop(0, n_img, step, 0)
    for img in range(n_img):
        copy(img).wait()


def solution(mesh):
    n_sp, n_sp2 = mesh.shape["sp"], mesh.shape["sp2"]

    def per_device(x, w_a, bn_a, w_down, bn_down, w_b, bn_b):
        n_img, rows, cols, ch = x.shape
        pairs, half = cols // 2, rows // 2
        n_dev = n_sp * n_sp2
        dims = (n_img, rows, pairs, ch, n_sp2, n_sp)
        vmem = pltpu.VMEM
        dma = pltpu.SemaphoreType.DMA
        scratch = [
            vmem((n_img, rows, ch, cols), BF16),
            vmem(w_a.shape, BF16), vmem(w_down.shape, BF16), vmem(w_b.shape, BF16),
            vmem((n_img, rows, pairs, 128), F32),
            [vmem((4 * (half + 1), pairs, 128), BF16) for _ in range(UNROLL)],
            [vmem(((rows + 2) * (pairs + 2 * EDGE), 128), F32) for _ in range(UNROLL)],
            vmem((2, 1536, 128), BF16),
            vmem((128, 128), BF16),
            vmem((n_img, pairs, 128), BF16), vmem((n_img, pairs, 128), BF16),
            vmem((n_img, pairs, 128), BF16), vmem((n_img, pairs, 128), BF16),
            vmem((n_img, rows, 128), F32),
            vmem((n_img, rows, 128), F32),
            vmem((2, n_img, pairs, 128), F32),
            vmem((2, n_img, pairs, 128), F32),
            vmem((2, n_img, rows, 128), F32),
            vmem((2, n_img, rows, 128), F32),
            vmem((4, n_img, 128), F32),
            vmem((2, 4, n_img, 128), F32),
            vmem((4, n_img, 128), F32),
            vmem((2, n_dev, 2, 128), F32),
            vmem((2, 8, 256), F32),
            vmem((8, 128), F32),
            dma((n_img // UNROLL,)),
            dma((3,)),
            dma((2,)), dma((2, 2)),
            dma((2,)), dma((2, 2)),
            dma((4,)), dma((2, 4)),
            dma((n_dev - 1,)), dma((2, n_dev)),
        ]
        in_vmem = pl.BlockSpec(memory_space=pltpu.VMEM)
        in_hbm = pl.BlockSpec(memory_space=pltpu.HBM)
        in_any = pl.BlockSpec(memory_space=pl.ANY)
        z, cst = pl.pallas_call(
            functools.partial(stack_kernel, dims),
            out_shape=(vmem((n_img, half, pairs, 128), F32), jax.ShapeDtypeStruct((8, 128), F32)),
            in_specs=[in_hbm, in_hbm, in_vmem, in_hbm, in_vmem, in_hbm, in_vmem],
            out_specs=(in_vmem, in_vmem),
            scratch_shapes=scratch,
            compiler_params=pltpu.CompilerParams(collective_id=0, has_side_effects=True, vmem_limit_bytes=VMEM_LIMIT),
        )(jnp.transpose(x, (0, 1, 3, 2)), w_a, bn_a, w_down, bn_down, w_b, bn_b)
        return pl.pallas_call(
            finish_kernel,
            out_shape=jax.ShapeDtypeStruct((n_img, half, pairs, 128), BF16),
            in_specs=[in_vmem, in_vmem],
            out_specs=in_any,
            scratch_shapes=[vmem((n_img, half, pairs, 128), BF16), dma((n_img,))],
            compiler_params=pltpu.CompilerParams(vmem_limit_bytes=16 * 1024 * 1024),
        )(z, cst)

    tile_spec = P("dp", "sp", "sp2", None)
    return jax.shard_map(per_device, mesh=mesh, in_specs=(tile_spec, P(), P(), P(), P(), P(), P()), out_specs=tile_spec, check_vma=False)
```

```python
import functools

import jax
import jax.numpy as jnp
from jax import lax
from jax.experimental import pallas as pl
from jax.experimental.pallas import tpu as pltpu
from jax.sharding import PartitionSpec as P

MESH = pl.DeviceIdType.MESH
F32 = jnp.float32
BF16 = jnp.bfloat16
EPS = 1e-5
UNROLL = 4
SPLIT = 1
VMEM_LIMIT = 51 * 1024 * 1024
EDGE = 8


def normalise(v, cst):
    return jnp.maximum((v - cst[0:1, :]) * cst[1:2, :] + cst[2:3, :], 0.0)


def stack_kernel(dims, x_ref, w_a_ref, bn_a, w_down_ref, bn_down, w_b_ref, bn_b, z_out, cst_out,
                 xv, w_a, w_down, w_b, z, bufs, lines, wmat, perm, edge_u, edge_d, first_u, first_d, edge_l, edge_r, halo_u, halo_d, halo_l, halo_r,
                 corner_s, corner_r, corner_n, stats, acc, cst,
                 x_sem, w_sem, row_send, row_recv, col_send, col_recv, cor_send, cor_recv, st_send, st_recv):
    n_img, rows, pairs, ch, n_sp2, n_sp = dims
    half, quarter = rows // 2, rows // 4
    wide = pairs + 2 * EDGE
    n_dev = n_sp2 * n_sp
    sp = lax.axis_index("sp")
    sp2 = lax.axis_index("sp2")
    me = sp2 * n_sp + sp
    has_u, has_d = sp > 0, sp < n_sp - 1
    has_l, has_r = sp2 > 0, sp2 < n_sp2 - 1

    def x_copy(t):
        some = pl.ds(t * UNROLL, UNROLL)
        return pltpu.make_async_copy(x_ref.at[some], xv.at[some], x_sem.at[t])

    for t in range(n_img // UNROLL):
        x_copy(t).start()

    w_copies = [pltpu.make_async_copy(src, dst, w_sem.at[i]) for i, (src, dst) in enumerate(((w_a_ref, w_a), (w_down_ref, w_down), (w_b_ref, w_b)))]
    for copy in w_copies:
        copy.start()

    barrier = pltpu.get_barrier_semaphore()
    for d in range(1, n_dev):
        peer = lax.rem(me + d, n_dev)
        pl.semaphore_signal(barrier, inc=1, device_id={"sp2": peer // n_sp, "sp": lax.rem(peer, n_sp)}, device_id_type=MESH)

    def rcopy(src, dst, ssem, rsem, to_sp2, to_sp):
        return pltpu.make_async_remote_copy(src_ref=src, dst_ref=dst, send_sem=ssem, recv_sem=rsem,
                                            device_id={"sp2": to_sp2, "sp": to_sp}, device_id_type=MESH)

    corner_to = ((has_u & has_l, -1, -1, 3), (has_u & has_r, 1, -1, 2), (has_d & has_l, -1, 1, 1), (has_d & has_r, 1, 1, 0))

    def start_edges(t, par, n_rows, first=False):
        some, r_all = pl.ds(t * UNROLL, UNROLL), pl.ds(0, n_rows)

        @pl.when(has_l)
        def _():
            rcopy(edge_l.at[some, r_all], halo_r.at[par, some, r_all], col_send.at[0], col_recv.at[par, 1, t], sp2 - 1, sp).start()

        @pl.when(has_r)
        def _():
            rcopy(edge_r.at[some, r_all], halo_l.at[par, some, r_all], col_send.at[1], col_recv.at[par, 0, t], sp2 + 1, sp).start()

        for c, (there, d_sp2, d_sp, slot) in enumerate(corner_to):
            @pl.when(there)
            def _():
                rcopy(corner_s.at[c, t], corner_r.at[par, slot, t], cor_send.at[c], cor_recv.at[par, slot, t], sp2 + d_sp2, sp + d_sp).start()

        @pl.when(has_u)
        def _():
            src, dst = (edge_u.at[some], first_d.at[some]) if first else (z.at[some, 0], halo_d.at[par, some])
            rcopy(src, dst, row_send.at[0], row_recv.at[par, 1, t], sp2, sp - 1).start()

        @pl.when(has_d)
        def _():
            src, dst = (edge_d.at[some], first_u.at[some]) if first else (z.at[some, n_rows - 1], halo_u.at[par, some])
            rcopy(src, dst, row_send.at[1], row_recv.at[par, 0, t], sp2, sp + 1).start()

    def wait_edges(t, par, n_rows, first=False):
        some, r_all = pl.ds(t * UNROLL, UNROLL), pl.ds(0, n_rows)

        @pl.when(has_u)
        def _():
            src, dst = (edge_u.at[some], first_u.at[some]) if first else (z.at[some, 0], halo_u.at[par, some])
            rcopy(src, dst, row_send.at[0], row_recv.at[par, 0, t], sp2, sp).wait_recv()

        @pl.when(has_d)
        def _():
            src, dst = (edge_d.at[some], first_d.at[some]) if first else (z.at[some, n_rows - 1], halo_d.at[par, some])
            rcopy(src, dst, row_send.at[1], row_recv.at[par, 1, t], sp2, sp).wait_recv()

        @pl.when(has_l)
        def _():
            rcopy(edge_l.at[some, r_all], halo_l.at[par, some, r_all], col_send.at[0], col_recv.at[par, 0, t], sp2, sp).wait_recv()

        @pl.when(has_r)
        def _():
            rcopy(edge_r.at[some, r_all], halo_r.at[par, some, r_all], col_send.at[1], col_recv.at[par, 1, t], sp2, sp).wait_recv()

        for c, (there, d_sp2, d_sp, slot) in enumerate(corner_to):
            @pl.when(there)
            def _():
                rcopy(corner_s.at[c, t], corner_r.at[par, c, t], cor_send.at[c], cor_recv.at[par, c, t], sp2, sp).wait_recv()

    def wait_edges_sent(n_rows, first=False):
        r_all = pl.ds(0, n_rows)
        every = pl.ds(0, n_img)

        @pl.when(has_u)
        def _():
            src, dst = (edge_u, first_u) if first else (z.at[every, 0], halo_u.at[0])
            rcopy(src, dst, row_send.at[0], row_recv.at[0, 0, 0], sp2, sp).wait_send()

        @pl.when(has_d)
        def _():
            src, dst = (edge_d, first_d) if first else (z.at[every, n_rows - 1], halo_d.at[0])
            rcopy(src, dst, row_send.at[1], row_recv.at[0, 1, 0], sp2, sp).wait_send()

        @pl.when(has_l)
        def _():
            rcopy(edge_l.at[every, r_all], halo_l.at[0, every, r_all], col_send.at[0], col_recv.at[0, 0, 0], sp2, sp).wait_send()

        @pl.when(has_r)
        def _():
            rcopy(edge_r.at[every, r_all], halo_r.at[0, every, r_all], col_send.at[1], col_recv.at[0, 1, 0], sp2, sp).wait_send()

        for c, (there, d_sp2, d_sp, slot) in enumerate(corner_to):
            @pl.when(there)
            def _():
                rcopy(corner_s.at[c], corner_r.at[0, c], cor_send.at[c], cor_recv.at[0, c, 0], sp2, sp).wait_send()

    def stat_copy(d, par):
        peer = lax.rem(me + d, n_dev)
        return rcopy(stats.at[par, me], stats.at[par, me], st_send.at[d - 1], st_recv.at[par, me], peer // n_sp, lax.rem(peer, n_sp))

    def start_stats(par):
        total = acc[0] + acc[1]
        stats[par, me] = jnp.concatenate([jnp.sum(total[:, :128], axis=0, keepdims=True), jnp.sum(total[:, 128:], axis=0, keepdims=True)], axis=0)
        for d in range(1, n_dev):
            stat_copy(d, par).start()

    def wait_stats(par):
        for d in range(1, n_dev):
            stat_copy(d, par).wait_send()
            src = lax.rem(me + d, n_dev)
            rcopy(stats.at[par, src], stats.at[par, src], st_send.at[d - 1], st_recv.at[par, src], sp2, sp).wait_recv()

    def set_constants(par, gain, shift, count, paired):
        total = stats[par, 0]
        for src in range(1, n_dev):
            total = total + stats[par, src]
        if paired:
            total = total + pltpu.roll(total, ch, 1)
        mean = total[0:1] * (1.0 / count)
        var = total[1:2] * (1.0 / count) - mean * mean
        cst[0:1, :] = mean
        cst[1:2, :] = gain * lax.rsqrt(var + EPS)
        cst[2:3, :] = shift

    lane = lax.broadcasted_iota(jnp.int32, (pairs, 128), 1)

    def save_edges(t, u, n_rows):
        img = t * UNROLL + u
        flat = z.at[img].reshape(rows * pairs, 128)
        first = flat[pl.ds(0, n_rows, stride=pairs), :]
        final = flat[pl.ds(pairs - 1, n_rows, stride=pairs), :]
        edge_l[img, 0:n_rows, :] = first
        edge_r[img, 0:n_rows, :] = final
        corner_s[0, t, u:u + 1, :] = first[0:1]
        corner_s[1, t, u:u + 1, :] = final[0:1]
        corner_s[2, t, u:u + 1, :] = first[n_rows - 1:n_rows]
        corner_s[3, t, u:u + 1, :] = final[n_rows - 1:n_rows]

    def act(v, raw):
        return v if raw else normalise(v, cst)

    def prepare_corners(t, par, raw):
        for c, (there, d_sp2, d_sp, slot) in enumerate(corner_to):
            corner_n[c] = jnp.where(there, act(corner_r[par, c, t], raw), 0.0)

    def fill_lines(t, par, u, n_rows, raw, first_p):
        buf, img = lines[u], t * UNROLL + u
        left = jnp.where(has_l, act(halo_l[par, img, 0:n_rows, :], raw), 0.0)
        right = jnp.where(has_r, act(halo_r[par, img, 0:n_rows, :], raw), 0.0)
        buf[pl.ds(wide + EDGE - 1, n_rows, stride=wide), :] = left
        buf[pl.ds(wide + EDGE + pairs, n_rows, stride=wide), :] = right
        bottom = (n_rows + 1) * wide
        buf[EDGE - 1:EDGE, :] = corner_n[0, u:u + 1, :]
        buf[EDGE + pairs:EDGE + pairs + 1, :] = corner_n[1, u:u + 1, :]
        buf[bottom + EDGE - 1:bottom + EDGE, :] = corner_n[2, u:u + 1, :]
        buf[bottom + EDGE + pairs:bottom + EDGE + pairs + 1, :] = corner_n[3, u:u + 1, :]
        out = []
        for p in range(first_p, n_rows + 2):
            if p == 0:
                v = jnp.where(has_u, first_u[img].astype(F32) if raw else act(halo_u[par, img], raw), 0.0)
            elif p == n_rows + 1:
                v = jnp.where(has_d, first_d[img].astype(F32) if raw else act(halo_d[par, img], raw), 0.0)
            else:
                v = act(z[img, p - 1], raw)
            base = p * wide + EDGE
            buf[base:base + pairs, :] = v
            out.append((p, base, v))
        return out

    def build_pairs(t, par, u, raw, first_p=0):
        n_q = half + 1
        for p, base, own in fill_lines(t, par, u, rows, raw, first_p):
            side = jnp.where(lane < ch, lines[u][base + 1:base + 1 + pairs, :], lines[u][base - 1:base - 1 + pairs, :])
            bufs[u][2 * (p % 2) * n_q + p // 2] = own.astype(BF16)
            bufs[u][(2 * (p % 2) + 1) * n_q + p // 2] = side.astype(BF16)

    def build_wide(t, par, u):
        n_q = quarter + 1
        for p, base, own in fill_lines(t, par, u, half, False, 0):
            at = 3 * (p % 2) * n_q + p // 2
            bufs[u][at] = lines[u][base - 1:base - 1 + pairs, :].astype(BF16)
            bufs[u][at + n_q] = own.astype(BF16)
            bufs[u][at + 2 * n_q] = lines[u][base + 1:base + 1 + pairs, :].astype(BF16)

    def finish_conv(img, i0, o, dst=z):
        folded = o.reshape(o.shape[0] // 8, 8, 256)
        s = jnp.sum(folded, axis=0)
        q = jnp.sum(folded * folded, axis=0)
        acc[0] += jnp.concatenate([s[:, :128], q[:, :128]], axis=1)
        acc[1] += jnp.concatenate([s[:, 128:], q[:, 128:]], axis=1)
        for i in range(o.shape[0] // pairs):
            dst[img, 2 * (i0 + i)] = o[i * pairs:(i + 1) * pairs, :128]
            dst[img, 2 * (i0 + i) + 1] = o[i * pairs:(i + 1) * pairs, 128:]

    def dot(parts):
        lhs = jnp.concatenate(parts, axis=1)
        rhs = jnp.concatenate([wmat[0, 0:lhs.shape[1]], wmat[1, 0:lhs.shape[1]]], axis=1)
        return jnp.dot(lhs, rhs, preferred_element_type=F32)

    def conv_pairs(t, u):
        n_q, n_i = half + 1, half // SPLIT
        for i0 in range(0, half, n_i):
            at = [c * n_q + i0 + lo for lo in (0, 1) for c in range(4)]
            finish_conv(t * UNROLL + u, i0, dot([bufs[u][k:k + n_i].reshape(n_i * pairs, 128) for k in at]))
        save_edges(t, u, rows)

    def conv_down(t, u):
        n_q = half + 1
        at = [c * n_q + k for k, c in ((0, 2), (0, 3), (1, 0), (1, 1), (1, 2), (1, 3), (2, 0), (2, 1), (2, 2), (2, 3))]
        finish_conv(t * UNROLL + u, 0, dot([jnp.concatenate([bufs[u][k + 2 * i] for i in range(quarter)], axis=0) for k in at]))
        save_edges(t, u, half)

    def conv_wide(t, u):
        n_q = quarter + 1
        at = [c * n_q + lo for lo in (0, 1) for c in range(6)]
        finish_conv(t * UNROLL + u, 0, dot([bufs[u][k:k + quarter].reshape(quarter * pairs, 128) for k in at]), z_out)

    n_steps = n_img // UNROLL

    def run_layer(par, raw, n_rows, build, conv, n_out, par_out):
        acc[...] = jnp.zeros_like(acc)

        def body(t, carry):
            wait_edges(t, par, n_rows, raw)
            prepare_corners(t, par, raw)
            for u in range(UNROLL):
                build(t, u)
                conv(t, u)
            if n_out:
                @pl.when(t < n_steps - 1)
                def _():
                    start_edges(t, par_out, n_out)
            return carry

        lax.fori_loop(0, n_steps, body, 0)
        start_stats(par_out)
        if n_out:
            start_edges(n_steps - 1, par_out, n_out)

    def put_block(k, n_k, blocks):
        for o, blk in enumerate(blocks):
            wmat[o, k * n_k:(k + 1) * n_k, :] = jnp.zeros((n_k, 128), BF16) if blk is None else blk

    def weights_pairs(layer):
        zero = jnp.zeros((ch, ch), BF16)
        q = []
        for kh in range(3):
            w0, w1, w2 = w_a[layer, kh, 0], w_a[layer, kh, 1], w_a[layer, kh, 2]
            q.append(jnp.concatenate([
                jnp.concatenate([w1, w0], axis=1),
                jnp.concatenate([w2, w1], axis=1),
                jnp.concatenate([zero, w2], axis=1),
                jnp.concatenate([w0, zero], axis=1)], axis=0))
        for k in range(4):
            put_block(k, 256, [q[k] if k < 3 else None, q[k - 1] if k > 0 else None])

    def weights_down():
        d = [jnp.concatenate([w_down[kh, 0], w_down[kh, 1], w_down[kh, 2], jnp.zeros((ch, 128), BF16)], axis=0) for kh in range(3)]
        for k in range(5):
            put_block(k, 256, [d[k] if k < 3 else None, d[k - 2] if k >= 2 else None])

    def weights_wide():
        e = [jnp.concatenate([w_b[0, kh, 0], w_b[0, kh, 1], w_b[0, kh, 2]], axis=0) for kh in range(3)]
        for k in range(4):
            put_block(k, 384, [e[k] if k < 3 else None, e[k - 1] if k > 0 else None])

    wrow = lax.broadcasted_iota(jnp.int32, (128, 128), 0)
    wcol = lax.broadcasted_iota(jnp.int32, (128, 128), 1)
    source = jnp.where(wrow < pairs, 2 * wrow, 2 * (wrow - pairs) + 1)
    perm[...] = jnp.where(source == wcol, 1.0, 0.0).astype(BF16)

    def load_images(t, carry):
        x_copy(t).wait()
        for img_u in range(UNROLL):
            img = t * UNROLL + img_u
            for g in range(rows // 4):
                block = xv[img, 4 * g:4 * g + 4].reshape(4 * ch, 128)
                m = lax.dot_general(perm[...], block, (((1,), (1,)), ((), ())), preferred_element_type=F32)
                for b in range(2):
                    even = m[0:pairs, 128 * b:128 * b + 128]
                    odd = m[pairs:2 * pairs, 128 * b:128 * b + 128]
                    r = 4 * g + 2 * b
                    upper = jnp.where(lane < ch, even, pltpu.roll(odd, ch, 1))
                    lower = jnp.where(lane < ch, pltpu.roll(even, ch, 1), odd)
                    z[img, r] = upper
                    z[img, r + 1] = lower
                    if r == 0:
                        edge_u[img] = upper.astype(BF16)
                    if r + 2 == rows:
                        edge_d[img] = lower.astype(BF16)
            save_edges(t, img_u, rows)

        @pl.when(t == 0)
        def _():
            pl.semaphore_wait(barrier, n_dev - 1)

        start_edges(t, 0, rows, True)
        return carry

    lax.fori_loop(0, n_steps, load_images, 0)

    count_a = float(n_dev * n_img * rows * pairs * 2)
    count_b = float(n_dev * n_img * half * pairs)

    for copy in w_copies:
        copy.wait()
    weights_pairs(0)
    wait_edges_sent(rows, True)
    run_layer(0, True, rows, lambda t, u: build_pairs(t, 0, u, True), conv_pairs, rows, 1)

    def gains(layer):
        g, s = bn_a[layer, 0:1, :], bn_a[layer, 1:2, :]
        return jnp.concatenate([g, g], axis=1), jnp.concatenate([s, s], axis=1)

    n_layers = w_a.shape[0]

    def a_layer(layer, carry):
        par = lax.rem(layer, 2)
        weights_pairs(layer)
        wait_edges_sent(rows)
        wait_stats(par)
        g, s = gains(layer - 1)
        set_constants(par, g, s, count_a, True)
        run_layer(par, False, rows, lambda t, u: build_pairs(t, par, u, False), conv_pairs, rows, 1 - par)
        return carry

    lax.fori_loop(1, n_layers, a_layer, 0)

    par = n_layers % 2
    weights_down()
    wait_edges_sent(rows)
    wait_stats(par)
    g, s = gains(n_layers - 1)
    set_constants(par, g, s, count_a, True)
    run_layer(par, False, rows, lambda t, u: build_pairs(t, par, u, False, 1), conv_down, half, 1 - par)

    weights_wide()
    wait_edges_sent(half)
    wait_stats(1 - par)
    set_constants(1 - par, bn_down[0:1, :], bn_down[1:2, :], count_b, False)
    run_layer(1 - par, False, half, lambda t, u: build_wide(t, 1 - par, u), conv_wide, 0, par)
    wait_stats(par)
    set_constants(par, bn_b[0, 0:1, :], bn_b[0, 1:2, :], count_b, False)
    cst_out[...] = cst[...]


def finish_kernel(z, cst_ref, out_ref, y, out_sem):
    n_img, n_rows = z.shape[:2]

    def copy(img):
        return pltpu.make_async_copy(y.at[img], out_ref.at[img], out_sem.at[img])

    def step(img, carry):
        for r in range(n_rows):
            y[img, r] = normalise(z[img, r], cst_ref).astype(BF16)
        copy(img).start()
        return carry

    lax.fori_loop(0, n_img, step, 0)
    for img in range(n_img):
        copy(img).wait()


def solution(mesh):
    n_sp, n_sp2 = mesh.shape["sp"], mesh.shape["sp2"]

    def per_device(x, w_a, bn_a, w_down, bn_down, w_b, bn_b):
        n_img, rows, cols, ch = x.shape
        pairs, half = cols // 2, rows // 2
        n_dev = n_sp * n_sp2
        dims = (n_img, rows, pairs, ch, n_sp2, n_sp)
        vmem = pltpu.VMEM
        dma = pltpu.SemaphoreType.DMA
        scratch = [
            vmem((n_img, rows, ch, cols), BF16),
            vmem(w_a.shape, BF16), vmem(w_down.shape, BF16), vmem(w_b.shape, BF16),
            vmem((n_img, rows, pairs, 128), F32),
            [vmem((4 * (half + 1), pairs, 128), BF16) for _ in range(UNROLL)],
            [vmem(((rows + 2) * (pairs + 2 * EDGE), 128), F32) for _ in range(UNROLL)],
            vmem((2, 1536, 128), BF16),
            vmem((128, 128), BF16),
            vmem((n_img, pairs, 128), BF16), vmem((n_img, pairs, 128), BF16),
            vmem((n_img, pairs, 128), BF16), vmem((n_img, pairs, 128), BF16),
            vmem((n_img, rows, 128), F32),
            vmem((n_img, rows, 128), F32),
            vmem((2, n_img, pairs, 128), F32),
            vmem((2, n_img, pairs, 128), F32),
            vmem((2, n_img, rows, 128), F32),
            vmem((2, n_img, rows, 128), F32),
            vmem((4, n_img // UNROLL, UNROLL, 128), F32),
            vmem((2, 4, n_img // UNROLL, UNROLL, 128), F32),
            vmem((4, UNROLL, 128), F32),
            vmem((2, n_dev, 2, 128), F32),
            vmem((2, 8, 256), F32),
            vmem((8, 128), F32),
            dma((n_img // UNROLL,)),
            dma((3,)),
            dma((2,)), dma((2, 2, n_img // UNROLL)),
            dma((2,)), dma((2, 2, n_img // UNROLL)),
            dma((4,)), dma((2, 4, n_img // UNROLL)),
            dma((n_dev - 1,)), dma((2, n_dev)),
        ]
        in_vmem = pl.BlockSpec(memory_space=pltpu.VMEM)
        in_hbm = pl.BlockSpec(memory_space=pltpu.HBM)
        in_any = pl.BlockSpec(memory_space=pl.ANY)
        z, cst = pl.pallas_call(
            functools.partial(stack_kernel, dims),
            out_shape=(vmem((n_img, half, pairs, 128), F32), vmem((8, 128), F32)),
            in_specs=[in_hbm, in_hbm, in_vmem, in_hbm, in_vmem, in_hbm, in_vmem],
            out_specs=(in_vmem, in_vmem),
            scratch_shapes=scratch,
            compiler_params=pltpu.CompilerParams(collective_id=0, has_side_effects=True, vmem_limit_bytes=VMEM_LIMIT),
        )(jnp.transpose(x, (0, 1, 3, 2)), w_a, bn_a, w_down, bn_down, w_b, bn_b)
        return pl.pallas_call(
            finish_kernel,
            out_shape=jax.ShapeDtypeStruct((n_img, half, pairs, 128), BF16),
            in_specs=[in_vmem, in_vmem],
            out_specs=in_any,
            scratch_shapes=[vmem((n_img, half, pairs, 128), BF16), dma((n_img,))],
            compiler_params=pltpu.CompilerParams(vmem_limit_bytes=16 * 1024 * 1024),
        )(z, cst)

    tile_spec = P("dp", "sp", "sp2", None)
    return jax.shard_map(per_device, mesh=mesh, in_specs=(tile_spec, P(), P(), P(), P(), P(), P()), out_specs=tile_spec, check_vma=False)
```

```python
import functools

import jax
import jax.numpy as jnp
from jax import lax
from jax.experimental import pallas as pl
from jax.experimental.pallas import tpu as pltpu
from jax.sharding import PartitionSpec as P

MESH = pl.DeviceIdType.MESH
F32 = jnp.float32
BF16 = jnp.bfloat16
EPS = 1e-5
UNROLL = 4
BATCHES = 2
SPLIT = 1
VMEM_LIMIT = 51 * 1024 * 1024
EDGE = 8


def normalise(v, cst):
    return jnp.maximum((v - cst[0:1, :]) * cst[1:2, :] + cst[2:3, :], 0.0)


def stack_kernel(dims, x_ref, w_a_ref, bn_a, w_down_ref, bn_down, w_b_ref, bn_b, z_out, cst_out,
                 xv, w_a, w_down, w_b, z, bufs, lines, wmat, perm, edge_u, edge_d, first_u, first_d, edge_l, edge_r, halo_u, halo_d, halo_l, halo_r,
                 corner_s, corner_r, corner_n, stats, acc, cst,
                 x_sem, w_sem, row_send, row_recv, col_send, col_recv, cor_send, cor_recv, st_send, st_recv):
    n_img, rows, pairs, ch, n_sp2, n_sp = dims
    half, quarter = rows // 2, rows // 4
    wide = pairs + 2 * EDGE
    n_dev = n_sp2 * n_sp
    sp = lax.axis_index("sp")
    sp2 = lax.axis_index("sp2")
    me = sp2 * n_sp + sp
    has_u, has_d = sp > 0, sp < n_sp - 1
    has_l, has_r = sp2 > 0, sp2 < n_sp2 - 1

    def x_copy(t):
        some = pl.ds(t * UNROLL, UNROLL)
        return pltpu.make_async_copy(x_ref.at[some], xv.at[some], x_sem.at[t])

    for t in range(n_img // UNROLL):
        x_copy(t).start()

    w_copies = [pltpu.make_async_copy(src, dst, w_sem.at[i]) for i, (src, dst) in enumerate(((w_a_ref, w_a), (w_down_ref, w_down), (w_b_ref, w_b)))]
    for copy in w_copies:
        copy.start()

    barrier = pltpu.get_barrier_semaphore()
    for d in range(1, n_dev):
        peer = lax.rem(me + d, n_dev)
        pl.semaphore_signal(barrier, inc=1, device_id={"sp2": peer // n_sp, "sp": lax.rem(peer, n_sp)}, device_id_type=MESH)

    def rcopy(src, dst, ssem, rsem, to_sp2, to_sp):
        return pltpu.make_async_remote_copy(src_ref=src, dst_ref=dst, send_sem=ssem, recv_sem=rsem,
                                            device_id={"sp2": to_sp2, "sp": to_sp}, device_id_type=MESH)

    corner_to = ((has_u & has_l, -1, -1, 3), (has_u & has_r, 1, -1, 2), (has_d & has_l, -1, 1, 1), (has_d & has_r, 1, 1, 0))

    def start_edges(t, par, n_rows, first=False):
        some, r_all = pl.ds(t * UNROLL, UNROLL), pl.ds(0, n_rows)

        @pl.when(has_l)
        def _():
            rcopy(edge_l.at[par, some, r_all], halo_r.at[par, some, r_all], col_send.at[par, 0], col_recv.at[par, 1, t], sp2 - 1, sp).start()

        @pl.when(has_r)
        def _():
            rcopy(edge_r.at[par, some, r_all], halo_l.at[par, some, r_all], col_send.at[par, 1], col_recv.at[par, 0, t], sp2 + 1, sp).start()

        for c, (there, d_sp2, d_sp, slot) in enumerate(corner_to):
            @pl.when(there)
            def _():
                rcopy(corner_s.at[par, c, t], corner_r.at[par, slot, t], cor_send.at[par, c], cor_recv.at[par, slot, t], sp2 + d_sp2, sp + d_sp).start()

        @pl.when(has_u)
        def _():
            src, dst = (edge_u.at[some], first_d.at[some]) if first else (z.at[some, 0], halo_d.at[par, some])
            rcopy(src, dst, row_send.at[par, 0], row_recv.at[par, 1, t], sp2, sp - 1).start()

        @pl.when(has_d)
        def _():
            src, dst = (edge_d.at[some], first_u.at[some]) if first else (z.at[some, n_rows - 1], halo_u.at[par, some])
            rcopy(src, dst, row_send.at[par, 1], row_recv.at[par, 0, t], sp2, sp + 1).start()

    def wait_edges(t, par, n_rows, first=False):
        some, r_all = pl.ds(t * UNROLL, UNROLL), pl.ds(0, n_rows)

        @pl.when(has_u)
        def _():
            src, dst = (edge_u.at[some], first_u.at[some]) if first else (z.at[some, 0], halo_u.at[par, some])
            rcopy(src, dst, row_send.at[par, 0], row_recv.at[par, 0, t], sp2, sp).wait_recv()

        @pl.when(has_d)
        def _():
            src, dst = (edge_d.at[some], first_d.at[some]) if first else (z.at[some, n_rows - 1], halo_d.at[par, some])
            rcopy(src, dst, row_send.at[par, 1], row_recv.at[par, 1, t], sp2, sp).wait_recv()

        @pl.when(has_l)
        def _():
            rcopy(edge_l.at[par, some, r_all], halo_l.at[par, some, r_all], col_send.at[par, 0], col_recv.at[par, 0, t], sp2, sp).wait_recv()

        @pl.when(has_r)
        def _():
            rcopy(edge_r.at[par, some, r_all], halo_r.at[par, some, r_all], col_send.at[par, 1], col_recv.at[par, 1, t], sp2, sp).wait_recv()

        for c, (there, d_sp2, d_sp, slot) in enumerate(corner_to):
            @pl.when(there)
            def _():
                rcopy(corner_s.at[par, c, t], corner_r.at[par, c, t], cor_send.at[par, c], cor_recv.at[par, c, t], sp2, sp).wait_recv()

    def wait_edges_sent(par, n_rows, first=False):
        r_all = pl.ds(0, n_rows)
        every = pl.ds(0, n_img)

        @pl.when(has_u)
        def _():
            src, dst = (edge_u, first_u) if first else (z.at[every, 0], halo_u.at[0])
            rcopy(src, dst, row_send.at[par, 0], row_recv.at[0, 0, 0], sp2, sp).wait_send()

        @pl.when(has_d)
        def _():
            src, dst = (edge_d, first_d) if first else (z.at[every, n_rows - 1], halo_d.at[0])
            rcopy(src, dst, row_send.at[par, 1], row_recv.at[0, 1, 0], sp2, sp).wait_send()

        @pl.when(has_l)
        def _():
            rcopy(edge_l.at[par, every, r_all], halo_l.at[0, every, r_all], col_send.at[par, 0], col_recv.at[0, 0, 0], sp2, sp).wait_send()

        @pl.when(has_r)
        def _():
            rcopy(edge_r.at[par, every, r_all], halo_r.at[0, every, r_all], col_send.at[par, 1], col_recv.at[0, 1, 0], sp2, sp).wait_send()

        for c, (there, d_sp2, d_sp, slot) in enumerate(corner_to):
            @pl.when(there)
            def _():
                rcopy(corner_s.at[par, c], corner_r.at[0, c], cor_send.at[par, c], cor_recv.at[0, c, 0], sp2, sp).wait_send()

    def stat_copy(d, par):
        peer = lax.rem(me + d, n_dev)
        return rcopy(stats.at[par, me], stats.at[par, me], st_send.at[d - 1], st_recv.at[par, me], peer // n_sp, lax.rem(peer, n_sp))

    def start_stats(par):
        total = acc[0] + acc[1]
        stats[par, me] = jnp.concatenate([jnp.sum(total[:, :128], axis=0, keepdims=True), jnp.sum(total[:, 128:], axis=0, keepdims=True)], axis=0)
        for d in range(1, n_dev):
            stat_copy(d, par).start()

    def wait_stats(par):
        for d in range(1, n_dev):
            stat_copy(d, par).wait_send()
            src = lax.rem(me + d, n_dev)
            rcopy(stats.at[par, src], stats.at[par, src], st_send.at[d - 1], st_recv.at[par, src], sp2, sp).wait_recv()

    def set_constants(par, gain, shift, count, paired):
        total = stats[par, 0]
        for src in range(1, n_dev):
            total = total + stats[par, src]
        if paired:
            total = total + pltpu.roll(total, ch, 1)
        mean = total[0:1] * (1.0 / count)
        var = total[1:2] * (1.0 / count) - mean * mean
        cst[0:1, :] = mean
        cst[1:2, :] = gain * lax.rsqrt(var + EPS)
        cst[2:3, :] = shift

    lane = lax.broadcasted_iota(jnp.int32, (pairs, 128), 1)

    def save_edges(t, u, n_rows, par):
        img = t * UNROLL + u
        flat = z.at[img].reshape(rows * pairs, 128)
        first = flat[pl.ds(0, n_rows, stride=pairs), :]
        final = flat[pl.ds(pairs - 1, n_rows, stride=pairs), :]
        edge_l[par, img, 0:n_rows, :] = first
        edge_r[par, img, 0:n_rows, :] = final
        corner_s[par, 0, t, u:u + 1, :] = first[0:1]
        corner_s[par, 1, t, u:u + 1, :] = final[0:1]
        corner_s[par, 2, t, u:u + 1, :] = first[n_rows - 1:n_rows]
        corner_s[par, 3, t, u:u + 1, :] = final[n_rows - 1:n_rows]

    def act(v, raw):
        return v if raw else normalise(v, cst)

    def prepare_corners(b, t, par, raw):
        for c, (there, d_sp2, d_sp, slot) in enumerate(corner_to):
            corner_n[b, c] = jnp.where(there, act(corner_r[par, c, t], raw), 0.0)

    def fill_lines(t, par, u, k, n_rows, raw, first_p):
        buf, img, b = lines[k], t * UNROLL + u, k // UNROLL
        left = jnp.where(has_l, act(halo_l[par, img, 0:n_rows, :], raw), 0.0)
        right = jnp.where(has_r, act(halo_r[par, img, 0:n_rows, :], raw), 0.0)
        buf[pl.ds(wide + EDGE - 1, n_rows, stride=wide), :] = left
        buf[pl.ds(wide + EDGE + pairs, n_rows, stride=wide), :] = right
        bottom = (n_rows + 1) * wide
        buf[EDGE - 1:EDGE, :] = corner_n[b, 0, u:u + 1, :]
        buf[EDGE + pairs:EDGE + pairs + 1, :] = corner_n[b, 1, u:u + 1, :]
        buf[bottom + EDGE - 1:bottom + EDGE, :] = corner_n[b, 2, u:u + 1, :]
        buf[bottom + EDGE + pairs:bottom + EDGE + pairs + 1, :] = corner_n[b, 3, u:u + 1, :]
        out = []
        for p in range(first_p, n_rows + 2):
            if p == 0:
                v = jnp.where(has_u, first_u[img].astype(F32) if raw else act(halo_u[par, img], raw), 0.0)
            elif p == n_rows + 1:
                v = jnp.where(has_d, first_d[img].astype(F32) if raw else act(halo_d[par, img], raw), 0.0)
            else:
                v = act(z[img, p - 1], raw)
            base = p * wide + EDGE
            buf[base:base + pairs, :] = v
            out.append((p, base, v))
        return out

    def build_pairs(t, par, u, k, raw, first_p=0):
        n_q = half + 1
        for p, base, own in fill_lines(t, par, u, k, rows, raw, first_p):
            side = jnp.where(lane < ch, lines[k][base + 1:base + 1 + pairs, :], lines[k][base - 1:base - 1 + pairs, :])
            bufs[k][2 * (p % 2) * n_q + p // 2] = own.astype(BF16)
            bufs[k][(2 * (p % 2) + 1) * n_q + p // 2] = side.astype(BF16)

    def build_wide(t, par, u, k):
        n_q = quarter + 1
        for p, base, own in fill_lines(t, par, u, k, half, False, 0):
            at = 3 * (p % 2) * n_q + p // 2
            bufs[k][at] = lines[k][base - 1:base - 1 + pairs, :].astype(BF16)
            bufs[k][at + n_q] = own.astype(BF16)
            bufs[k][at + 2 * n_q] = lines[k][base + 1:base + 1 + pairs, :].astype(BF16)

    def finish_conv(img, i0, o, dst=z):
        folded = o.reshape(o.shape[0] // 8, 8, 256)
        s = jnp.sum(folded, axis=0)
        q = jnp.sum(folded * folded, axis=0)
        acc[0] += jnp.concatenate([s[:, :128], q[:, :128]], axis=1)
        acc[1] += jnp.concatenate([s[:, 128:], q[:, 128:]], axis=1)
        for i in range(o.shape[0] // pairs):
            dst[img, 2 * (i0 + i)] = o[i * pairs:(i + 1) * pairs, :128]
            dst[img, 2 * (i0 + i) + 1] = o[i * pairs:(i + 1) * pairs, 128:]

    def dot(parts):
        lhs = jnp.concatenate(parts, axis=1)
        rhs = jnp.concatenate([wmat[0, 0:lhs.shape[1]], wmat[1, 0:lhs.shape[1]]], axis=1)
        return jnp.dot(lhs, rhs, preferred_element_type=F32)

    def conv_pairs(t, u, k, par_out):
        n_q, n_i = half + 1, half // SPLIT
        for i0 in range(0, half, n_i):
            at = [c * n_q + i0 + lo for lo in (0, 1) for c in range(4)]
            finish_conv(t * UNROLL + u, i0, dot([bufs[k][j:j + n_i].reshape(n_i * pairs, 128) for j in at]))
        save_edges(t, u, rows, par_out)

    def conv_down(t, u, k, par_out):
        n_q = half + 1
        at = [c * n_q + j for j, c in ((0, 2), (0, 3), (1, 0), (1, 1), (1, 2), (1, 3), (2, 0), (2, 1), (2, 2), (2, 3))]
        finish_conv(t * UNROLL + u, 0, dot([jnp.concatenate([bufs[k][j + 2 * i] for i in range(quarter)], axis=0) for j in at]))
        save_edges(t, u, half, par_out)

    def conv_wide(t, u, k, par_out):
        n_q = quarter + 1
        at = [c * n_q + lo for lo in (0, 1) for c in range(6)]
        finish_conv(t * UNROLL + u, 0, dot([bufs[k][j:j + quarter].reshape(quarter * pairs, 128) for j in at]), z_out)

    n_steps = n_img // UNROLL

    n_steps = n_img // UNROLL

    def run_layer(par, raw, n_rows, build, conv, n_out, par_out, batches=1):
        acc[...] = jnp.zeros_like(acc)

        def body(step, carry):
            steps = [step * batches + b for b in range(batches)]
            for b, t in enumerate(steps):
                wait_edges(t, par, n_rows, raw)
                prepare_corners(b, t, par, raw)
            for b, t in enumerate(steps):
                for u in range(UNROLL):
                    build(t, u, b * UNROLL + u)
                    conv(t, u, b * UNROLL + u, par_out)
            if n_out:
                @pl.when(step < n_steps // batches - 1)
                def _():
                    for t in steps:
                        start_edges(t, par_out, n_out)
            return carry

        lax.fori_loop(0, n_steps // batches, body, 0)
        start_stats(par_out)
        if n_out:
            for b in range(batches):
                start_edges(n_steps - batches + b, par_out, n_out)

    def put_block(k, n_k, blocks):
        for o, blk in enumerate(blocks):
            wmat[o, k * n_k:(k + 1) * n_k, :] = jnp.zeros((n_k, 128), BF16) if blk is None else blk

    def weights_pairs(layer):
        zero = jnp.zeros((ch, ch), BF16)
        q = []
        for kh in range(3):
            w0, w1, w2 = w_a[layer, kh, 0], w_a[layer, kh, 1], w_a[layer, kh, 2]
            q.append(jnp.concatenate([
                jnp.concatenate([w1, w0], axis=1),
                jnp.concatenate([w2, w1], axis=1),
                jnp.concatenate([zero, w2], axis=1),
                jnp.concatenate([w0, zero], axis=1)], axis=0))
        for k in range(4):
            put_block(k, 256, [q[k] if k < 3 else None, q[k - 1] if k > 0 else None])

    def weights_down():
        d = [jnp.concatenate([w_down[kh, 0], w_down[kh, 1], w_down[kh, 2], jnp.zeros((ch, 128), BF16)], axis=0) for kh in range(3)]
        for k in range(5):
            put_block(k, 256, [d[k] if k < 3 else None, d[k - 2] if k >= 2 else None])

    def weights_wide():
        e = [jnp.concatenate([w_b[0, kh, 0], w_b[0, kh, 1], w_b[0, kh, 2]], axis=0) for kh in range(3)]
        for k in range(4):
            put_block(k, 384, [e[k] if k < 3 else None, e[k - 1] if k > 0 else None])

    wrow = lax.broadcasted_iota(jnp.int32, (128, 128), 0)
    wcol = lax.broadcasted_iota(jnp.int32, (128, 128), 1)
    source = jnp.where(wrow < pairs, 2 * wrow, 2 * (wrow - pairs) + 1)
    perm[...] = jnp.where(source == wcol, 1.0, 0.0).astype(BF16)

    def load_images(t, carry):
        x_copy(t).wait()
        for img_u in range(UNROLL):
            img = t * UNROLL + img_u
            for g in range(rows // 4):
                block = xv[img, 4 * g:4 * g + 4].reshape(4 * ch, 128)
                m = lax.dot_general(perm[...], block, (((1,), (1,)), ((), ())), preferred_element_type=F32)
                for b in range(2):
                    even = m[0:pairs, 128 * b:128 * b + 128]
                    odd = m[pairs:2 * pairs, 128 * b:128 * b + 128]
                    r = 4 * g + 2 * b
                    upper = jnp.where(lane < ch, even, pltpu.roll(odd, ch, 1))
                    lower = jnp.where(lane < ch, pltpu.roll(even, ch, 1), odd)
                    z[img, r] = upper
                    z[img, r + 1] = lower
                    if r == 0:
                        edge_u[img] = upper.astype(BF16)
                    if r + 2 == rows:
                        edge_d[img] = lower.astype(BF16)
            save_edges(t, img_u, rows, 0)

        @pl.when(t == 0)
        def _():
            pl.semaphore_wait(barrier, n_dev - 1)

        start_edges(t, 0, rows, True)
        return carry

    lax.fori_loop(0, n_steps, load_images, 0)

    count_a = float(n_dev * n_img * rows * pairs * 2)
    count_b = float(n_dev * n_img * half * pairs)

    for copy in w_copies:
        copy.wait()
    weights_pairs(0)
    run_layer(0, True, rows, lambda t, u, k: build_pairs(t, 0, u, k, True), conv_pairs, rows, 1)
    wait_edges_sent(0, rows, True)

    def gains(layer):
        g, s = bn_a[layer, 0:1, :], bn_a[layer, 1:2, :]
        return jnp.concatenate([g, g], axis=1), jnp.concatenate([s, s], axis=1)

    n_layers = w_a.shape[0]

    def a_layer(layer, carry):
        par = lax.rem(layer, 2)
        weights_pairs(layer)
        wait_edges_sent(par, rows)
        wait_stats(par)
        g, s = gains(layer - 1)
        set_constants(par, g, s, count_a, True)
        run_layer(par, False, rows, lambda t, u, k: build_pairs(t, par, u, k, False), conv_pairs, rows, 1 - par, BATCHES)
        return carry

    lax.fori_loop(1, n_layers, a_layer, 0)

    par = n_layers % 2
    weights_down()
    wait_edges_sent(par, rows)
    wait_stats(par)
    g, s = gains(n_layers - 1)
    set_constants(par, g, s, count_a, True)
    run_layer(par, False, rows, lambda t, u, k: build_pairs(t, par, u, k, False, 1), conv_down, half, 1 - par)

    weights_wide()
    wait_edges_sent(1 - par, half)
    wait_stats(1 - par)
    set_constants(1 - par, bn_down[0:1, :], bn_down[1:2, :], count_b, False)
    run_layer(1 - par, False, half, lambda t, u, k: build_wide(t, 1 - par, u, k), conv_wide, 0, par)
    wait_stats(par)
    set_constants(par, bn_b[0, 0:1, :], bn_b[0, 1:2, :], count_b, False)
    cst_out[...] = cst[...]


def finish_kernel(z, cst_ref, out_ref, y, out_sem):
    n_img, n_rows = z.shape[:2]

    def copy(img):
        return pltpu.make_async_copy(y.at[img], out_ref.at[img], out_sem.at[img])

    def step(img, carry):
        for r in range(n_rows):
            y[img, r] = normalise(z[img, r], cst_ref).astype(BF16)
        copy(img).start()
        return carry

    lax.fori_loop(0, n_img, step, 0)
    for img in range(n_img):
        copy(img).wait()


def solution(mesh):
    n_sp, n_sp2 = mesh.shape["sp"], mesh.shape["sp2"]

    def per_device(x, w_a, bn_a, w_down, bn_down, w_b, bn_b):
        n_img, rows, cols, ch = x.shape
        pairs, half = cols // 2, rows // 2
        n_dev = n_sp * n_sp2
        dims = (n_img, rows, pairs, ch, n_sp2, n_sp)
        vmem = pltpu.VMEM
        dma = pltpu.SemaphoreType.DMA
        scratch = [
            vmem((n_img, rows, ch, cols), BF16),
            vmem(w_a.shape, BF16), vmem(w_down.shape, BF16), vmem(w_b.shape, BF16),
            vmem((n_img, rows, pairs, 128), F32),
            [vmem((4 * (half + 1), pairs, 128), BF16) for _ in range(BATCHES * UNROLL)],
            [vmem(((rows + 2) * (pairs + 2 * EDGE), 128), F32) for _ in range(BATCHES * UNROLL)],
            vmem((2, 1536, 128), BF16),
            vmem((128, 128), BF16),
            vmem((n_img, pairs, 128), BF16), vmem((n_img, pairs, 128), BF16),
            vmem((n_img, pairs, 128), BF16), vmem((n_img, pairs, 128), BF16),
            vmem((2, n_img, rows, 128), F32),
            vmem((2, n_img, rows, 128), F32),
            vmem((2, n_img, pairs, 128), F32),
            vmem((2, n_img, pairs, 128), F32),
            vmem((2, n_img, rows, 128), F32),
            vmem((2, n_img, rows, 128), F32),
            vmem((2, 4, n_img // UNROLL, UNROLL, 128), F32),
            vmem((2, 4, n_img // UNROLL, UNROLL, 128), F32),
            vmem((2, 4, UNROLL, 128), F32),
            vmem((2, n_dev, 2, 128), F32),
            vmem((2, 8, 256), F32),
            vmem((8, 128), F32),
            dma((n_img // UNROLL,)),
            dma((3,)),
            dma((2, 2)), dma((2, 2, n_img // UNROLL)),
            dma((2, 2)), dma((2, 2, n_img // UNROLL)),
            dma((2, 4)), dma((2, 4, n_img // UNROLL)),
            dma((n_dev - 1,)), dma((2, n_dev)),
        ]
        in_vmem = pl.BlockSpec(memory_space=pltpu.VMEM)
        in_hbm = pl.BlockSpec(memory_space=pltpu.HBM)
        in_any = pl.BlockSpec(memory_space=pl.ANY)
        z, cst = pl.pallas_call(
            functools.partial(stack_kernel, dims),
            out_shape=(vmem((n_img, half, pairs, 128), F32), vmem((8, 128), F32)),
            in_specs=[in_hbm, in_hbm, in_vmem, in_hbm, in_vmem, in_hbm, in_vmem],
            out_specs=(in_vmem, in_vmem),
            scratch_shapes=scratch,
            compiler_params=pltpu.CompilerParams(collective_id=0, has_side_effects=True, vmem_limit_bytes=VMEM_LIMIT),
        )(jnp.transpose(x, (0, 1, 3, 2)), w_a, bn_a, w_down, bn_down, w_b, bn_b)
        return pl.pallas_call(
            finish_kernel,
            out_shape=jax.ShapeDtypeStruct((n_img, half, pairs, 128), BF16),
            in_specs=[in_vmem, in_vmem],
            out_specs=in_any,
            scratch_shapes=[vmem((n_img, half, pairs, 128), BF16), dma((n_img,))],
            compiler_params=pltpu.CompilerParams(vmem_limit_bytes=16 * 1024 * 1024),
        )(z, cst)

    tile_spec = P("dp", "sp", "sp2", None)
    return jax.shard_map(per_device, mesh=mesh, in_specs=(tile_spec, P(), P(), P(), P(), P(), P()), out_specs=tile_spec, check_vma=False)
```

```python
import functools

import jax
import jax.numpy as jnp
from jax import lax
from jax.experimental import pallas as pl
from jax.experimental.pallas import tpu as pltpu
from jax.sharding import PartitionSpec as P

MESH = pl.DeviceIdType.MESH
F32 = jnp.float32
BF16 = jnp.bfloat16
EPS = 1e-5
UNROLL = 4
BATCHES = 2
JOIN = 2
VMEM_LIMIT = 51 * 1024 * 1024
EDGE = 8


def normalise(v, cst):
    return jnp.maximum((v - cst[0:1, :]) * cst[1:2, :] + cst[2:3, :], 0.0)


def stack_kernel(dims, x_ref, w_a_ref, bn_a, w_down_ref, bn_down, w_b_ref, bn_b, z_out, cst_out,
                 xv, w_a, w_down, w_b, z, bufs, lines, wmat, perm, edge_u, edge_d, first_u, first_d, edge_l, edge_r, halo_u, halo_d, halo_l, halo_r,
                 corner_s, corner_r, corner_n, stats, acc, cst,
                 x_sem, w_sem, row_send, row_recv, col_send, col_recv, cor_send, cor_recv, st_send, st_recv):
    n_img, rows, pairs, ch, n_sp2, n_sp = dims
    half, quarter = rows // 2, rows // 4
    wide = pairs + 2 * EDGE
    n_dev = n_sp2 * n_sp
    sp = lax.axis_index("sp")
    sp2 = lax.axis_index("sp2")
    me = sp2 * n_sp + sp
    has_u, has_d = sp > 0, sp < n_sp - 1
    has_l, has_r = sp2 > 0, sp2 < n_sp2 - 1

    def x_copy(t):
        some = pl.ds(t * UNROLL, UNROLL)
        return pltpu.make_async_copy(x_ref.at[some], xv.at[some], x_sem.at[t])

    for t in range(n_img // UNROLL):
        x_copy(t).start()

    w_copies = [pltpu.make_async_copy(src, dst, w_sem.at[i]) for i, (src, dst) in enumerate(((w_a_ref, w_a), (w_down_ref, w_down), (w_b_ref, w_b)))]
    for copy in w_copies:
        copy.start()

    barrier = pltpu.get_barrier_semaphore()
    for d in range(1, n_dev):
        peer = lax.rem(me + d, n_dev)
        pl.semaphore_signal(barrier, inc=1, device_id={"sp2": peer // n_sp, "sp": lax.rem(peer, n_sp)}, device_id_type=MESH)

    def rcopy(src, dst, ssem, rsem, to_sp2, to_sp):
        return pltpu.make_async_remote_copy(src_ref=src, dst_ref=dst, send_sem=ssem, recv_sem=rsem,
                                            device_id={"sp2": to_sp2, "sp": to_sp}, device_id_type=MESH)

    corner_to = ((has_u & has_l, -1, -1, 3), (has_u & has_r, 1, -1, 2), (has_d & has_l, -1, 1, 1), (has_d & has_r, 1, 1, 0))

    def start_edges(t, par, n_rows, first=False):
        some, r_all = pl.ds(t * UNROLL, UNROLL), pl.ds(0, n_rows)

        @pl.when(has_l)
        def _():
            rcopy(edge_l.at[par, some, r_all], halo_r.at[par, some, r_all], col_send.at[par, 0], col_recv.at[par, 1, t], sp2 - 1, sp).start()

        @pl.when(has_r)
        def _():
            rcopy(edge_r.at[par, some, r_all], halo_l.at[par, some, r_all], col_send.at[par, 1], col_recv.at[par, 0, t], sp2 + 1, sp).start()

        for c, (there, d_sp2, d_sp, slot) in enumerate(corner_to):
            @pl.when(there)
            def _():
                rcopy(corner_s.at[par, c, t], corner_r.at[par, slot, t], cor_send.at[par, c], cor_recv.at[par, slot, t], sp2 + d_sp2, sp + d_sp).start()

        @pl.when(has_u)
        def _():
            src, dst = (edge_u.at[some], first_d.at[some]) if first else (z.at[some, 0], halo_d.at[par, some])
            rcopy(src, dst, row_send.at[par, 0], row_recv.at[par, 1, t], sp2, sp - 1).start()

        @pl.when(has_d)
        def _():
            src, dst = (edge_d.at[some], first_u.at[some]) if first else (z.at[some, n_rows - 1], halo_u.at[par, some])
            rcopy(src, dst, row_send.at[par, 1], row_recv.at[par, 0, t], sp2, sp + 1).start()

    def wait_edges(t, par, n_rows, first=False):
        some, r_all = pl.ds(t * UNROLL, UNROLL), pl.ds(0, n_rows)

        @pl.when(has_u)
        def _():
            src, dst = (edge_u.at[some], first_u.at[some]) if first else (z.at[some, 0], halo_u.at[par, some])
            rcopy(src, dst, row_send.at[par, 0], row_recv.at[par, 0, t], sp2, sp).wait_recv()

        @pl.when(has_d)
        def _():
            src, dst = (edge_d.at[some], first_d.at[some]) if first else (z.at[some, n_rows - 1], halo_d.at[par, some])
            rcopy(src, dst, row_send.at[par, 1], row_recv.at[par, 1, t], sp2, sp).wait_recv()

        @pl.when(has_l)
        def _():
            rcopy(edge_l.at[par, some, r_all], halo_l.at[par, some, r_all], col_send.at[par, 0], col_recv.at[par, 0, t], sp2, sp).wait_recv()

        @pl.when(has_r)
        def _():
            rcopy(edge_r.at[par, some, r_all], halo_r.at[par, some, r_all], col_send.at[par, 1], col_recv.at[par, 1, t], sp2, sp).wait_recv()

        for c, (there, d_sp2, d_sp, slot) in enumerate(corner_to):
            @pl.when(there)
            def _():
                rcopy(corner_s.at[par, c, t], corner_r.at[par, c, t], cor_send.at[par, c], cor_recv.at[par, c, t], sp2, sp).wait_recv()

    def wait_edges_sent(par, n_rows, first=False):
        r_all = pl.ds(0, n_rows)
        every = pl.ds(0, n_img)

        @pl.when(has_u)
        def _():
            src, dst = (edge_u, first_u) if first else (z.at[every, 0], halo_u.at[0])
            rcopy(src, dst, row_send.at[par, 0], row_recv.at[0, 0, 0], sp2, sp).wait_send()

        @pl.when(has_d)
        def _():
            src, dst = (edge_d, first_d) if first else (z.at[every, n_rows - 1], halo_d.at[0])
            rcopy(src, dst, row_send.at[par, 1], row_recv.at[0, 1, 0], sp2, sp).wait_send()

        @pl.when(has_l)
        def _():
            rcopy(edge_l.at[par, every, r_all], halo_l.at[0, every, r_all], col_send.at[par, 0], col_recv.at[0, 0, 0], sp2, sp).wait_send()

        @pl.when(has_r)
        def _():
            rcopy(edge_r.at[par, every, r_all], halo_r.at[0, every, r_all], col_send.at[par, 1], col_recv.at[0, 1, 0], sp2, sp).wait_send()

        for c, (there, d_sp2, d_sp, slot) in enumerate(corner_to):
            @pl.when(there)
            def _():
                rcopy(corner_s.at[par, c], corner_r.at[0, c], cor_send.at[par, c], cor_recv.at[0, c, 0], sp2, sp).wait_send()

    def stat_copy(d, par):
        peer = lax.rem(me + d, n_dev)
        return rcopy(stats.at[par, me], stats.at[par, me], st_send.at[d - 1], st_recv.at[par, me], peer // n_sp, lax.rem(peer, n_sp))

    def start_stats(par):
        total = acc[0] + acc[1]
        stats[par, me] = jnp.concatenate([jnp.sum(total[:, :128], axis=0, keepdims=True), jnp.sum(total[:, 128:], axis=0, keepdims=True)], axis=0)
        for d in range(1, n_dev):
            stat_copy(d, par).start()

    def wait_stats(par):
        for d in range(1, n_dev):
            stat_copy(d, par).wait_send()
            src = lax.rem(me + d, n_dev)
            rcopy(stats.at[par, src], stats.at[par, src], st_send.at[d - 1], st_recv.at[par, src], sp2, sp).wait_recv()

    def set_constants(par, gain, shift, count, paired):
        total = stats[par, 0]
        for src in range(1, n_dev):
            total = total + stats[par, src]
        if paired:
            total = total + pltpu.roll(total, ch, 1)
        mean = total[0:1] * (1.0 / count)
        var = total[1:2] * (1.0 / count) - mean * mean
        cst[0:1, :] = mean
        cst[1:2, :] = gain * lax.rsqrt(var + EPS)
        cst[2:3, :] = shift

    lane = lax.broadcasted_iota(jnp.int32, (pairs, 128), 1)

    def save_edges(t, u, n_rows, par):
        img = t * UNROLL + u
        flat = z.at[img].reshape(rows * pairs, 128)
        first = flat[pl.ds(0, n_rows, stride=pairs), :]
        final = flat[pl.ds(pairs - 1, n_rows, stride=pairs), :]
        edge_l[par, img, 0:n_rows, :] = first
        edge_r[par, img, 0:n_rows, :] = final
        corner_s[par, 0, t, u:u + 1, :] = first[0:1]
        corner_s[par, 1, t, u:u + 1, :] = final[0:1]
        corner_s[par, 2, t, u:u + 1, :] = first[n_rows - 1:n_rows]
        corner_s[par, 3, t, u:u + 1, :] = final[n_rows - 1:n_rows]

    def act(v, raw):
        return v if raw else normalise(v, cst)

    def prepare_corners(b, t, par, raw):
        for c, (there, d_sp2, d_sp, slot) in enumerate(corner_to):
            corner_n[b, c] = jnp.where(there, act(corner_r[par, c, t], raw), 0.0)

    def fill_lines(t, par, u, k, n_rows, raw, first_p):
        buf, img, b = lines[k], t * UNROLL + u, k // UNROLL
        left = jnp.where(has_l, act(halo_l[par, img, 0:n_rows, :], raw), 0.0)
        right = jnp.where(has_r, act(halo_r[par, img, 0:n_rows, :], raw), 0.0)
        buf[pl.ds(wide + EDGE - 1, n_rows, stride=wide), :] = left
        buf[pl.ds(wide + EDGE + pairs, n_rows, stride=wide), :] = right
        bottom = (n_rows + 1) * wide
        buf[EDGE - 1:EDGE, :] = corner_n[b, 0, u:u + 1, :]
        buf[EDGE + pairs:EDGE + pairs + 1, :] = corner_n[b, 1, u:u + 1, :]
        buf[bottom + EDGE - 1:bottom + EDGE, :] = corner_n[b, 2, u:u + 1, :]
        buf[bottom + EDGE + pairs:bottom + EDGE + pairs + 1, :] = corner_n[b, 3, u:u + 1, :]
        out = []
        for p in range(first_p, n_rows + 2):
            if p == 0:
                v = jnp.where(has_u, first_u[img].astype(F32) if raw else act(halo_u[par, img], raw), 0.0)
            elif p == n_rows + 1:
                v = jnp.where(has_d, first_d[img].astype(F32) if raw else act(halo_d[par, img], raw), 0.0)
            else:
                v = act(z[img, p - 1], raw)
            base = p * wide + EDGE
            buf[base:base + pairs, :] = v
            out.append((p, base, v))
        return out

    def build_pairs(t, par, u, k, raw, first_p=0):
        n_q = half + 1
        for p, base, own in fill_lines(t, par, u, k, rows, raw, first_p):
            side = jnp.where(lane < ch, lines[k][base + 1:base + 1 + pairs, :], lines[k][base - 1:base - 1 + pairs, :])
            bufs[k][2 * (p % 2) * n_q + p // 2] = own.astype(BF16)
            bufs[k][(2 * (p % 2) + 1) * n_q + p // 2] = side.astype(BF16)

    def build_wide(t, par, u, k):
        n_q = quarter + 1
        for p, base, own in fill_lines(t, par, u, k, half, False, 0):
            at = 3 * (p % 2) * n_q + p // 2
            bufs[k][at] = lines[k][base - 1:base - 1 + pairs, :].astype(BF16)
            bufs[k][at + n_q] = own.astype(BF16)
            bufs[k][at + 2 * n_q] = lines[k][base + 1:base + 1 + pairs, :].astype(BF16)

    def finish_conv(img, i0, o, dst=z):
        folded = o.reshape(o.shape[0] // 8, 8, 256)
        s = jnp.sum(folded, axis=0)
        q = jnp.sum(folded * folded, axis=0)
        acc[0] += jnp.concatenate([s[:, :128], q[:, :128]], axis=1)
        acc[1] += jnp.concatenate([s[:, 128:], q[:, 128:]], axis=1)
        for i in range(o.shape[0] // pairs):
            dst[img, 2 * (i0 + i)] = o[i * pairs:(i + 1) * pairs, :128]
            dst[img, 2 * (i0 + i) + 1] = o[i * pairs:(i + 1) * pairs, 128:]

    def dot(parts):
        lhs = jnp.concatenate(parts, axis=1)
        rhs = jnp.concatenate([wmat[0, 0:lhs.shape[1]], wmat[1, 0:lhs.shape[1]]], axis=1)
        return jnp.dot(lhs, rhs, preferred_element_type=F32)

    def join(k, slots, size, n):
        return [jnp.concatenate([block for a in range(n) for block in size(bufs[k + a], j)], axis=0) for j in slots]

    def conv_pairs(t, u, k, par_out, n):
        slots = [c * (half + 1) + lo for lo in (0, 1) for c in range(4)]
        o = dot(join(k, slots, lambda buf, j: [buf[j:j + half].reshape(half * pairs, 128)], n))
        for a in range(n):
            finish_conv(t * UNROLL + u + a, 0, o[a * half * pairs:(a + 1) * half * pairs])
            save_edges(t, u + a, rows, par_out)

    def conv_down(t, u, k, par_out, n):
        slots = [c * (half + 1) + j for j, c in ((0, 2), (0, 3), (1, 0), (1, 1), (1, 2), (1, 3), (2, 0), (2, 1), (2, 2), (2, 3))]
        o = dot(join(k, slots, lambda buf, j: [buf[j + 2 * i] for i in range(quarter)], n))
        for a in range(n):
            finish_conv(t * UNROLL + u + a, 0, o[a * quarter * pairs:(a + 1) * quarter * pairs])
            save_edges(t, u + a, half, par_out)

    def conv_wide(t, u, k, par_out, n):
        slots = [c * (quarter + 1) + lo for lo in (0, 1) for c in range(6)]
        o = dot(join(k, slots, lambda buf, j: [buf[j:j + quarter].reshape(quarter * pairs, 128)], n))
        for a in range(n):
            finish_conv(t * UNROLL + u + a, 0, o[a * quarter * pairs:(a + 1) * quarter * pairs], z_out)

    n_steps = n_img // UNROLL

    def run_layer(par, raw, n_rows, build, conv, n_out, par_out, n_join, batches=1):
        acc[...] = jnp.zeros_like(acc)

        def body(step, carry):
            steps = [step * batches + b for b in range(batches)]
            for b, t in enumerate(steps):
                wait_edges(t, par, n_rows, raw)
                prepare_corners(b, t, par, raw)
            for b, t in enumerate(steps):
                for u in range(0, UNROLL, n_join):
                    for a in range(n_join):
                        build(t, u + a, b * UNROLL + u + a)
                    conv(t, u, b * UNROLL + u, par_out, n_join)
            if n_out:
                @pl.when(step < n_steps // batches - 1)
                def _():
                    for t in steps:
                        start_edges(t, par_out, n_out)
            return carry

        lax.fori_loop(0, n_steps // batches, body, 0)
        start_stats(par_out)
        if n_out:
            for b in range(batches):
                start_edges(n_steps - batches + b, par_out, n_out)

    def put_block(k, n_k, blocks):
        for o, blk in enumerate(blocks):
            wmat[o, k * n_k:(k + 1) * n_k, :] = jnp.zeros((n_k, 128), BF16) if blk is None else blk

    def weights_pairs(layer):
        zero = jnp.zeros((ch, ch), BF16)
        q = []
        for kh in range(3):
            w0, w1, w2 = w_a[layer, kh, 0], w_a[layer, kh, 1], w_a[layer, kh, 2]
            q.append(jnp.concatenate([
                jnp.concatenate([w1, w0], axis=1),
                jnp.concatenate([w2, w1], axis=1),
                jnp.concatenate([zero, w2], axis=1),
                jnp.concatenate([w0, zero], axis=1)], axis=0))
        for k in range(4):
            put_block(k, 256, [q[k] if k < 3 else None, q[k - 1] if k > 0 else None])

    def weights_down():
        d = [jnp.concatenate([w_down[kh, 0], w_down[kh, 1], w_down[kh, 2], jnp.zeros((ch, 128), BF16)], axis=0) for kh in range(3)]
        for k in range(5):
            put_block(k, 256, [d[k] if k < 3 else None, d[k - 2] if k >= 2 else None])

    def weights_wide():
        e = [jnp.concatenate([w_b[0, kh, 0], w_b[0, kh, 1], w_b[0, kh, 2]], axis=0) for kh in range(3)]
        for k in range(4):
            put_block(k, 384, [e[k] if k < 3 else None, e[k - 1] if k > 0 else None])

    wrow = lax.broadcasted_iota(jnp.int32, (128, 128), 0)
    wcol = lax.broadcasted_iota(jnp.int32, (128, 128), 1)
    source = jnp.where(wrow < pairs, 2 * wrow, 2 * (wrow - pairs) + 1)
    perm[...] = jnp.where(source == wcol, 1.0, 0.0).astype(BF16)

    def load_images(t, carry):
        x_copy(t).wait()
        for img_u in range(UNROLL):
            img = t * UNROLL + img_u
            for g in range(rows // 4):
                block = xv[img, 4 * g:4 * g + 4].reshape(4 * ch, 128)
                m = lax.dot_general(perm[...], block, (((1,), (1,)), ((), ())), preferred_element_type=F32)
                for b in range(2):
                    even = m[0:pairs, 128 * b:128 * b + 128]
                    odd = m[pairs:2 * pairs, 128 * b:128 * b + 128]
                    r = 4 * g + 2 * b
                    upper = jnp.where(lane < ch, even, pltpu.roll(odd, ch, 1))
                    lower = jnp.where(lane < ch, pltpu.roll(even, ch, 1), odd)
                    z[img, r] = upper
                    z[img, r + 1] = lower
                    if r == 0:
                        edge_u[img] = upper.astype(BF16)
                    if r + 2 == rows:
                        edge_d[img] = lower.astype(BF16)
            save_edges(t, img_u, rows, 0)

        @pl.when(t == 0)
        def _():
            pl.semaphore_wait(barrier, n_dev - 1)

        start_edges(t, 0, rows, True)
        return carry

    lax.fori_loop(0, n_steps, load_images, 0)

    count_a = float(n_dev * n_img * rows * pairs * 2)
    count_b = float(n_dev * n_img * half * pairs)

    for copy in w_copies:
        copy.wait()
    weights_pairs(0)
    run_layer(0, True, rows, lambda t, u, k: build_pairs(t, 0, u, k, True), conv_pairs, rows, 1, JOIN)
    wait_edges_sent(0, rows, True)

    def gains(layer):
        g, s = bn_a[layer, 0:1, :], bn_a[layer, 1:2, :]
        return jnp.concatenate([g, g], axis=1), jnp.concatenate([s, s], axis=1)

    n_layers = w_a.shape[0]

    def a_layer(layer, carry):
        par = lax.rem(layer, 2)
        weights_pairs(layer)
        wait_edges_sent(par, rows)
        wait_stats(par)
        g, s = gains(layer - 1)
        set_constants(par, g, s, count_a, True)
        run_layer(par, False, rows, lambda t, u, k: build_pairs(t, par, u, k, False), conv_pairs, rows, 1 - par, JOIN, BATCHES)
        return carry

    lax.fori_loop(1, n_layers, a_layer, 0)

    par = n_layers % 2
    weights_down()
    wait_edges_sent(par, rows)
    wait_stats(par)
    g, s = gains(n_layers - 1)
    set_constants(par, g, s, count_a, True)
    run_layer(par, False, rows, lambda t, u, k: build_pairs(t, par, u, k, False, 1), conv_down, half, 1 - par, JOIN)

    weights_wide()
    wait_edges_sent(1 - par, half)
    wait_stats(1 - par)
    set_constants(1 - par, bn_down[0:1, :], bn_down[1:2, :], count_b, False)
    run_layer(1 - par, False, half, lambda t, u, k: build_wide(t, 1 - par, u, k), conv_wide, 0, par, JOIN)
    wait_stats(par)
    set_constants(par, bn_b[0, 0:1, :], bn_b[0, 1:2, :], count_b, False)
    cst_out[...] = cst[...]


def finish_kernel(z, cst_ref, out_ref, y, out_sem):
    n_img, n_rows = z.shape[:2]

    def copy(img):
        return pltpu.make_async_copy(y.at[img], out_ref.at[img], out_sem.at[img])

    def step(img, carry):
        for r in range(n_rows):
            y[img, r] = normalise(z[img, r], cst_ref).astype(BF16)
        copy(img).start()
        return carry

    lax.fori_loop(0, n_img, step, 0)
    for img in range(n_img):
        copy(img).wait()


def solution(mesh):
    n_sp, n_sp2 = mesh.shape["sp"], mesh.shape["sp2"]

    def per_device(x, w_a, bn_a, w_down, bn_down, w_b, bn_b):
        n_img, rows, cols, ch = x.shape
        pairs, half = cols // 2, rows // 2
        n_dev = n_sp * n_sp2
        dims = (n_img, rows, pairs, ch, n_sp2, n_sp)
        vmem = pltpu.VMEM
        dma = pltpu.SemaphoreType.DMA
        scratch = [
            vmem((n_img, rows, ch, cols), BF16),
            vmem(w_a.shape, BF16), vmem(w_down.shape, BF16), vmem(w_b.shape, BF16),
            vmem((n_img, rows, pairs, 128), F32),
            [vmem((4 * (half + 1), pairs, 128), BF16) for _ in range(BATCHES * UNROLL)],
            [vmem(((rows + 2) * (pairs + 2 * EDGE), 128), F32) for _ in range(BATCHES * UNROLL)],
            vmem((2, 1536, 128), BF16),
            vmem((128, 128), BF16),
            vmem((n_img, pairs, 128), BF16), vmem((n_img, pairs, 128), BF16),
            vmem((n_img, pairs, 128), BF16), vmem((n_img, pairs, 128), BF16),
            vmem((2, n_img, rows, 128), F32),
            vmem((2, n_img, rows, 128), F32),
            vmem((2, n_img, pairs, 128), F32),
            vmem((2, n_img, pairs, 128), F32),
            vmem((2, n_img, rows, 128), F32),
            vmem((2, n_img, rows, 128), F32),
            vmem((2, 4, n_img // UNROLL, UNROLL, 128), F32),
            vmem((2, 4, n_img // UNROLL, UNROLL, 128), F32),
            vmem((2, 4, UNROLL, 128), F32),
            vmem((2, n_dev, 2, 128), F32),
            vmem((2, 8, 256), F32),
            vmem((8, 128), F32),
            dma((n_img // UNROLL,)),
            dma((3,)),
            dma((2, 2)), dma((2, 2, n_img // UNROLL)),
            dma((2, 2)), dma((2, 2, n_img // UNROLL)),
            dma((2, 4)), dma((2, 4, n_img // UNROLL)),
            dma((n_dev - 1,)), dma((2, n_dev)),
        ]
        in_vmem = pl.BlockSpec(memory_space=pltpu.VMEM)
        in_hbm = pl.BlockSpec(memory_space=pltpu.HBM)
        in_any = pl.BlockSpec(memory_space=pl.ANY)
        z, cst = pl.pallas_call(
            functools.partial(stack_kernel, dims),
            out_shape=(vmem((n_img, half, pairs, 128), F32), vmem((8, 128), F32)),
            in_specs=[in_hbm, in_hbm, in_vmem, in_hbm, in_vmem, in_hbm, in_vmem],
            out_specs=(in_vmem, in_vmem),
            scratch_shapes=scratch,
            compiler_params=pltpu.CompilerParams(collective_id=0, has_side_effects=True, vmem_limit_bytes=VMEM_LIMIT),
        )(jnp.transpose(x, (0, 1, 3, 2)), w_a, bn_a, w_down, bn_down, w_b, bn_b)
        return pl.pallas_call(
            finish_kernel,
            out_shape=jax.ShapeDtypeStruct((n_img, half, pairs, 128), BF16),
            in_specs=[in_vmem, in_vmem],
            out_specs=in_any,
            scratch_shapes=[vmem((n_img, half, pairs, 128), BF16), dma((n_img,))],
            compiler_params=pltpu.CompilerParams(vmem_limit_bytes=16 * 1024 * 1024),
        )(z, cst)

    tile_spec = P("dp", "sp", "sp2", None)
    return jax.shard_map(per_device, mesh=mesh, in_specs=(tile_spec, P(), P(), P(), P(), P(), P()), out_specs=tile_spec, check_vma=False)
```

```python
import functools

import jax
import jax.numpy as jnp
from jax import lax
from jax.experimental import pallas as pl
from jax.experimental.pallas import tpu as pltpu
from jax.sharding import PartitionSpec as P

MESH = pl.DeviceIdType.MESH
F32 = jnp.float32
BF16 = jnp.bfloat16
EPS = 1e-5
UNROLL = 4
BATCHES = 2
JOINS = (2, 2)
LONG_JOINS = (1, 1, 2, 2, 2)
VMEM_LIMIT = 51 * 1024 * 1024
EDGE = 8


def normalise(v, cst):
    return jnp.maximum((v - cst[0:1, :]) * cst[1:2, :] + cst[2:3, :], 0.0)


def stack_kernel(dims, x_ref, w_a_ref, bn_a, w_down_ref, bn_down, w_b_ref, bn_b, z_out, cst_out,
                 xv, w_a, w_down, w_b, z, bufs, lines, wmat, perm, edge_u, edge_d, first_u, first_d, edge_l, edge_r, halo_u, halo_d, halo_l, halo_r,
                 corner_s, corner_r, corner_n, stats, acc, cst,
                 x_sem, w_sem, row_send, row_recv, col_send, col_recv, cor_send, cor_recv, st_send, st_recv):
    n_img, rows, pairs, ch, n_sp2, n_sp = dims
    half, quarter = rows // 2, rows // 4
    wide = pairs + EDGE
    data = pl.ds(0, pairs)
    n_dev = n_sp2 * n_sp
    sp = lax.axis_index("sp")
    sp2 = lax.axis_index("sp2")
    me = sp2 * n_sp + sp
    has_u, has_d = sp > 0, sp < n_sp - 1
    has_l, has_r = sp2 > 0, sp2 < n_sp2 - 1

    def x_copy(t):
        some = pl.ds(t * UNROLL, UNROLL)
        return pltpu.make_async_copy(x_ref.at[some], xv.at[some], x_sem.at[t])

    for t in range(n_img // UNROLL):
        x_copy(t).start()

    w_copies = [pltpu.make_async_copy(src, dst, w_sem.at[i]) for i, (src, dst) in enumerate(((w_a_ref, w_a), (w_down_ref, w_down), (w_b_ref, w_b)))]
    for copy in w_copies:
        copy.start()

    barrier = pltpu.get_barrier_semaphore()
    for d in range(1, n_dev):
        peer = lax.rem(me + d, n_dev)
        pl.semaphore_signal(barrier, inc=1, device_id={"sp2": peer // n_sp, "sp": lax.rem(peer, n_sp)}, device_id_type=MESH)

    def rcopy(src, dst, ssem, rsem, to_sp2, to_sp):
        return pltpu.make_async_remote_copy(src_ref=src, dst_ref=dst, send_sem=ssem, recv_sem=rsem,
                                            device_id={"sp2": to_sp2, "sp": to_sp}, device_id_type=MESH)

    corner_to = ((has_u & has_l, -1, -1, 3), (has_u & has_r, 1, -1, 2), (has_d & has_l, -1, 1, 1), (has_d & has_r, 1, 1, 0))

    def start_edges(t, par, n_rows, first=False):
        some, r_all = pl.ds(t * UNROLL, UNROLL), pl.ds(0, n_rows)

        @pl.when(has_l)
        def _():
            rcopy(edge_l.at[par, some, r_all], halo_r.at[par, some, r_all], col_send.at[par, 0], col_recv.at[par, 1, t], sp2 - 1, sp).start()

        @pl.when(has_r)
        def _():
            rcopy(edge_r.at[par, some, r_all], halo_l.at[par, some, r_all], col_send.at[par, 1], col_recv.at[par, 0, t], sp2 + 1, sp).start()

        for c, (there, d_sp2, d_sp, slot) in enumerate(corner_to):
            @pl.when(there)
            def _():
                rcopy(corner_s.at[par, c, t], corner_r.at[par, slot, t], cor_send.at[par, c], cor_recv.at[par, slot, t], sp2 + d_sp2, sp + d_sp).start()

        @pl.when(has_u)
        def _():
            src, dst = (edge_u.at[some], first_d.at[some]) if first else (z.at[some, 0, data], halo_d.at[par, some])
            rcopy(src, dst, row_send.at[par, 0], row_recv.at[par, 1, t], sp2, sp - 1).start()

        @pl.when(has_d)
        def _():
            src, dst = (edge_d.at[some], first_u.at[some]) if first else (z.at[some, n_rows - 1, data], halo_u.at[par, some])
            rcopy(src, dst, row_send.at[par, 1], row_recv.at[par, 0, t], sp2, sp + 1).start()

    def wait_edges(t, par, n_rows, first=False):
        some, r_all = pl.ds(t * UNROLL, UNROLL), pl.ds(0, n_rows)

        @pl.when(has_u)
        def _():
            src, dst = (edge_u.at[some], first_u.at[some]) if first else (z.at[some, 0, data], halo_u.at[par, some])
            rcopy(src, dst, row_send.at[par, 0], row_recv.at[par, 0, t], sp2, sp).wait_recv()

        @pl.when(has_d)
        def _():
            src, dst = (edge_d.at[some], first_d.at[some]) if first else (z.at[some, n_rows - 1, data], halo_d.at[par, some])
            rcopy(src, dst, row_send.at[par, 1], row_recv.at[par, 1, t], sp2, sp).wait_recv()

        @pl.when(has_l)
        def _():
            rcopy(edge_l.at[par, some, r_all], halo_l.at[par, some, r_all], col_send.at[par, 0], col_recv.at[par, 0, t], sp2, sp).wait_recv()

        @pl.when(has_r)
        def _():
            rcopy(edge_r.at[par, some, r_all], halo_r.at[par, some, r_all], col_send.at[par, 1], col_recv.at[par, 1, t], sp2, sp).wait_recv()

        for c, (there, d_sp2, d_sp, slot) in enumerate(corner_to):
            @pl.when(there)
            def _():
                rcopy(corner_s.at[par, c, t], corner_r.at[par, c, t], cor_send.at[par, c], cor_recv.at[par, c, t], sp2, sp).wait_recv()

    def wait_edges_sent(par, n_rows, first=False):
        r_all = pl.ds(0, n_rows)
        every = pl.ds(0, n_img)

        @pl.when(has_u)
        def _():
            src, dst = (edge_u, first_u) if first else (z.at[every, 0, data], halo_u.at[0])
            rcopy(src, dst, row_send.at[par, 0], row_recv.at[0, 0, 0], sp2, sp).wait_send()

        @pl.when(has_d)
        def _():
            src, dst = (edge_d, first_d) if first else (z.at[every, n_rows - 1, data], halo_d.at[0])
            rcopy(src, dst, row_send.at[par, 1], row_recv.at[0, 1, 0], sp2, sp).wait_send()

        @pl.when(has_l)
        def _():
            rcopy(edge_l.at[par, every, r_all], halo_l.at[0, every, r_all], col_send.at[par, 0], col_recv.at[0, 0, 0], sp2, sp).wait_send()

        @pl.when(has_r)
        def _():
            rcopy(edge_r.at[par, every, r_all], halo_r.at[0, every, r_all], col_send.at[par, 1], col_recv.at[0, 1, 0], sp2, sp).wait_send()

        for c, (there, d_sp2, d_sp, slot) in enumerate(corner_to):
            @pl.when(there)
            def _():
                rcopy(corner_s.at[par, c], corner_r.at[0, c], cor_send.at[par, c], cor_recv.at[0, c, 0], sp2, sp).wait_send()

    def stat_copy(d, par):
        peer = lax.rem(me + d, n_dev)
        return rcopy(stats.at[par, me], stats.at[par, me], st_send.at[d - 1], st_recv.at[par, me], peer // n_sp, lax.rem(peer, n_sp))

    def start_stats(par):
        total = acc[0] + acc[1]
        stats[par, me] = jnp.concatenate([jnp.sum(total[:, :128], axis=0, keepdims=True), jnp.sum(total[:, 128:], axis=0, keepdims=True)], axis=0)
        for d in range(1, n_dev):
            stat_copy(d, par).start()

    def wait_stats(par):
        for d in range(1, n_dev):
            stat_copy(d, par).wait_send()
        for d in range(1, n_dev):
            src = lax.rem(me + d, n_dev)
            rcopy(stats.at[par, src], stats.at[par, src], st_send.at[d - 1], st_recv.at[par, src], sp2, sp).wait_recv()

    def set_constants(par, gain, shift, count, paired):
        parts = [stats[par, src] for src in range(n_dev)]
        while len(parts) > 1:
            parts = [a + b for a, b in zip(parts[0::2], parts[1::2])]
        total = parts[0]
        if paired:
            total = total + pltpu.roll(total, ch, 1)
        mean = total[0:1] * (1.0 / count)
        var = total[1:2] * (1.0 / count) - mean * mean
        cst[0:1, :] = mean
        cst[1:2, :] = gain * lax.rsqrt(var + EPS)
        cst[2:3, :] = shift

    lane = lax.broadcasted_iota(jnp.int32, (pairs, 128), 1)

    def save_edges(t, u, n_rows, par):
        img = t * UNROLL + u
        flat = z.at[img].reshape(rows * wide, 128)
        first = flat[pl.ds(0, n_rows, stride=wide), :]
        final = flat[pl.ds(pairs - 1, n_rows, stride=wide), :]
        edge_l[par, img, 0:n_rows, :] = first
        edge_r[par, img, 0:n_rows, :] = final
        corner_s[par, 0, t, u:u + 1, :] = first[0:1]
        corner_s[par, 1, t, u:u + 1, :] = final[0:1]
        corner_s[par, 2, t, u:u + 1, :] = first[n_rows - 1:n_rows]
        corner_s[par, 3, t, u:u + 1, :] = final[n_rows - 1:n_rows]

    def act(v, raw):
        return v if raw else normalise(v, cst)

    def prepare_corners(b, t, par, raw):
        for c, (there, d_sp2, d_sp, slot) in enumerate(corner_to):
            corner_n[b, c] = jnp.where(there, act(corner_r[par, c, t], raw), 0.0)

    def fill_lines(t, par, u, k, n_rows, raw, first_p):
        buf, img, b = lines[k], t * UNROLL + u, k // UNROLL
        left = jnp.where(has_l, act(halo_l[par, img, 0:n_rows, :], raw), 0.0)
        right = jnp.where(has_r, act(halo_r[par, img, 0:n_rows, :], raw), 0.0)
        buf[pl.ds(wide + EDGE - 1, n_rows, stride=wide), :] = left
        buf[pl.ds(wide + EDGE + pairs, n_rows, stride=wide), :] = right
        bottom = (n_rows + 1) * wide
        buf[EDGE - 1:EDGE, :] = corner_n[b, 0, u:u + 1, :]
        buf[EDGE + pairs:EDGE + pairs + 1, :] = corner_n[b, 1, u:u + 1, :]
        buf[bottom + EDGE - 1:bottom + EDGE, :] = corner_n[b, 2, u:u + 1, :]
        buf[bottom + EDGE + pairs:bottom + EDGE + pairs + 1, :] = corner_n[b, 3, u:u + 1, :]
        out = []
        for p in range(first_p, n_rows + 2):
            if p == 0:
                v = jnp.where(has_u, first_u[img].astype(F32) if raw else act(halo_u[par, img], raw), 0.0)
            elif p == n_rows + 1:
                v = jnp.where(has_d, first_d[img].astype(F32) if raw else act(halo_d[par, img], raw), 0.0)
            else:
                v = act(z[img, p - 1, 0:pairs], raw)
            base = p * wide + EDGE
            buf[base:base + pairs, :] = v
            out.append((p, base, v))
        return out

    def build_pairs(t, par, u, k, raw, first_p=0):
        n_q = half + 1
        for p, base, own in fill_lines(t, par, u, k, rows, raw, first_p):
            side = jnp.where(lane < ch, lines[k][base + 1:base + 1 + pairs, :], lines[k][base - 1:base - 1 + pairs, :])
            bufs[k][2 * (p % 2) * n_q + p // 2] = own.astype(BF16)
            bufs[k][(2 * (p % 2) + 1) * n_q + p // 2] = side.astype(BF16)

    def build_wide(t, par, u, k):
        n_q = quarter + 1
        for p, base, own in fill_lines(t, par, u, k, half, False, 0):
            at = 3 * (p % 2) * n_q + p // 2
            bufs[k][at] = lines[k][base - 1:base - 1 + pairs, :].astype(BF16)
            bufs[k][at + n_q] = own.astype(BF16)
            bufs[k][at + 2 * n_q] = lines[k][base + 1:base + 1 + pairs, :].astype(BF16)

    def finish_conv(img, i0, o, dst=z):
        folded = o.reshape(o.shape[0] // 8, 8, 256)
        s = jnp.sum(folded, axis=0)
        q = jnp.sum(folded * folded, axis=0)
        acc[0] += jnp.concatenate([s[:, :128], q[:, :128]], axis=1)
        acc[1] += jnp.concatenate([s[:, 128:], q[:, 128:]], axis=1)
        for i in range(o.shape[0] // pairs):
            dst[img, 2 * (i0 + i), 0:pairs] = o[i * pairs:(i + 1) * pairs, :128]
            dst[img, 2 * (i0 + i) + 1, 0:pairs] = o[i * pairs:(i + 1) * pairs, 128:]

    def dot(parts):
        lhs = jnp.concatenate(parts, axis=1)
        rhs = jnp.concatenate([wmat[0, 0:lhs.shape[1]], wmat[1, 0:lhs.shape[1]]], axis=1)
        return jnp.dot(lhs, rhs, preferred_element_type=F32)

    def join(k, slots, size, n):
        return [jnp.concatenate([block for a in range(n) for block in size(bufs[k + a], j)], axis=0) for j in slots]

    def conv_pairs(t, u, k, par_out, n):
        slots = [c * (half + 1) + lo for lo in (0, 1) for c in range(4)]
        o = dot(join(k, slots, lambda buf, j: [buf[j:j + half].reshape(half * pairs, 128)], n))
        for a in range(n):
            finish_conv(t * UNROLL + u + a, 0, o[a * half * pairs:(a + 1) * half * pairs])
            save_edges(t, u + a, rows, par_out)

    def conv_down(t, u, k, par_out, n):
        slots = [c * (half + 1) + j for j, c in ((0, 2), (0, 3), (1, 0), (1, 1), (1, 2), (1, 3), (2, 0), (2, 1), (2, 2), (2, 3))]
        o = dot(join(k, slots, lambda buf, j: [buf[j + 2 * i] for i in range(quarter)], n))
        for a in range(n):
            finish_conv(t * UNROLL + u + a, 0, o[a * quarter * pairs:(a + 1) * quarter * pairs])
            save_edges(t, u + a, half, par_out)

    def conv_wide(t, u, k, par_out, n):
        slots = [c * (quarter + 1) + lo for lo in (0, 1) for c in range(6)]
        o = dot(join(k, slots, lambda buf, j: [buf[j:j + quarter].reshape(quarter * pairs, 128)], n))
        for a in range(n):
            finish_conv(t * UNROLL + u + a, 0, o[a * quarter * pairs:(a + 1) * quarter * pairs], z_out)

    n_steps = n_img // UNROLL

    def run_layer(par, raw, n_rows, build, conv, n_out, par_out, constants, joins, batches=1):
        acc[...] = jnp.zeros_like(acc)
        for t in range(batches):
            wait_edges(t, par, n_rows, raw)
        constants()

        def body(step, carry):
            steps = [step * batches + b for b in range(batches)]

            @pl.when(step > 0)
            def _():
                for t in steps:
                    wait_edges(t, par, n_rows, raw)

            for b, t in enumerate(steps):
                prepare_corners(b, t, par, raw)
            k = 0
            for n in joins:
                t, u = steps[k // UNROLL], k % UNROLL
                for a in range(n):
                    build(t, u + a, k + a)
                conv(t, u, k, par_out, n)
                k += n
            if n_out:
                @pl.when(step < n_steps // batches - 1)
                def _():
                    for t in steps:
                        start_edges(t, par_out, n_out)
            return carry

        lax.fori_loop(0, n_steps // batches, body, 0)
        start_stats(par_out)
        if n_out:
            for b in range(batches):
                start_edges(n_steps - batches + b, par_out, n_out)

    def put_block(k, n_k, blocks):
        for o, blk in enumerate(blocks):
            wmat[o, k * n_k:(k + 1) * n_k, :] = jnp.zeros((n_k, 128), BF16) if blk is None else blk

    def weights_pairs(layer):
        zero = jnp.zeros((ch, ch), BF16)
        q = []
        for kh in range(3):
            w0, w1, w2 = w_a[layer, kh, 0], w_a[layer, kh, 1], w_a[layer, kh, 2]
            q.append(jnp.concatenate([
                jnp.concatenate([w1, w0], axis=1),
                jnp.concatenate([w2, w1], axis=1),
                jnp.concatenate([zero, w2], axis=1),
                jnp.concatenate([w0, zero], axis=1)], axis=0))
        for k in range(4):
            put_block(k, 256, [q[k] if k < 3 else None, q[k - 1] if k > 0 else None])

    def weights_down():
        d = [jnp.concatenate([w_down[kh, 0], w_down[kh, 1], w_down[kh, 2], jnp.zeros((ch, 128), BF16)], axis=0) for kh in range(3)]
        for k in range(5):
            put_block(k, 256, [d[k] if k < 3 else None, d[k - 2] if k >= 2 else None])

    def weights_wide():
        e = [jnp.concatenate([w_b[0, kh, 0], w_b[0, kh, 1], w_b[0, kh, 2]], axis=0) for kh in range(3)]
        for k in range(4):
            put_block(k, 384, [e[k] if k < 3 else None, e[k - 1] if k > 0 else None])

    wrow = lax.broadcasted_iota(jnp.int32, (128, 128), 0)
    wcol = lax.broadcasted_iota(jnp.int32, (128, 128), 1)
    source = jnp.where(wrow < pairs, 2 * wrow, 2 * (wrow - pairs) + 1)
    perm[...] = jnp.where(source == wcol, 1.0, 0.0).astype(BF16)

    def load_images(t, carry):
        x_copy(t).wait()
        for img_u in range(UNROLL):
            img = t * UNROLL + img_u
            for g in range(rows // 4):
                block = xv[img, 4 * g:4 * g + 4].reshape(4 * ch, 128)
                m = lax.dot_general(perm[...], block, (((1,), (1,)), ((), ())), preferred_element_type=F32)
                for b in range(2):
                    even = m[0:pairs, 128 * b:128 * b + 128]
                    odd = m[pairs:2 * pairs, 128 * b:128 * b + 128]
                    r = 4 * g + 2 * b
                    upper = jnp.where(lane < ch, even, pltpu.roll(odd, ch, 1))
                    lower = jnp.where(lane < ch, pltpu.roll(even, ch, 1), odd)
                    z[img, r, 0:pairs] = upper
                    z[img, r + 1, 0:pairs] = lower
                    if r == 0:
                        edge_u[img] = upper.astype(BF16)
                    if r + 2 == rows:
                        edge_d[img] = lower.astype(BF16)
            save_edges(t, img_u, rows, 0)

        @pl.when(t == 0)
        def _():
            pl.semaphore_wait(barrier, n_dev - 1)

        start_edges(t, 0, rows, True)
        return carry

    lax.fori_loop(0, n_steps, load_images, 0)

    count_a = float(n_dev * n_img * rows * pairs * 2)
    count_b = float(n_dev * n_img * half * pairs)

    for copy in w_copies:
        copy.wait()
    weights_pairs(0)
    run_layer(0, True, rows, lambda t, u, k: build_pairs(t, 0, u, k, True), conv_pairs, rows, 1, lambda: None, JOINS)
    wait_edges_sent(0, rows, True)

    def gains(layer):
        g, s = bn_a[layer, 0:1, :], bn_a[layer, 1:2, :]
        return jnp.concatenate([g, g], axis=1), jnp.concatenate([s, s], axis=1)

    n_layers = w_a.shape[0]

    def a_layer(layer, carry):
        par = lax.rem(layer, 2)
        weights_pairs(layer)
        wait_edges_sent(par, rows)

        def constants():
            wait_stats(par)
            g, s = gains(layer - 1)
            set_constants(par, g, s, count_a, True)

        run_layer(par, False, rows, lambda t, u, k: build_pairs(t, par, u, k, False), conv_pairs, rows, 1 - par, constants, LONG_JOINS, BATCHES)
        return carry

    lax.fori_loop(1, n_layers, a_layer, 0)

    par = n_layers % 2
    weights_down()
    wait_edges_sent(par, rows)

    def constants():
        wait_stats(par)
        g, s = gains(n_layers - 1)
        set_constants(par, g, s, count_a, True)

    run_layer(par, False, rows, lambda t, u, k: build_pairs(t, par, u, k, False, 1), conv_down, half, 1 - par, constants, JOINS)

    weights_wide()
    wait_edges_sent(1 - par, half)

    def constants():
        wait_stats(1 - par)
        set_constants(1 - par, bn_down[0:1, :], bn_down[1:2, :], count_b, False)

    run_layer(1 - par, False, half, lambda t, u, k: build_wide(t, 1 - par, u, k), conv_wide, 0, par, constants, JOINS)
    wait_stats(par)
    set_constants(par, bn_b[0, 0:1, :], bn_b[0, 1:2, :], count_b, False)
    cst_out[...] = cst[...]


def finish_kernel(z, cst_ref, out_ref, y, out_sem):
    n_img, n_rows = z.shape[:2]

    def copy(img):
        return pltpu.make_async_copy(y.at[img], out_ref.at[img], out_sem.at[img])

    def step(img, carry):
        for r in range(n_rows):
            y[img, r] = normalise(z[img, r], cst_ref).astype(BF16)
        copy(img).start()
        return carry

    lax.fori_loop(0, n_img, step, 0)
    for img in range(n_img):
        copy(img).wait()


def solution(mesh):
    n_sp, n_sp2 = mesh.shape["sp"], mesh.shape["sp2"]

    def per_device(x, w_a, bn_a, w_down, bn_down, w_b, bn_b):
        n_img, rows, cols, ch = x.shape
        pairs, half = cols // 2, rows // 2
        n_dev = n_sp * n_sp2
        dims = (n_img, rows, pairs, ch, n_sp2, n_sp)
        vmem = pltpu.VMEM
        dma = pltpu.SemaphoreType.DMA
        scratch = [
            vmem((n_img, rows, ch, cols), BF16),
            vmem(w_a.shape, BF16), vmem(w_down.shape, BF16), vmem(w_b.shape, BF16),
            vmem((n_img, rows, pairs + EDGE, 128), F32),
            [vmem((4 * (half + 1), pairs, 128), BF16) for _ in range(BATCHES * UNROLL)],
            [vmem(((rows + 2) * (pairs + EDGE) + EDGE, 128), F32) for _ in range(BATCHES * UNROLL)],
            vmem((2, 1536, 128), BF16),
            vmem((128, 128), BF16),
            vmem((n_img, pairs, 128), BF16), vmem((n_img, pairs, 128), BF16),
            vmem((n_img, pairs, 128), BF16), vmem((n_img, pairs, 128), BF16),
            vmem((2, n_img, rows, 128), F32),
            vmem((2, n_img, rows, 128), F32),
            vmem((2, n_img, pairs, 128), F32),
            vmem((2, n_img, pairs, 128), F32),
            vmem((2, n_img, rows, 128), F32),
            vmem((2, n_img, rows, 128), F32),
            vmem((2, 4, n_img // UNROLL, UNROLL, 128), F32),
            vmem((2, 4, n_img // UNROLL, UNROLL, 128), F32),
            vmem((2, 4, UNROLL, 128), F32),
            vmem((2, n_dev, 2, 128), F32),
            vmem((2, 8, 256), F32),
            vmem((8, 128), F32),
            dma((n_img // UNROLL,)),
            dma((3,)),
            dma((2, 2)), dma((2, 2, n_img // UNROLL)),
            dma((2, 2)), dma((2, 2, n_img // UNROLL)),
            dma((2, 4)), dma((2, 4, n_img // UNROLL)),
            dma((n_dev - 1,)), dma((2, n_dev)),
        ]
        in_vmem = pl.BlockSpec(memory_space=pltpu.VMEM)
        in_hbm = pl.BlockSpec(memory_space=pltpu.HBM)
        in_any = pl.BlockSpec(memory_space=pl.ANY)
        z, cst = pl.pallas_call(
            functools.partial(stack_kernel, dims),
            out_shape=(vmem((n_img, half, pairs, 128), F32), vmem((8, 128), F32)),
            in_specs=[in_hbm, in_hbm, in_vmem, in_hbm, in_vmem, in_hbm, in_vmem],
            out_specs=(in_vmem, in_vmem),
            scratch_shapes=scratch,
            compiler_params=pltpu.CompilerParams(collective_id=0, has_side_effects=True, vmem_limit_bytes=VMEM_LIMIT),
        )(jnp.transpose(x, (0, 1, 3, 2)), w_a, bn_a, w_down, bn_down, w_b, bn_b)
        return pl.pallas_call(
            finish_kernel,
            out_shape=jax.ShapeDtypeStruct((n_img, half, pairs, 128), BF16),
            in_specs=[in_vmem, in_vmem],
            out_specs=in_any,
            scratch_shapes=[vmem((n_img, half, pairs, 128), BF16), dma((n_img,))],
            compiler_params=pltpu.CompilerParams(vmem_limit_bytes=16 * 1024 * 1024),
        )(z, cst)

    tile_spec = P("dp", "sp", "sp2", None)
    return jax.shard_map(per_device, mesh=mesh, in_specs=(tile_spec, P(), P(), P(), P(), P(), P()), out_specs=tile_spec, check_vma=False)
```

```python
import functools

import jax
import jax.numpy as jnp
from jax import lax
from jax.experimental import pallas as pl
from jax.experimental.pallas import tpu as pltpu
from jax.sharding import PartitionSpec as P

MESH = pl.DeviceIdType.MESH
F32 = jnp.float32
BF16 = jnp.bfloat16
EPS = 1e-5
UNROLL = 4
BATCHES = 2
JOINS = (2, 2)
LONG_JOINS = (1, 1, 2, 2, 2)
VMEM_LIMIT = 51 * 1024 * 1024
EDGE = 8


def normalise(v, cst):
    return jnp.maximum((v - cst[0:1, :]) * cst[1:2, :] + cst[2:3, :], 0.0)


def stack_kernel(dims, x_ref, w_a_ref, bn_a, w_down_ref, bn_down, w_b_ref, bn_b, z_out, cst_out,
                 xv, w_a, w_down, w_b, z, bufs, lines, wmat, perm, edge_u, edge_d, first_u, first_d, edge_l, edge_r, halo_u, halo_d, halo_l, halo_r,
                 corner_s, corner_r, corner_n, stats, acc, cst,
                 x_sem, w_sem, row_send, row_recv, col_send, col_recv, cor_send, cor_recv, st_send, st_recv):
    n_img, rows, pairs, ch, n_sp2, n_sp = dims
    half, quarter = rows // 2, rows // 4
    wide = pairs + EDGE
    data = pl.ds(0, pairs)
    n_dev = n_sp2 * n_sp
    sp = lax.axis_index("sp")
    sp2 = lax.axis_index("sp2")
    me = sp2 * n_sp + sp
    has_u, has_d = sp > 0, sp < n_sp - 1
    has_l, has_r = sp2 > 0, sp2 < n_sp2 - 1

    def x_copy(t):
        some = pl.ds(t * UNROLL, UNROLL)
        return pltpu.make_async_copy(x_ref.at[some], xv.at[some], x_sem.at[t])

    for t in range(n_img // UNROLL):
        x_copy(t).start()

    w_copies = [pltpu.make_async_copy(src, dst, w_sem.at[i]) for i, (src, dst) in enumerate(((w_a_ref, w_a), (w_down_ref, w_down), (w_b_ref, w_b)))]
    for copy in w_copies:
        copy.start()

    barrier = pltpu.get_barrier_semaphore()
    for d in range(1, n_dev):
        peer = lax.rem(me + d, n_dev)
        pl.semaphore_signal(barrier, inc=1, device_id={"sp2": peer // n_sp, "sp": lax.rem(peer, n_sp)}, device_id_type=MESH)

    def rcopy(src, dst, ssem, rsem, to_sp2, to_sp):
        return pltpu.make_async_remote_copy(src_ref=src, dst_ref=dst, send_sem=ssem, recv_sem=rsem,
                                            device_id={"sp2": to_sp2, "sp": to_sp}, device_id_type=MESH)

    corner_to = ((has_u & has_l, -1, -1, 3), (has_u & has_r, 1, -1, 2), (has_d & has_l, -1, 1, 1), (has_d & has_r, 1, 1, 0))

    def start_edges(t, par, n_rows, first=False):
        some, r_all = pl.ds(t * UNROLL, UNROLL), pl.ds(0, n_rows)

        @pl.when(has_l)
        def _():
            rcopy(edge_l.at[par, some, r_all], halo_r.at[par, some, r_all], col_send.at[par, 0], col_recv.at[par, 1, t], sp2 - 1, sp).start()

        @pl.when(has_r)
        def _():
            rcopy(edge_r.at[par, some, r_all], halo_l.at[par, some, r_all], col_send.at[par, 1], col_recv.at[par, 0, t], sp2 + 1, sp).start()

        for c, (there, d_sp2, d_sp, slot) in enumerate(corner_to):
            @pl.when(there)
            def _():
                rcopy(corner_s.at[par, c, t], corner_r.at[par, slot, t], cor_send.at[par, c], cor_recv.at[par, slot, t], sp2 + d_sp2, sp + d_sp).start()

        @pl.when(has_u)
        def _():
            src, dst = (edge_u.at[some], first_d.at[some]) if first else (z.at[some, 0, data], halo_d.at[par, some])
            rcopy(src, dst, row_send.at[par, 0], row_recv.at[par, 1, t], sp2, sp - 1).start()

        @pl.when(has_d)
        def _():
            src, dst = (edge_d.at[some], first_u.at[some]) if first else (z.at[some, n_rows - 1, data], halo_u.at[par, some])
            rcopy(src, dst, row_send.at[par, 1], row_recv.at[par, 0, t], sp2, sp + 1).start()

    def wait_edges(t, par, n_rows, first=False):
        some, r_all = pl.ds(t * UNROLL, UNROLL), pl.ds(0, n_rows)

        @pl.when(has_u)
        def _():
            src, dst = (edge_u.at[some], first_u.at[some]) if first else (z.at[some, 0, data], halo_u.at[par, some])
            rcopy(src, dst, row_send.at[par, 0], row_recv.at[par, 0, t], sp2, sp).wait_recv()

        @pl.when(has_d)
        def _():
            src, dst = (edge_d.at[some], first_d.at[some]) if first else (z.at[some, n_rows - 1, data], halo_d.at[par, some])
            rcopy(src, dst, row_send.at[par, 1], row_recv.at[par, 1, t], sp2, sp).wait_recv()

        @pl.when(has_l)
        def _():
            rcopy(edge_l.at[par, some, r_all], halo_l.at[par, some, r_all], col_send.at[par, 0], col_recv.at[par, 0, t], sp2, sp).wait_recv()

        @pl.when(has_r)
        def _():
            rcopy(edge_r.at[par, some, r_all], halo_r.at[par, some, r_all], col_send.at[par, 1], col_recv.at[par, 1, t], sp2, sp).wait_recv()

        for c, (there, d_sp2, d_sp, slot) in enumerate(corner_to):
            @pl.when(there)
            def _():
                rcopy(corner_s.at[par, c, t], corner_r.at[par, c, t], cor_send.at[par, c], cor_recv.at[par, c, t], sp2, sp).wait_recv()

    def wait_edges_sent(par, n_rows, first=False):
        r_all = pl.ds(0, n_rows)
        every = pl.ds(0, n_img)

        @pl.when(has_u)
        def _():
            src, dst = (edge_u, first_u) if first else (z.at[every, 0, data], halo_u.at[0])
            rcopy(src, dst, row_send.at[par, 0], row_recv.at[0, 0, 0], sp2, sp).wait_send()

        @pl.when(has_d)
        def _():
            src, dst = (edge_d, first_d) if first else (z.at[every, n_rows - 1, data], halo_d.at[0])
            rcopy(src, dst, row_send.at[par, 1], row_recv.at[0, 1, 0], sp2, sp).wait_send()

        @pl.when(has_l)
        def _():
            rcopy(edge_l.at[par, every, r_all], halo_l.at[0, every, r_all], col_send.at[par, 0], col_recv.at[0, 0, 0], sp2, sp).wait_send()

        @pl.when(has_r)
        def _():
            rcopy(edge_r.at[par, every, r_all], halo_r.at[0, every, r_all], col_send.at[par, 1], col_recv.at[0, 1, 0], sp2, sp).wait_send()

        for c, (there, d_sp2, d_sp, slot) in enumerate(corner_to):
            @pl.when(there)
            def _():
                rcopy(corner_s.at[par, c], corner_r.at[0, c], cor_send.at[par, c], cor_recv.at[0, c, 0], sp2, sp).wait_send()

    def stat_copy(d, par):
        peer = lax.rem(me + d, n_dev)
        return rcopy(stats.at[par, me], stats.at[par, me], st_send.at[d - 1], st_recv.at[par, me], peer // n_sp, lax.rem(peer, n_sp))

    def start_stats(par):
        total = acc[0] + acc[1]
        stats[par, me] = jnp.concatenate([jnp.sum(total[:, :128], axis=0, keepdims=True), jnp.sum(total[:, 128:], axis=0, keepdims=True)], axis=0)
        for d in range(1, n_dev):
            stat_copy(d, par).start()

    def wait_stats(par):
        for d in range(1, n_dev):
            stat_copy(d, par).wait_send()
        for d in range(1, n_dev):
            src = lax.rem(me + d, n_dev)
            rcopy(stats.at[par, src], stats.at[par, src], st_send.at[d - 1], st_recv.at[par, src], sp2, sp).wait_recv()

    def set_constants(par, gain, shift, count, paired):
        parts = [stats[par, src] for src in range(n_dev)]
        while len(parts) > 1:
            parts = [a + b for a, b in zip(parts[0::2], parts[1::2])]
        total = parts[0]
        if paired:
            total = total + pltpu.roll(total, ch, 1)
        mean = total[0:1] * (1.0 / count)
        var = total[1:2] * (1.0 / count) - mean * mean
        cst[0:1, :] = mean
        cst[1:2, :] = gain * lax.rsqrt(var + EPS)
        cst[2:3, :] = shift

    lane = lax.broadcasted_iota(jnp.int32, (pairs, 128), 1)

    def save_edges(t, u, n_rows, par):
        img = t * UNROLL + u
        flat = z.at[img].reshape(rows * wide, 128)
        first = flat[pl.ds(0, n_rows, stride=wide), :]
        final = flat[pl.ds(pairs - 1, n_rows, stride=wide), :]
        edge_l[par, img, 0:n_rows, :] = first
        edge_r[par, img, 0:n_rows, :] = final
        corner_s[par, 0, t, u:u + 1, :] = first[0:1]
        corner_s[par, 1, t, u:u + 1, :] = final[0:1]
        corner_s[par, 2, t, u:u + 1, :] = first[n_rows - 1:n_rows]
        corner_s[par, 3, t, u:u + 1, :] = final[n_rows - 1:n_rows]

    def act(v, raw):
        return v if raw else normalise(v, cst)

    def prepare_corners(b, t, par, raw):
        for c, (there, d_sp2, d_sp, slot) in enumerate(corner_to):
            corner_n[b, c] = jnp.where(there, act(corner_r[par, c, t], raw), 0.0)

    def fill_lines(t, par, u, k, n_rows, raw, first_p):
        buf, img, b = lines[k], t * UNROLL + u, k // UNROLL
        left = jnp.where(has_l, act(halo_l[par, img, 0:n_rows, :], raw), 0.0)
        right = jnp.where(has_r, act(halo_r[par, img, 0:n_rows, :], raw), 0.0)
        buf[pl.ds(wide + EDGE - 1, n_rows, stride=wide), :] = left
        buf[pl.ds(wide + EDGE + pairs, n_rows, stride=wide), :] = right
        bottom = (n_rows + 1) * wide
        buf[EDGE - 1:EDGE, :] = corner_n[b, 0, u:u + 1, :]
        buf[EDGE + pairs:EDGE + pairs + 1, :] = corner_n[b, 1, u:u + 1, :]
        buf[bottom + EDGE - 1:bottom + EDGE, :] = corner_n[b, 2, u:u + 1, :]
        buf[bottom + EDGE + pairs:bottom + EDGE + pairs + 1, :] = corner_n[b, 3, u:u + 1, :]
        out = []
        for p in range(first_p, n_rows + 2):
            if p == 0:
                v = jnp.where(has_u, first_u[img].astype(F32) if raw else act(halo_u[par, img], raw), 0.0)
            elif p == n_rows + 1:
                v = jnp.where(has_d, first_d[img].astype(F32) if raw else act(halo_d[par, img], raw), 0.0)
            else:
                v = act(z[img, p - 1, 0:pairs], raw)
            base = p * wide + EDGE
            buf[base:base + pairs, :] = v
            out.append((p, base, v))
        return out

    def build_pairs(t, par, u, k, raw, first_p=0):
        n_q = half + 1
        for p, base, own in fill_lines(t, par, u, k, rows, raw, first_p):
            side = jnp.where(lane < ch, lines[k][base + 1:base + 1 + pairs, :], lines[k][base - 1:base - 1 + pairs, :])
            bufs[k][2 * (p % 2) * n_q + p // 2] = own.astype(BF16)
            bufs[k][(2 * (p % 2) + 1) * n_q + p // 2] = side.astype(BF16)

    def build_wide(t, par, u, k):
        n_q = quarter + 1
        for p, base, own in fill_lines(t, par, u, k, half, False, 0):
            at = 3 * (p % 2) * n_q + p // 2
            bufs[k][at] = lines[k][base - 1:base - 1 + pairs, :].astype(BF16)
            bufs[k][at + n_q] = own.astype(BF16)
            bufs[k][at + 2 * n_q] = lines[k][base + 1:base + 1 + pairs, :].astype(BF16)

    def finish_conv(img, i0, o, dst=z):
        folded = o.reshape(o.shape[0] // 8, 8, 256)
        s = jnp.sum(folded, axis=0)
        q = jnp.sum(folded * folded, axis=0)
        acc[0] += jnp.concatenate([s[:, :128], q[:, :128]], axis=1)
        acc[1] += jnp.concatenate([s[:, 128:], q[:, 128:]], axis=1)
        for i in range(o.shape[0] // pairs):
            dst[img, 2 * (i0 + i), 0:pairs] = o[i * pairs:(i + 1) * pairs, :128]
            dst[img, 2 * (i0 + i) + 1, 0:pairs] = o[i * pairs:(i + 1) * pairs, 128:]

    def dot(parts):
        lhs = jnp.concatenate(parts, axis=1)
        rhs = jnp.concatenate([wmat[0, 0:lhs.shape[1]], wmat[1, 0:lhs.shape[1]]], axis=1)
        return jnp.dot(lhs, rhs, preferred_element_type=F32)

    def join(k, slots, size, n):
        return [jnp.concatenate([block for a in range(n) for block in size(bufs[k + a], j)], axis=0) for j in slots]

    def conv_pairs(t, u, k, par_out, n):
        slots = [c * (half + 1) + lo for lo in (0, 1) for c in range(4)]
        o = dot(join(k, slots, lambda buf, j: [buf[j:j + half].reshape(half * pairs, 128)], n))
        for a in range(n):
            finish_conv(t * UNROLL + u + a, 0, o[a * half * pairs:(a + 1) * half * pairs])
            save_edges(t, u + a, rows, par_out)

    def conv_down(t, u, k, par_out, n):
        slots = [c * (half + 1) + j for j, c in ((0, 2), (0, 3), (1, 0), (1, 1), (1, 2), (1, 3), (2, 0), (2, 1), (2, 2), (2, 3))]
        o = dot(join(k, slots, lambda buf, j: [buf[j + 2 * i] for i in range(quarter)], n))
        for a in range(n):
            finish_conv(t * UNROLL + u + a, 0, o[a * quarter * pairs:(a + 1) * quarter * pairs])
            save_edges(t, u + a, half, par_out)

    def conv_wide(t, u, k, par_out, n):
        slots = [c * (quarter + 1) + lo for lo in (0, 1) for c in range(6)]
        o = dot(join(k, slots, lambda buf, j: [buf[j:j + quarter].reshape(quarter * pairs, 128)], n))
        for a in range(n):
            finish_conv(t * UNROLL + u + a, 0, o[a * quarter * pairs:(a + 1) * quarter * pairs], z_out)

    n_steps = n_img // UNROLL

    def run_layer(par, raw, n_rows, build, conv, n_out, par_out, constants, joins, batches=1):
        acc[...] = jnp.zeros_like(acc)
        for t in range(batches):
            wait_edges(t, par, n_rows, raw)
        constants()

        def body(step, carry):
            steps = [step * batches + b for b in range(batches)]

            @pl.when(step > 0)
            def _():
                for t in steps:
                    wait_edges(t, par, n_rows, raw)

            for b, t in enumerate(steps):
                prepare_corners(b, t, par, raw)
            k = 0
            for n in joins:
                t, u = steps[k // UNROLL], k % UNROLL
                for a in range(n):
                    build(t, u + a, k + a)
                conv(t, u, k, par_out, n)
                k += n
            if n_out:
                @pl.when(step < n_steps // batches - 1)
                def _():
                    for t in steps:
                        start_edges(t, par_out, n_out)
            return carry

        lax.fori_loop(0, n_steps // batches, body, 0)
        start_stats(par_out)
        if n_out:
            for b in range(batches):
                start_edges(n_steps - batches + b, par_out, n_out)

    def put_block(k, n_k, blocks):
        for o, blk in enumerate(blocks):
            wmat[o, k * n_k:(k + 1) * n_k, :] = jnp.zeros((n_k, 128), BF16) if blk is None else blk

    def weights_pairs(layer):
        zero = jnp.zeros((ch, ch), BF16)
        q = []
        for kh in range(3):
            w0, w1, w2 = w_a[layer, kh, 0], w_a[layer, kh, 1], w_a[layer, kh, 2]
            q.append(jnp.concatenate([
                jnp.concatenate([w1, w0], axis=1),
                jnp.concatenate([w2, w1], axis=1),
                jnp.concatenate([zero, w2], axis=1),
                jnp.concatenate([w0, zero], axis=1)], axis=0))
        for k in range(4):
            put_block(k, 256, [q[k] if k < 3 else None, q[k - 1] if k > 0 else None])

    def weights_down():
        d = [jnp.concatenate([w_down[kh, 0], w_down[kh, 1], w_down[kh, 2], jnp.zeros((ch, 128), BF16)], axis=0) for kh in range(3)]
        for k in range(5):
            put_block(k, 256, [d[k] if k < 3 else None, d[k - 2] if k >= 2 else None])

    def weights_wide():
        e = [jnp.concatenate([w_b[0, kh, 0], w_b[0, kh, 1], w_b[0, kh, 2]], axis=0) for kh in range(3)]
        for k in range(4):
            put_block(k, 384, [e[k] if k < 3 else None, e[k - 1] if k > 0 else None])

    wrow = lax.broadcasted_iota(jnp.int32, (128, 128), 0)
    wcol = lax.broadcasted_iota(jnp.int32, (128, 128), 1)
    source = jnp.where(wrow < pairs, 2 * wrow, 2 * (wrow - pairs) + 1)
    perm[...] = jnp.where(source == wcol, 1.0, 0.0).astype(BF16)

    def load_images(t, carry):
        x_copy(t).wait()
        for img_u in range(UNROLL):
            img = t * UNROLL + img_u
            for g in range(rows // 4):
                block = xv[img, 4 * g:4 * g + 4].reshape(4 * ch, 128)
                m = lax.dot_general(perm[...], block, (((1,), (1,)), ((), ())), preferred_element_type=F32)
                for b in range(2):
                    even = m[0:pairs, 128 * b:128 * b + 128]
                    odd = m[pairs:2 * pairs, 128 * b:128 * b + 128]
                    r = 4 * g + 2 * b
                    upper = jnp.where(lane < ch, even, pltpu.roll(odd, ch, 1))
                    lower = jnp.where(lane < ch, pltpu.roll(even, ch, 1), odd)
                    z[img, r, 0:pairs] = upper
                    z[img, r + 1, 0:pairs] = lower
                    if r == 0:
                        edge_u[img] = upper.astype(BF16)
                    if r + 2 == rows:
                        edge_d[img] = lower.astype(BF16)
            save_edges(t, img_u, rows, 0)

        @pl.when(t == 0)
        def _():
            pl.semaphore_wait(barrier, n_dev - 1)

        start_edges(t, 0, rows, True)
        return carry

    lax.fori_loop(0, n_steps, load_images, 0)

    count_a = float(n_dev * n_img * rows * pairs * 2)
    count_b = float(n_dev * n_img * half * pairs)

    for copy in w_copies:
        copy.wait()
    weights_pairs(0)
    run_layer(0, True, rows, lambda t, u, k: build_pairs(t, 0, u, k, True), conv_pairs, rows, 1, lambda: None, JOINS)
    wait_edges_sent(0, rows, True)

    def gains(layer):
        g, s = bn_a[layer, 0:1, :], bn_a[layer, 1:2, :]
        return jnp.concatenate([g, g], axis=1), jnp.concatenate([s, s], axis=1)

    n_layers = w_a.shape[0]

    def a_layer(layer, carry):
        par = lax.rem(layer, 2)
        weights_pairs(layer)
        wait_edges_sent(par, rows)

        def constants():
            wait_stats(par)
            g, s = gains(layer - 1)
            set_constants(par, g, s, count_a, True)

        run_layer(par, False, rows, lambda t, u, k: build_pairs(t, par, u, k, False), conv_pairs, rows, 1 - par, constants, LONG_JOINS, BATCHES)
        return carry

    lax.fori_loop(1, n_layers, a_layer, 0)

    par = n_layers % 2
    weights_down()
    wait_edges_sent(par, rows)

    def constants():
        wait_stats(par)
        g, s = gains(n_layers - 1)
        set_constants(par, g, s, count_a, True)

    run_layer(par, False, rows, lambda t, u, k: build_pairs(t, par, u, k, False, 1), conv_down, half, 1 - par, constants, JOINS * 2, BATCHES)

    weights_wide()
    wait_edges_sent(1 - par, half)

    def constants():
        wait_stats(1 - par)
        set_constants(1 - par, bn_down[0:1, :], bn_down[1:2, :], count_b, False)

    run_layer(1 - par, False, half, lambda t, u, k: build_wide(t, 1 - par, u, k), conv_wide, 0, par, constants, JOINS * 2, BATCHES)
    wait_stats(par)
    set_constants(par, bn_b[0, 0:1, :], bn_b[0, 1:2, :], count_b, False)
    cst_out[...] = cst[...]


def finish_kernel(z, cst_ref, out_ref, y, out_sem):
    n_img, n_rows = z.shape[:2]

    def copy(img):
        return pltpu.make_async_copy(y.at[img], out_ref.at[img], out_sem.at[img])

    def step(img, carry):
        for r in range(n_rows):
            y[img, r] = normalise(z[img, r], cst_ref).astype(BF16)
        copy(img).start()
        return carry

    lax.fori_loop(0, n_img, step, 0)
    for img in range(n_img):
        copy(img).wait()


def solution(mesh):
    n_sp, n_sp2 = mesh.shape["sp"], mesh.shape["sp2"]

    def per_device(x, w_a, bn_a, w_down, bn_down, w_b, bn_b):
        n_img, rows, cols, ch = x.shape
        pairs, half = cols // 2, rows // 2
        n_dev = n_sp * n_sp2
        dims = (n_img, rows, pairs, ch, n_sp2, n_sp)
        vmem = pltpu.VMEM
        dma = pltpu.SemaphoreType.DMA
        scratch = [
            vmem((n_img, rows, ch, cols), BF16),
            vmem(w_a.shape, BF16), vmem(w_down.shape, BF16), vmem(w_b.shape, BF16),
            vmem((n_img, rows, pairs + EDGE, 128), F32),
            [vmem((4 * (half + 1), pairs, 128), BF16) for _ in range(BATCHES * UNROLL)],
            [vmem(((rows + 2) * (pairs + EDGE) + EDGE, 128), F32) for _ in range(BATCHES * UNROLL)],
            vmem((2, 1536, 128), BF16),
            vmem((128, 128), BF16),
            vmem((n_img, pairs, 128), BF16), vmem((n_img, pairs, 128), BF16),
            vmem((n_img, pairs, 128), BF16), vmem((n_img, pairs, 128), BF16),
            vmem((2, n_img, rows, 128), F32),
            vmem((2, n_img, rows, 128), F32),
            vmem((2, n_img, pairs, 128), F32),
            vmem((2, n_img, pairs, 128), F32),
            vmem((2, n_img, rows, 128), F32),
            vmem((2, n_img, rows, 128), F32),
            vmem((2, 4, n_img // UNROLL, UNROLL, 128), F32),
            vmem((2, 4, n_img // UNROLL, UNROLL, 128), F32),
            vmem((2, 4, UNROLL, 128), F32),
            vmem((2, n_dev, 2, 128), F32),
            vmem((2, 8, 256), F32),
            vmem((8, 128), F32),
            dma((n_img // UNROLL,)),
            dma((3,)),
            dma((2, 2)), dma((2, 2, n_img // UNROLL)),
            dma((2, 2)), dma((2, 2, n_img // UNROLL)),
            dma((2, 4)), dma((2, 4, n_img // UNROLL)),
            dma((n_dev - 1,)), dma((2, n_dev)),
        ]
        in_vmem = pl.BlockSpec(memory_space=pltpu.VMEM)
        in_hbm = pl.BlockSpec(memory_space=pltpu.HBM)
        in_any = pl.BlockSpec(memory_space=pl.ANY)
        z, cst = pl.pallas_call(
            functools.partial(stack_kernel, dims),
            out_shape=(vmem((n_img, half, pairs, 128), F32), vmem((8, 128), F32)),
            in_specs=[in_hbm, in_hbm, in_vmem, in_hbm, in_vmem, in_hbm, in_vmem],
            out_specs=(in_vmem, in_vmem),
            scratch_shapes=scratch,
            compiler_params=pltpu.CompilerParams(collective_id=0, has_side_effects=True, vmem_limit_bytes=VMEM_LIMIT),
        )(jnp.transpose(x, (0, 1, 3, 2)), w_a, bn_a, w_down, bn_down, w_b, bn_b)
        return pl.pallas_call(
            finish_kernel,
            out_shape=jax.ShapeDtypeStruct((n_img, half, pairs, 128), BF16),
            in_specs=[in_vmem, in_vmem],
            out_specs=in_any,
            scratch_shapes=[vmem((n_img, half, pairs, 128), BF16), dma((n_img,))],
            compiler_params=pltpu.CompilerParams(vmem_limit_bytes=16 * 1024 * 1024),
        )(z, cst)

    tile_spec = P("dp", "sp", "sp2", None)
    return jax.shard_map(per_device, mesh=mesh, in_specs=(tile_spec, P(), P(), P(), P(), P(), P()), out_specs=tile_spec, check_vma=False)
```

```python
import functools

import jax
import jax.numpy as jnp
from jax import lax
from jax.experimental import pallas as pl
from jax.experimental.pallas import tpu as pltpu
from jax.sharding import PartitionSpec as P

MESH = pl.DeviceIdType.MESH
F32 = jnp.float32
BF16 = jnp.bfloat16
EPS = 1e-5
UNROLL = 4
BATCHES = 2
JOINS = (2, 2)
LONG_JOINS = (1, 1, 2, 2, 2)
VMEM_LIMIT = 51 * 1024 * 1024
EDGE = 8


def normalise(v, cst):
    return jnp.maximum((v - cst[0:1, :]) * cst[1:2, :] + cst[2:3, :], 0.0)


def stack_kernel(dims, x_ref, w_a_ref, bn_a, w_down_ref, bn_down, w_b_ref, bn_b, z_out, cst_out,
                 xv, w_a, w_down, w_b, z, bufs, lines, wmat, perm, edge_u, edge_d, first_u, first_d, edge_l, edge_r, halo_u, halo_d, halo_l, halo_r,
                 corner_s, corner_r, corner_n, stats, acc, cst,
                 x_sem, w_sem, row_send, row_recv, col_send, col_recv, cor_send, cor_recv, st_send, st_recv):
    n_img, rows, pairs, ch, n_sp2, n_sp = dims
    half, quarter = rows // 2, rows // 4
    wide = pairs + EDGE
    data = pl.ds(0, pairs)
    n_dev = n_sp2 * n_sp
    sp = lax.axis_index("sp")
    sp2 = lax.axis_index("sp2")
    me = sp2 * n_sp + sp
    has_u, has_d = sp > 0, sp < n_sp - 1
    has_l, has_r = sp2 > 0, sp2 < n_sp2 - 1

    def x_copy(t):
        some = pl.ds(t * UNROLL, UNROLL)
        return pltpu.make_async_copy(x_ref.at[some], xv.at[some], x_sem.at[t])

    for t in range(n_img // UNROLL):
        x_copy(t).start()

    w_copies = [pltpu.make_async_copy(src, dst, w_sem.at[i]) for i, (src, dst) in enumerate(((w_a_ref, w_a), (w_down_ref, w_down), (w_b_ref, w_b)))]
    for copy in w_copies:
        copy.start()

    barrier = pltpu.get_barrier_semaphore()
    for d in range(1, n_dev):
        peer = lax.rem(me + d, n_dev)
        pl.semaphore_signal(barrier, inc=1, device_id={"sp2": peer // n_sp, "sp": lax.rem(peer, n_sp)}, device_id_type=MESH)

    def rcopy(src, dst, ssem, rsem, to_sp2, to_sp):
        return pltpu.make_async_remote_copy(src_ref=src, dst_ref=dst, send_sem=ssem, recv_sem=rsem,
                                            device_id={"sp2": to_sp2, "sp": to_sp}, device_id_type=MESH)

    corner_to = ((has_u & has_l, -1, -1, 3), (has_u & has_r, 1, -1, 2), (has_d & has_l, -1, 1, 1), (has_d & has_r, 1, 1, 0))

    def start_edges(t, par, n_rows, first=False):
        some, r_all = pl.ds(t * UNROLL, UNROLL), pl.ds(0, n_rows)

        @pl.when(has_l)
        def _():
            rcopy(edge_l.at[par, some, r_all], halo_r.at[par, some, r_all], col_send.at[par, 0], col_recv.at[par, 1, t], sp2 - 1, sp).start()

        @pl.when(has_r)
        def _():
            rcopy(edge_r.at[par, some, r_all], halo_l.at[par, some, r_all], col_send.at[par, 1], col_recv.at[par, 0, t], sp2 + 1, sp).start()

        for c, (there, d_sp2, d_sp, slot) in enumerate(corner_to):
            @pl.when(there)
            def _():
                rcopy(corner_s.at[par, c, t], corner_r.at[par, slot, t], cor_send.at[par, c], cor_recv.at[par, slot, t], sp2 + d_sp2, sp + d_sp).start()

        @pl.when(has_u)
        def _():
            src, dst = (edge_u.at[some], first_d.at[some]) if first else (z.at[some, 0, data], halo_d.at[par, some])
            rcopy(src, dst, row_send.at[par, 0], row_recv.at[par, 1, t], sp2, sp - 1).start()

        @pl.when(has_d)
        def _():
            src, dst = (edge_d.at[some], first_u.at[some]) if first else (z.at[some, n_rows - 1, data], halo_u.at[par, some])
            rcopy(src, dst, row_send.at[par, 1], row_recv.at[par, 0, t], sp2, sp + 1).start()

    def wait_edges(t, par, n_rows, first=False):
        some, r_all = pl.ds(t * UNROLL, UNROLL), pl.ds(0, n_rows)

        @pl.when(has_u)
        def _():
            src, dst = (edge_u.at[some], first_u.at[some]) if first else (z.at[some, 0, data], halo_u.at[par, some])
            rcopy(src, dst, row_send.at[par, 0], row_recv.at[par, 0, t], sp2, sp).wait_recv()

        @pl.when(has_d)
        def _():
            src, dst = (edge_d.at[some], first_d.at[some]) if first else (z.at[some, n_rows - 1, data], halo_d.at[par, some])
            rcopy(src, dst, row_send.at[par, 1], row_recv.at[par, 1, t], sp2, sp).wait_recv()

        @pl.when(has_l)
        def _():
            rcopy(edge_l.at[par, some, r_all], halo_l.at[par, some, r_all], col_send.at[par, 0], col_recv.at[par, 0, t], sp2, sp).wait_recv()

        @pl.when(has_r)
        def _():
            rcopy(edge_r.at[par, some, r_all], halo_r.at[par, some, r_all], col_send.at[par, 1], col_recv.at[par, 1, t], sp2, sp).wait_recv()

        for c, (there, d_sp2, d_sp, slot) in enumerate(corner_to):
            @pl.when(there)
            def _():
                rcopy(corner_s.at[par, c, t], corner_r.at[par, c, t], cor_send.at[par, c], cor_recv.at[par, c, t], sp2, sp).wait_recv()

    def wait_edges_sent(par, n_rows, first=False):
        r_all = pl.ds(0, n_rows)
        every = pl.ds(0, n_img)

        @pl.when(has_u)
        def _():
            src, dst = (edge_u, first_u) if first else (z.at[every, 0, data], halo_u.at[0])
            rcopy(src, dst, row_send.at[par, 0], row_recv.at[0, 0, 0], sp2, sp).wait_send()

        @pl.when(has_d)
        def _():
            src, dst = (edge_d, first_d) if first else (z.at[every, n_rows - 1, data], halo_d.at[0])
            rcopy(src, dst, row_send.at[par, 1], row_recv.at[0, 1, 0], sp2, sp).wait_send()

        @pl.when(has_l)
        def _():
            rcopy(edge_l.at[par, every, r_all], halo_l.at[0, every, r_all], col_send.at[par, 0], col_recv.at[0, 0, 0], sp2, sp).wait_send()

        @pl.when(has_r)
        def _():
            rcopy(edge_r.at[par, every, r_all], halo_r.at[0, every, r_all], col_send.at[par, 1], col_recv.at[0, 1, 0], sp2, sp).wait_send()

        for c, (there, d_sp2, d_sp, slot) in enumerate(corner_to):
            @pl.when(there)
            def _():
                rcopy(corner_s.at[par, c], corner_r.at[0, c], cor_send.at[par, c], cor_recv.at[0, c, 0], sp2, sp).wait_send()

    def stat_copy(d, par):
        peer = lax.rem(me + d, n_dev)
        return rcopy(stats.at[par, me], stats.at[par, me], st_send.at[d - 1], st_recv.at[par, me], peer // n_sp, lax.rem(peer, n_sp))

    def start_stats(par):
        total = acc[0] + acc[1]
        stats[par, me] = jnp.concatenate([jnp.sum(total[:, :128], axis=0, keepdims=True), jnp.sum(total[:, 128:], axis=0, keepdims=True)], axis=0)
        for d in range(1, n_dev):
            stat_copy(d, par).start()

    def wait_stats(par):
        for d in range(1, n_dev):
            stat_copy(d, par).wait_send()
        for d in range(1, n_dev):
            src = lax.rem(me + d, n_dev)
            rcopy(stats.at[par, src], stats.at[par, src], st_send.at[d - 1], st_recv.at[par, src], sp2, sp).wait_recv()

    def set_constants(par, gain, shift, count, paired):
        parts = [stats[par, src] for src in range(n_dev)]
        while len(parts) > 1:
            parts = [a + b for a, b in zip(parts[0::2], parts[1::2])]
        total = parts[0]
        if paired:
            total = total + pltpu.roll(total, ch, 1)
        mean = total[0:1] * (1.0 / count)
        var = total[1:2] * (1.0 / count) - mean * mean
        cst[0:1, :] = mean
        cst[1:2, :] = gain * lax.rsqrt(var + EPS)
        cst[2:3, :] = shift

    lane = lax.broadcasted_iota(jnp.int32, (pairs, 128), 1)

    def save_edges(t, u, n_rows, par):
        img = t * UNROLL + u
        flat = z.at[img].reshape(rows * wide, 128)
        first = flat[pl.ds(0, n_rows, stride=wide), :]
        final = flat[pl.ds(pairs - 1, n_rows, stride=wide), :]
        edge_l[par, img, 0:n_rows, :] = first
        edge_r[par, img, 0:n_rows, :] = final
        corner_s[par, 0, t, u:u + 1, :] = first[0:1]
        corner_s[par, 1, t, u:u + 1, :] = final[0:1]
        corner_s[par, 2, t, u:u + 1, :] = first[n_rows - 1:n_rows]
        corner_s[par, 3, t, u:u + 1, :] = final[n_rows - 1:n_rows]

    def act(v, raw):
        return v if raw else normalise(v, cst)

    def prepare_corners(b, t, par, raw):
        for c, (there, d_sp2, d_sp, slot) in enumerate(corner_to):
            corner_n[b, c] = jnp.where(there, act(corner_r[par, c, t], raw), 0.0)

    def fill_lines(t, par, u, k, n_rows, raw, first_p):
        buf, img, b = lines[k], t * UNROLL + u, k // UNROLL
        left = jnp.where(has_l, act(halo_l[par, img, 0:n_rows, :], raw), 0.0)
        right = jnp.where(has_r, act(halo_r[par, img, 0:n_rows, :], raw), 0.0)
        buf[pl.ds(wide + EDGE - 1, n_rows, stride=wide), :] = left
        buf[pl.ds(wide + EDGE + pairs, n_rows, stride=wide), :] = right
        bottom = (n_rows + 1) * wide
        buf[EDGE - 1:EDGE, :] = corner_n[b, 0, u:u + 1, :]
        buf[EDGE + pairs:EDGE + pairs + 1, :] = corner_n[b, 1, u:u + 1, :]
        buf[bottom + EDGE - 1:bottom + EDGE, :] = corner_n[b, 2, u:u + 1, :]
        buf[bottom + EDGE + pairs:bottom + EDGE + pairs + 1, :] = corner_n[b, 3, u:u + 1, :]
        out = []
        for p in range(first_p, n_rows + 2):
            if p == 0:
                v = jnp.where(has_u, first_u[img].astype(F32) if raw else act(halo_u[par, img], raw), 0.0)
            elif p == n_rows + 1:
                v = jnp.where(has_d, first_d[img].astype(F32) if raw else act(halo_d[par, img], raw), 0.0)
            else:
                v = act(z[img, p - 1, 0:pairs], raw)
            base = p * wide + EDGE
            buf[base:base + pairs, :] = v
            out.append((p, base, v))
        return out

    def build_pairs(t, par, u, k, raw, first_p=0):
        n_q = half + 1
        for p, base, own in fill_lines(t, par, u, k, rows, raw, first_p):
            side = jnp.where(lane < ch, lines[k][base + 1:base + 1 + pairs, :], lines[k][base - 1:base - 1 + pairs, :])
            bufs[k][2 * (p % 2) * n_q + p // 2] = own.astype(BF16)
            bufs[k][(2 * (p % 2) + 1) * n_q + p // 2] = side.astype(BF16)

    def build_wide(t, par, u, k):
        n_q = quarter + 1
        for p, base, own in fill_lines(t, par, u, k, half, False, 0):
            at = 3 * (p % 2) * n_q + p // 2
            bufs[k][at] = lines[k][base - 1:base - 1 + pairs, :].astype(BF16)
            bufs[k][at + n_q] = own.astype(BF16)
            bufs[k][at + 2 * n_q] = lines[k][base + 1:base + 1 + pairs, :].astype(BF16)

    def finish_conv(img, i0, o, dst=z):
        folded = o.reshape(o.shape[0] // 8, 8, 256)
        s = jnp.sum(folded, axis=0)
        q = jnp.sum(folded * folded, axis=0)
        acc[0] += jnp.concatenate([s[:, :128], q[:, :128]], axis=1)
        acc[1] += jnp.concatenate([s[:, 128:], q[:, 128:]], axis=1)
        for i in range(o.shape[0] // pairs):
            dst[img, 2 * (i0 + i), 0:pairs] = o[i * pairs:(i + 1) * pairs, :128]
            dst[img, 2 * (i0 + i) + 1, 0:pairs] = o[i * pairs:(i + 1) * pairs, 128:]

    def dot(parts):
        lhs = jnp.concatenate(parts, axis=1)
        rhs = jnp.concatenate([wmat[0, 0:lhs.shape[1]], wmat[1, 0:lhs.shape[1]]], axis=1)
        return jnp.dot(lhs, rhs, preferred_element_type=F32)

    def join(k, slots, size, n):
        return [jnp.concatenate([block for a in range(n) for block in size(bufs[k + a], j)], axis=0) for j in slots]

    def conv_pairs(t, u, k, par_out, n):
        slots = [c * (half + 1) + lo for lo in (0, 1) for c in range(4)]
        o = dot(join(k, slots, lambda buf, j: [buf[j:j + half].reshape(half * pairs, 128)], n))
        for a in range(n):
            finish_conv(t * UNROLL + u + a, 0, o[a * half * pairs:(a + 1) * half * pairs])
            save_edges(t, u + a, rows, par_out)

    def conv_down(t, u, k, par_out, n):
        slots = [c * (half + 1) + j for j, c in ((0, 2), (0, 3), (1, 0), (1, 1), (1, 2), (1, 3), (2, 0), (2, 1), (2, 2), (2, 3))]
        o = dot(join(k, slots, lambda buf, j: [buf[j + 2 * i] for i in range(quarter)], n))
        for a in range(n):
            finish_conv(t * UNROLL + u + a, 0, o[a * quarter * pairs:(a + 1) * quarter * pairs])
            save_edges(t, u + a, half, par_out)

    def conv_wide(t, u, k, par_out, n):
        slots = [c * (quarter + 1) + lo for lo in (0, 1) for c in range(6)]
        o = dot(join(k, slots, lambda buf, j: [buf[j:j + quarter].reshape(quarter * pairs, 128)], n))
        for a in range(n):
            finish_conv(t * UNROLL + u + a, 0, o[a * quarter * pairs:(a + 1) * quarter * pairs], z_out)

    n_steps = n_img // UNROLL

    def run_layer(par, raw, n_rows, build, conv, n_out, par_out, constants, joins, batches=1):
        acc[...] = jnp.zeros_like(acc)
        for t in range(batches):
            wait_edges(t, par, n_rows, raw)
        constants()

        def body(step, carry):
            steps = [step * batches + b for b in range(batches)]

            @pl.when(step > 0)
            def _():
                for t in steps:
                    wait_edges(t, par, n_rows, raw)

            for b, t in enumerate(steps):
                prepare_corners(b, t, par, raw)
            k = 0
            for n in joins:
                t, u = steps[k // UNROLL], k % UNROLL
                for a in range(n):
                    build(t, u + a, k + a)
                conv(t, u, k, par_out, n)
                k += n
            if n_out:
                @pl.when(step < n_steps // batches - 1)
                def _():
                    for t in steps:
                        start_edges(t, par_out, n_out)
            return carry

        lax.fori_loop(0, n_steps // batches, body, 0)
        start_stats(par_out)
        if n_out:
            for b in range(batches):
                start_edges(n_steps - batches + b, par_out, n_out)

    def put_block(k, n_k, blocks):
        for o, blk in enumerate(blocks):
            wmat[o, k * n_k:(k + 1) * n_k, :] = jnp.zeros((n_k, 128), BF16) if blk is None else blk

    def weights_pairs(layer):
        zero = jnp.zeros((ch, ch), BF16)
        q = []
        for kh in range(3):
            w0, w1, w2 = w_a[layer, kh, 0], w_a[layer, kh, 1], w_a[layer, kh, 2]
            q.append(jnp.concatenate([
                jnp.concatenate([w1, w0], axis=1),
                jnp.concatenate([w2, w1], axis=1),
                jnp.concatenate([zero, w2], axis=1),
                jnp.concatenate([w0, zero], axis=1)], axis=0))
        for k in range(4):
            put_block(k, 256, [q[k] if k < 3 else None, q[k - 1] if k > 0 else None])

    def weights_down():
        d = [jnp.concatenate([w_down[kh, 0], w_down[kh, 1], w_down[kh, 2], jnp.zeros((ch, 128), BF16)], axis=0) for kh in range(3)]
        for k in range(5):
            put_block(k, 256, [d[k] if k < 3 else None, d[k - 2] if k >= 2 else None])

    def weights_wide():
        e = [jnp.concatenate([w_b[0, kh, 0], w_b[0, kh, 1], w_b[0, kh, 2]], axis=0) for kh in range(3)]
        for k in range(4):
            put_block(k, 384, [e[k] if k < 3 else None, e[k - 1] if k > 0 else None])

    wrow = lax.broadcasted_iota(jnp.int32, (128, 128), 0)
    wcol = lax.broadcasted_iota(jnp.int32, (128, 128), 1)
    source = jnp.where(wrow < pairs, 2 * wrow, 2 * (wrow - pairs) + 1)
    perm[...] = jnp.where(source == wcol, 1.0, 0.0).astype(BF16)

    def load_images(t, carry):
        x_copy(t).wait()
        for img_u in range(UNROLL):
            img = t * UNROLL + img_u
            for g in range(rows // 4):
                block = xv[img, 4 * g:4 * g + 4].reshape(4 * ch, 128)
                m = lax.dot_general(perm[...], block, (((1,), (1,)), ((), ())), preferred_element_type=F32)
                for b in range(2):
                    even = m[0:pairs, 128 * b:128 * b + 128]
                    odd = m[pairs:2 * pairs, 128 * b:128 * b + 128]
                    r = 4 * g + 2 * b
                    upper = jnp.where(lane < ch, even, pltpu.roll(odd, ch, 1))
                    lower = jnp.where(lane < ch, pltpu.roll(even, ch, 1), odd)
                    z[img, r, 0:pairs] = upper
                    z[img, r + 1, 0:pairs] = lower
                    if r == 0:
                        edge_u[img] = upper.astype(BF16)
                    if r + 2 == rows:
                        edge_d[img] = lower.astype(BF16)
            save_edges(t, img_u, rows, 0)

        @pl.when(t == 0)
        def _():
            pl.semaphore_wait(barrier, n_dev - 1)

        start_edges(t, 0, rows, True)
        return carry

    lax.fori_loop(0, n_steps, load_images, 0)

    count_a = float(n_dev * n_img * rows * pairs * 2)
    count_b = float(n_dev * n_img * half * pairs)

    for copy in w_copies:
        copy.wait()
    weights_pairs(0)
    run_layer(0, True, rows, lambda t, u, k: build_pairs(t, 0, u, k, True), conv_pairs, rows, 1, lambda: None, LONG_JOINS, BATCHES)
    wait_edges_sent(0, rows, True)

    def gains(layer):
        g, s = bn_a[layer, 0:1, :], bn_a[layer, 1:2, :]
        return jnp.concatenate([g, g], axis=1), jnp.concatenate([s, s], axis=1)

    n_layers = w_a.shape[0]

    def a_layer(layer, carry):
        par = lax.rem(layer, 2)
        weights_pairs(layer)
        wait_edges_sent(par, rows)

        def constants():
            wait_stats(par)
            g, s = gains(layer - 1)
            set_constants(par, g, s, count_a, True)

        run_layer(par, False, rows, lambda t, u, k: build_pairs(t, par, u, k, False), conv_pairs, rows, 1 - par, constants, LONG_JOINS, BATCHES)
        return carry

    lax.fori_loop(1, n_layers, a_layer, 0)

    par = n_layers % 2
    weights_down()
    wait_edges_sent(par, rows)

    def constants():
        wait_stats(par)
        g, s = gains(n_layers - 1)
        set_constants(par, g, s, count_a, True)

    run_layer(par, False, rows, lambda t, u, k: build_pairs(t, par, u, k, False, 1), conv_down, half, 1 - par, constants, JOINS)

    weights_wide()
    wait_edges_sent(1 - par, half)

    def constants():
        wait_stats(1 - par)
        set_constants(1 - par, bn_down[0:1, :], bn_down[1:2, :], count_b, False)

    run_layer(1 - par, False, half, lambda t, u, k: build_wide(t, 1 - par, u, k), conv_wide, 0, par, constants, JOINS * 2, BATCHES)
    wait_stats(par)
    set_constants(par, bn_b[0, 0:1, :], bn_b[0, 1:2, :], count_b, False)
    cst_out[...] = cst[...]


def finish_kernel(z, cst_ref, out_ref, y, out_sem):
    n_img, n_rows = z.shape[:2]

    def copy(img):
        return pltpu.make_async_copy(y.at[img], out_ref.at[img], out_sem.at[img])

    def step(img, carry):
        for r in range(n_rows):
            y[img, r] = normalise(z[img, r], cst_ref).astype(BF16)
        copy(img).start()
        return carry

    lax.fori_loop(0, n_img, step, 0)
    for img in range(n_img):
        copy(img).wait()


def solution(mesh):
    n_sp, n_sp2 = mesh.shape["sp"], mesh.shape["sp2"]

    def per_device(x, w_a, bn_a, w_down, bn_down, w_b, bn_b):
        n_img, rows, cols, ch = x.shape
        pairs, half = cols // 2, rows // 2
        n_dev = n_sp * n_sp2
        dims = (n_img, rows, pairs, ch, n_sp2, n_sp)
        vmem = pltpu.VMEM
        dma = pltpu.SemaphoreType.DMA
        scratch = [
            vmem((n_img, rows, ch, cols), BF16),
            vmem(w_a.shape, BF16), vmem(w_down.shape, BF16), vmem(w_b.shape, BF16),
            vmem((n_img, rows, pairs + EDGE, 128), F32),
            [vmem((4 * (half + 1), pairs, 128), BF16) for _ in range(BATCHES * UNROLL)],
            [vmem(((rows + 2) * (pairs + EDGE) + EDGE, 128), F32) for _ in range(BATCHES * UNROLL)],
            vmem((2, 1536, 128), BF16),
            vmem((128, 128), BF16),
            vmem((n_img, pairs, 128), BF16), vmem((n_img, pairs, 128), BF16),
            vmem((n_img, pairs, 128), BF16), vmem((n_img, pairs, 128), BF16),
            vmem((2, n_img, rows, 128), F32),
            vmem((2, n_img, rows, 128), F32),
            vmem((2, n_img, pairs, 128), F32),
            vmem((2, n_img, pairs, 128), F32),
            vmem((2, n_img, rows, 128), F32),
            vmem((2, n_img, rows, 128), F32),
            vmem((2, 4, n_img // UNROLL, UNROLL, 128), F32),
            vmem((2, 4, n_img // UNROLL, UNROLL, 128), F32),
            vmem((2, 4, UNROLL, 128), F32),
            vmem((2, n_dev, 2, 128), F32),
            vmem((2, 8, 256), F32),
            vmem((8, 128), F32),
            dma((n_img // UNROLL,)),
            dma((3,)),
            dma((2, 2)), dma((2, 2, n_img // UNROLL)),
            dma((2, 2)), dma((2, 2, n_img // UNROLL)),
            dma((2, 4)), dma((2, 4, n_img // UNROLL)),
            dma((n_dev - 1,)), dma((2, n_dev)),
        ]
        in_vmem = pl.BlockSpec(memory_space=pltpu.VMEM)
        in_hbm = pl.BlockSpec(memory_space=pltpu.HBM)
        in_any = pl.BlockSpec(memory_space=pl.ANY)
        z, cst = pl.pallas_call(
            functools.partial(stack_kernel, dims),
            out_shape=(vmem((n_img, half, pairs, 128), F32), vmem((8, 128), F32)),
            in_specs=[in_hbm, in_hbm, in_vmem, in_hbm, in_vmem, in_hbm, in_vmem],
            out_specs=(in_vmem, in_vmem),
            scratch_shapes=scratch,
            compiler_params=pltpu.CompilerParams(collective_id=0, has_side_effects=True, vmem_limit_bytes=VMEM_LIMIT),
        )(jnp.transpose(x, (0, 1, 3, 2)), w_a, bn_a, w_down, bn_down, w_b, bn_b)
        return pl.pallas_call(
            finish_kernel,
            out_shape=jax.ShapeDtypeStruct((n_img, half, pairs, 128), BF16),
            in_specs=[in_vmem, in_vmem],
            out_specs=in_any,
            scratch_shapes=[vmem((n_img, half, pairs, 128), BF16), dma((n_img,))],
            compiler_params=pltpu.CompilerParams(vmem_limit_bytes=16 * 1024 * 1024),
        )(z, cst)

    tile_spec = P("dp", "sp", "sp2", None)
    return jax.shard_map(per_device, mesh=mesh, in_specs=(tile_spec, P(), P(), P(), P(), P(), P()), out_specs=tile_spec, check_vma=False)
```
